32 devices in a mesh: seq: 8 (over y, x, core), fsdp: 4 (over z).
Axes of the slice: x: 2, y: 2, z: 4, core: 2. Of those that a mesh axis runs over, the one named last changes fastest.
Arguments:
- hidden: bfloat16 [4096, 8192], P(('seq', 'fsdp')), may hold values from -6 to 6
- kv_blocks: bfloat16 [8192, 1024], P('fsdp'), may hold values from -0.0625 to 0.0625
- kv_scale: float32 [64, 8], P('fsdp'), may hold values from 0.5 to 2
- queries: bfloat16 [4096, 4096], P(('seq', 'fsdp')), may hold values from -24 to 24
- grad_out: bfloat16 [4096, 4096], P(('seq', 'fsdp')), may hold values from -6 to 6
Outputs:
- attn_out: bfloat16 [4096, 4096], P(('seq', 'fsdp'))
- grad_queries: bfloat16 [4096, 4096], P(('seq', 'fsdp'))
- grad_hidden: bfloat16 [4096, 8192], P(('seq', 'fsdp'))
- weight_grad: float32 [8192, 1024], P('fsdp')
The draws below stay inside these ranges and needn't reach their ends.
All inputs are finite; a program needn't handle non-finite values.
Results may differ from the reference program's by a relative error of at most 0.0075.
The reference program's roundings to bfloat16 on the way (of `weights`, `kv`, `probs_b` and `dscores`) count: a program that leaves them out, or rounds other values in their place, can miss the bound.
Values may be sent and summed in bfloat16 or wider, within the bound.
A program may use at most 128 MiB of HBM per device.

```python
import math
import jax
import jax.numpy as jnp
from jax import lax

D = 8192
HEADS = 32
KV_HEADS = 4
HEAD = 128
QB = 128
TOK_DEV = 128
KVW = 512
SEG = 512
SPAN = 256
TOKENS = 4096


def draw_queries(key, part):
    shape = (TOKENS, HEADS * HEAD)
    first = jax.random.fold_in(jax.random.fold_in(key, 17), 0)
    return jnp.clip(jax.random.normal(first, shape, jnp.float32), -4.0, 4.0).astype(jnp.bfloat16)


def strengthened(array, rng, source, target, blocks, factor):
    def block_of(axis_at):
        return (jnp.arange(array.shape[axis_at]) // (array.shape[axis_at] // blocks)).reshape((-1,) + (1,) * (array.ndim - 1 - axis_at))

    first = jax.random.permutation(rng, blocks)[block_of(target)]
    far = (block_of(target) + blocks // 2) % blocks
    return jnp.where((block_of(source) == first) | (block_of(source) == far), factor * array, array)


def shard_levels(own_key, shape, cuts, low, top_value):
    gain, own = 1.0, jax.random.fold_in(own_key, 6)
    for axis_at, shards_of in cuts:
        draws = jnp.exp(jax.random.uniform(jax.random.fold_in(own, axis_at), (shards_of,), jnp.float32, low / len(cuts), top_value / len(cuts)))
        gain = gain * jnp.repeat(draws, shape[axis_at] // shards_of).reshape([-1 if axis == axis_at else 1 for axis in range(len(shape))])
    return gain


def centred(key, shape, scale, bound, shards=(), held_as=jnp.bfloat16):
    entries = jax.random.normal(key, shape, jnp.float32) * scale
    if len(shards) > 0:
        entries = shard_levels(key, shape, shards, -0.22, 0.18) * entries
    return jnp.clip(entries, min=-bound, max=bound).astype(held_as)


def noise_with(rng, shape, scale, bound, cuts, heavy, kind=jnp.bfloat16):
    entries = scale * jax.random.normal(rng, shape, jnp.float32)
    if cuts:
        entries = entries * shard_levels(rng, shape, cuts, -0.22, 0.18)
    return jnp.clip(strengthened(entries, jax.random.fold_in(rng, 3), *heavy), -bound, bound).astype(kind)


def setup_inputs(seed: int = 0) -> dict:
    key_list = jax.random.split(jax.random.key(seed), 6)
    return {
        "hidden": noise_with(key_list[0], (TOKENS, D), 1.0, 6.0, ((0, 32),), (0, 1, 32, 2.75)),
        "kv_blocks": centred(key_list[1], (D, 2 * KVW), D ** -0.5, 0.0625, ((0, 4),)),
        "kv_scale": jnp.clip(jnp.exp(math.log(2.0) - 1.3862944 * jax.random.uniform(key_list[2], (D // QB, 2 * KVW // QB), jnp.float32) ** shard_levels(key_list[2], (D // QB, 2 * KVW // QB), ((0, 4),), -0.2, 0.2)), 0.5, 2.0),
        "queries": draw_queries(jax.random.fold_in(key_list[5], 71), 0),
        "grad_out": centred(key_list[4], (TOKENS, HEADS * HEAD), 1.0, 6.0, ((0, 32),)),
    }


NEG = -1e+30

def dequantize(blocks, scale):
    rows, cols = blocks.shape
    grid = blocks.astype(jnp.float32).reshape(scale.shape[0], QB, scale.shape[1], QB)
    return (grid * scale[:, None, :, None]).reshape(rows, cols).astype(jnp.bfloat16)

def attend_group(operands, allowed):
    qgrp, kgrp, vgrp, ggrp = operands
    factor = 1.0 / math_sqrt(HEAD)
    qf = qgrp.astype(jnp.float32)
    kf = kgrp.astype(jnp.float32)
    vf = vgrp.astype(jnp.float32)
    gf = ggrp.astype(jnp.float32)
    scores = jnp.einsum('rhd,kd->rhk', qf, kf) * factor
    scores = jnp.where(allowed[:, None, :], scores, NEG)
    top = lax.optimization_barrier(jnp.max(scores, axis=-1, keepdims=True))
    expd = jnp.exp(scores - top)
    probs = expd / lax.optimization_barrier(jnp.sum(expd, axis=-1, keepdims=True))
    probs_b = probs.astype(jnp.bfloat16)
    pf = probs_b.astype(jnp.float32)
    output = jnp.einsum('rhk,kd->rhd', pf, vf).astype(jnp.bfloat16)
    dprobs = jnp.einsum('rhd,kd->rhk', gf, vf)
    delta = lax.optimization_barrier(jnp.sum(probs * dprobs, axis=-1, keepdims=True))
    dscores = (probs * (dprobs - delta) * factor).astype(jnp.bfloat16)
    df = dscores.astype(jnp.float32)
    gradq = jnp.einsum('rhk,kd->rhd', df, kf).astype(jnp.bfloat16)
    gradk = jnp.einsum('rhk,rhd->kd', df, qf)
    gradv = jnp.einsum('rhk,rhd->kd', pf, gf)
    return (output, gradq, gradk, gradv)

def math_sqrt(value):
    return float(value) ** 0.5

def attend(queries, window, grad_out, allowed):
    rows = queries.shape[0]
    count = window.shape[0]
    group = HEADS // KV_HEADS
    qgrp = queries.reshape(rows, KV_HEADS, group, HEAD).transpose(1, 0, 2, 3)
    ggrp = grad_out.reshape(rows, KV_HEADS, group, HEAD).transpose(1, 0, 2, 3)
    kgrp = window[:, :KVW].reshape(count, KV_HEADS, HEAD).transpose(1, 0, 2)
    vgrp = window[:, KVW:].reshape(count, KV_HEADS, HEAD).transpose(1, 0, 2)
    output, gradq, gradk, gradv = lax.map(lambda ops: attend_group(ops, allowed), (qgrp, kgrp, vgrp, ggrp))
    output = output.transpose(1, 0, 2, 3).reshape(rows, HEADS * HEAD)
    gradq = gradq.transpose(1, 0, 2, 3).reshape(rows, HEADS * HEAD)
    gradk = gradk.transpose(1, 0, 2).reshape(count, KVW)
    gradv = gradv.transpose(1, 0, 2).reshape(count, KVW)
    return (output, gradq, jnp.concatenate([gradk, gradv], axis=1))

def reference(hidden, kv_blocks, kv_scale, queries, grad_out):
    weights = dequantize(kv_blocks, kv_scale)
    kv = jnp.dot(hidden, weights, preferred_element_type=jnp.float32).astype(jnp.bfloat16)
    padded = jnp.concatenate([jnp.zeros((SPAN, 2 * KVW), jnp.bfloat16), kv], axis=0)
    width = SPAN + TOK_DEV
    blocks = TOKENS // TOK_DEV

    def step(carry, index):
        acc_all, acc_seg = carry
        start = (index * TOK_DEV).astype(jnp.int32)
        qrows = lax.dynamic_slice_in_dim(queries, start, TOK_DEV, 0)
        grows = lax.dynamic_slice_in_dim(grad_out, start, TOK_DEV, 0)
        window = lax.dynamic_slice_in_dim(padded, start, width, 0)
        qpos = start + jnp.arange(TOK_DEV, dtype=jnp.int32)
        kpos = start - SPAN + jnp.arange(width, dtype=jnp.int32)
        allowed = (qpos[:, None] - kpos[None, :] < SPAN) & (kpos[None, :] <= qpos[:, None]) & (kpos[None, :] >= 0)
        seg_start = start // SEG * SEG
        inside = (kpos >= seg_start).astype(jnp.float32)
        output, gradq, dwin = attend(qrows, window, grows, allowed)
        old_all = lax.dynamic_slice_in_dim(acc_all, start, width, 0)
        acc_all = lax.dynamic_update_slice_in_dim(acc_all, old_all + dwin, start, 0)
        old_seg = lax.dynamic_slice_in_dim(acc_seg, start, width, 0)
        acc_seg = lax.dynamic_update_slice_in_dim(acc_seg, old_seg + dwin * inside[:, None], start, 0)
        return ((acc_all, acc_seg), (output, gradq))
    zeros = jnp.zeros((SPAN + TOKENS, 2 * KVW), jnp.float32)
    (acc_all, acc_seg), (outputs, gradqs) = lax.scan(step, (zeros, zeros), jnp.arange(blocks, dtype=jnp.int32))
    attn_out = outputs.reshape(TOKENS, HEADS * HEAD)
    grad_queries = gradqs.reshape(TOKENS, HEADS * HEAD)
    dkv_all = acc_all[SPAN:].astype(jnp.bfloat16)
    dkv_seg = acc_seg[SPAN:].astype(jnp.bfloat16)
    grad_hidden = jnp.dot(dkv_seg, weights.T, preferred_element_type=jnp.float32).astype(jnp.bfloat16)
    weight_grad = jnp.dot(hidden.T, dkv_all, preferred_element_type=jnp.float32)
    return (attn_out, grad_queries, grad_hidden, weight_grad)
```

```python
import functools

import jax
import jax.numpy as jnp
from jax import lax
from jax.experimental import pallas as pl
from jax.experimental.pallas import tpu as pltpu
from jax.sharding import PartitionSpec as P

HEADS = 32
KV_HEADS = 4
HEAD = 128
QB = 128


NEG = -1e30
PLANNED = (4, 4, 8)
(SEND, FORWARD, BEGIN, CUBE, PAIR, LAND, PROJECT, ATTEND, SETTLE, WIDEN, SHARE) = range(11)
(PRODUCT, HOP, REDUCE, EXPAND, RELAY, FINISH, SPREAD, HIDDEN, TURN) = range(11, 20)
VMEM_LIMIT = 50 << 20
WIDE = (2,)
ORDER = (
    (HIDDEN, 3), (SEND, 1), (FORWARD, 1, 0), (FORWARD, 0, 0), (BEGIN, 1, 0), (SEND, 2), (FORWARD, 0, 1), (TURN, 3),
    (BEGIN, 0, 0), (BEGIN, 0, 1), (SEND, 3), (CUBE, 1, 0), (CUBE, 0, 0), (FORWARD, 2, 0), (FORWARD, 0, 2),
    (BEGIN, 2, 0), (FORWARD, 1, 1), (BEGIN, 0, 2), (CUBE, 0, 1), (FORWARD, 1, 2), (PAIR, 0, 2), (CUBE, 2, 0),
    (BEGIN, 1, 2), (FORWARD, 2, 2), (BEGIN, 2, 2), (PAIR, 2, 0), (PAIR, 0, 0), (FORWARD, 1, 3), (BEGIN, 1, 3),
    (PAIR, 0, 1), (BEGIN, 1, 1), (FORWARD, 0, 3), (PAIR, 1, 0), (LAND, 0, 1), (LAND, 0, 0), (LAND, 2, 0),
    (FORWARD, 2, 1), (BEGIN, 0, 3), (BEGIN, 2, 1), (PAIR, 1, 2), (PAIR, 2, 2), (LAND, 1, 0), (FORWARD, 2, 3),
    (PROJECT, 0), (BEGIN, 2, 3), (LAND, 0, 2), (LAND, 2, 2), (LAND, 1, 2), (CUBE, 1, 3), (CUBE, 0, 3), (PROJECT, 2),
    (CUBE, 2, 3), (ATTEND, 0), (CUBE, 2, 1), (CUBE, 1, 1), (PAIR, 0, 3), (ATTEND, 2), (SETTLE, 0), (PAIR, 1, 3),
    (PAIR, 2, 3), (TURN, 0), (HIDDEN, 2), (LAND, 1, 3), (LAND, 0, 3), (WIDEN, 0), (PAIR, 1, 1), (HIDDEN, 1),
    (PAIR, 2, 1), (LAND, 2, 3), (PROJECT, 3), (LAND, 1, 1), (LAND, 2, 1), (PROJECT, 1), (ATTEND, 3), (TURN, 2),
    (SHARE, 0), (ATTEND, 1), (SETTLE, 2), (TURN, 1), (PRODUCT, 0), (WIDEN, 2), (SHARE, 2), (PRODUCT, 2), (SETTLE, 1),
    (SETTLE, 3), (HOP, 0, 1), (WIDEN, 1), (HOP, 0, 2), (SHARE, 1), (WIDEN, 3), (PRODUCT, 1), (HOP, 2, 1), (REDUCE, 0),
    (SPREAD, 3), (EXPAND, 0), (SHARE, 3), (HOP, 2, 2), (SPREAD, 0), (HOP, 1, 1), (REDUCE, 2), (HOP, 1, 2),
    (PRODUCT, 3), (EXPAND, 2), (RELAY, 0), (REDUCE, 1), (HOP, 3, 1), (RELAY, 2), (HOP, 3, 2), (EXPAND, 1),
    (REDUCE, 3), (EXPAND, 3), (RELAY, 1), (SPREAD, 2), (SPREAD, 1), (FINISH, 2), (FINISH, 0), (RELAY, 3), (FINISH, 1),
    (FINISH, 3),
)


def shifted(block, axis, distance):
    devices = range(lax.axis_size(axis))
    route = [(i - distance, i) for i in devices if i - distance in devices]
    return lax.ppermute(block, axis, route)


def attend_kernel(reach, q_ref, g_ref, k_ref, v_ref, out_ref, dq_ref, dk_ref, dv_ref):
    tok = q_ref.shape[0]
    group = q_ref.shape[1] // HEAD
    count = k_ref.shape[0]
    span = reach * tok
    factor = 1.0 / float(HEAD) ** 0.5
    base = (lax.axis_index("seq") * lax.axis_size("fsdp") + lax.axis_index("fsdp")) * tok
    row = lax.broadcasted_iota(jnp.int32, (tok, count), 0)
    col = lax.broadcasted_iota(jnp.int32, (tok, count), 1)
    allowed = (col > row) & (col <= row + span) & (col >= span - base)
    keys = k_ref[...]
    values = v_ref[...]
    nt = (((1,), (1,)), ((), ()))
    tn = (((0,), (0,)), ((), ()))
    ps, ds, qs, gs = [], [], [], []
    for h in range(group):
        cut = slice(h * HEAD, (h + 1) * HEAD)
        q = q_ref[:, cut]
        g = g_ref[:, cut]
        scores = lax.dot_general(q, keys, nt, preferred_element_type=jnp.float32) * factor
        scores = jnp.where(allowed, scores, NEG)
        expd = jnp.exp(scores - jnp.max(scores, axis=-1, keepdims=True))
        probs = expd * (1.0 / jnp.sum(expd, axis=-1, keepdims=True))
        probs_b = probs.astype(jnp.bfloat16)
        out_ref[:, cut] = jnp.dot(probs_b, values, preferred_element_type=jnp.float32).astype(jnp.bfloat16)
        dprobs = lax.dot_general(g, values, nt, preferred_element_type=jnp.float32)
        delta = jnp.sum(probs * dprobs, axis=-1, keepdims=True)
        dscores = (probs * (dprobs - delta) * factor).astype(jnp.bfloat16)
        dq_ref[:, cut] = jnp.dot(dscores, keys, preferred_element_type=jnp.float32).astype(jnp.bfloat16)
        ps.append(probs_b)
        ds.append(dscores)
        qs.append(q)
        gs.append(g)
    cat = lambda parts: jnp.concatenate(parts, axis=0)
    dk_ref[...] = lax.dot_general(cat(ds), cat(qs), tn, preferred_element_type=jnp.float32)
    dv_ref[...] = lax.dot_general(cat(ps), cat(gs), tn, preferred_element_type=jnp.float32)


def attend(queries, window, grad_out, reach):
    tok, width = queries.shape
    count = window.shape[0]
    heads = window.shape[1] // (2 * HEAD)
    wide = pl.BlockSpec((tok, width // heads), lambda i: (0, i))
    key = pl.BlockSpec((count, HEAD), lambda i: (0, i))
    value = pl.BlockSpec((count, HEAD), lambda i: (0, i + heads))
    out, dq, dk, dv = pl.pallas_call(
        functools.partial(attend_kernel, reach),
        grid=(heads,),
        in_specs=[wide, wide, key, value],
        out_specs=[wide, wide, key, key],
        out_shape=[
            jax.ShapeDtypeStruct((tok, width), jnp.bfloat16),
            jax.ShapeDtypeStruct((tok, width), jnp.bfloat16),
            jax.ShapeDtypeStruct((count, heads * HEAD), jnp.float32),
            jax.ShapeDtypeStruct((count, heads * HEAD), jnp.float32),
        ],
        cost_estimate=pl.CostEstimate(flops=12 * tok * width * count, bytes_accessed=8 * tok * width, transcendentals=0),
        name="attend",
    )(queries, grad_out, window, window)
    return out, dq, jnp.concatenate([dk, dv], axis=1)


def flipped(index, mask):
    for place in range(mask.bit_length()):
        if mask >> place & 1:
            index = index + (1 << place) * (1 - 2 * (index // (1 << place) % 2))
    return index


def orders_of(bits):
    return (list(range(1, bits)) + [0], list(range(bits - 1, 0, -1)) + [0])


def project_kernel(seqs, groups, hid_ref, blk_ref, sc_ref, out_ref, kv_ref, col_ref, w_ref, acc, zsend, zrecv, qsend, qrecv, csend, crecv, wsem):
    s = lax.axis_index("seq")
    z = lax.axis_index("fsdp")
    rows = blk_ref.shape[0]
    unit = rows // seqs
    half = unit // 2
    bits = seqs.bit_length() - 1
    chunk = min(512, rows)

    def scale_block(i, carry):
        at = pl.multiple_of(i * QB, QB)
        block = blk_ref[pl.ds(at, QB), :].astype(jnp.float32) * sc_ref[pl.ds(i, 1), :]
        w_ref[pl.ds(pl.multiple_of(z * rows + at, QB), QB), :] = block.astype(jnp.bfloat16)
        return carry

    lax.fori_loop(0, rows // QB, scale_block, 0)

    def line_copy(shard, up):
        piece = w_ref.at[pl.ds(pl.multiple_of(shard * rows + s * unit, 16), unit), :]
        return pltpu.make_async_remote_copy(
            src_ref=piece,
            dst_ref=piece,
            send_sem=zsend.at[up, shard],
            recv_sem=zrecv.at[shard],
            device_id=(s, z + 1 if up else z - 1),
            device_id_type=pl.DeviceIdType.MESH,
        )

    def cube_copy(turn, shard, order, step, which, incoming):
        bit = order[step]
        mask = 0
        for k in range(step):
            if which >> k & 1:
                mask |= 1 << order[k]
        h = 0 if order is orders[0] else 1
        owner = flipped(s, mask | (1 << bit) if incoming else mask)
        piece = w_ref.at[pl.ds(pl.multiple_of(shard * rows + owner * unit + h * half, 16), half), :]
        slot = (1 << step) - 1 + which
        return pltpu.make_async_remote_copy(
            src_ref=piece,
            dst_ref=piece,
            send_sem=qsend.at[turn, h, slot],
            recv_sem=qrecv.at[turn, h, slot],
            device_id=(flipped(s, 1 << bit), z),
            device_id_type=pl.DeviceIdType.MESH,
        )

    orders = orders_of(bits)
    near = jnp.minimum(z, groups - 1 - z)

    def shard_at(turn):
        step = turn // 2 + 1
        paired = z - step if turn % 2 == 0 else z + step
        far = turn - near + 1
        single = jnp.where(z > groups - 1 - z, z - far, z + far)
        return jnp.where(turn < 2 * near, paired, single)

    shards = [shard_at(turn) for turn in range(groups - 1)]

    @pl.when(z < groups - 1)
    def _():
        line_copy(z, 1).start()

    @pl.when(z > 0)
    def _():
        line_copy(z, 0).start()

    def column_copy(gap, incoming):
        other = (z - gap + groups) % groups if incoming else (z + gap) % groups
        part = pl.multiple_of(other * rows, 128)
        return pltpu.make_async_remote_copy(
            src_ref=hid_ref.at[:, pl.ds(part, rows)],
            dst_ref=col_ref.at[other if incoming else z],
            send_sem=csend.at[gap - 1],
            recv_sem=crecv.at[gap - 1],
            device_id=(s, other),
            device_id_type=pl.DeviceIdType.MESH,
        )

    acc[...] = jnp.zeros_like(acc)

    def store_copy(turn, shard):
        part = pl.ds(pl.multiple_of(shard * rows, 16), rows)
        return pltpu.make_async_copy(w_ref.at[part, :], out_ref.at[part, :], wsem.at[turn])

    def multiply(shard):
        def part(i, carry):
            at = pl.multiple_of(shard * rows + i * chunk, 128)
            acc[...] += jnp.dot(
                hid_ref[:, pl.ds(at, chunk)], w_ref[pl.ds(at, chunk), :], preferred_element_type=jnp.float32
            )
            return carry

        lax.fori_loop(0, rows // chunk, part, 0)

    multiply(z)
    store_copy(groups - 1, z).start()
    col_ref[z] = hid_ref[:, pl.ds(pl.multiple_of(z * rows, 128), rows)]
    for tick in range(groups - 1 + bits):
        for stage in range(bits, -1, -1):
            turn = tick - stage
            if turn < 0 or turn >= groups - 1:
                continue
            shard = shards[turn]
            if stage == 0:
                line_copy(shard, 0).wait_recv()

                @pl.when((shard < z) & (z < groups - 1))
                def _():
                    line_copy(shard, 1).start()

                @pl.when((shard > z) & (z > 0))
                def _():
                    line_copy(shard, 0).start()
            else:
                for order in orders:
                    for which in range(1 << (stage - 1)):
                        cube_copy(turn, shard, order, stage - 1, which, True).wait_recv()
            if stage < bits:
                for order in orders:
                    for which in range(1 << stage):
                        cube_copy(turn, shard, order, stage, which, False).start()
            else:
                multiply(shard)
                store_copy(turn, shard).start()
        if tick == groups - 2:
            for gap in range(1, groups):
                column_copy(gap, False).start()
    kv_ref[...] = acc[...].astype(jnp.bfloat16)
    for turn in range(groups - 1):
        store_copy(turn, shards[turn]).wait()
    store_copy(groups - 1, z).wait()
    for gap in range(1, groups):
        column_copy(gap, True).wait_recv()
        column_copy(gap, False).wait_send()
    for shard in range(groups):

        @pl.when((shard <= z) & (z < groups - 1))
        def _():
            line_copy(shard, 1).wait_send()

        @pl.when((shard >= z) & (z > 0))
        def _():
            line_copy(shard, 0).wait_send()

    for turn in range(groups - 1):
        for order in orders:
            for stage in range(bits):
                for which in range(1 << stage):
                    cube_copy(turn, shards[turn], order, stage, which, False).wait_send()


def project(hidden, kv_blocks, kv_scale):
    seqs = lax.axis_size("seq")
    groups = lax.axis_size("fsdp")
    tok, width = hidden.shape
    cols = kv_blocks.shape[1]
    spread = jnp.repeat(kv_scale, QB, axis=1)
    vmem = pl.BlockSpec(memory_space=pltpu.VMEM)
    return pl.pallas_call(
        functools.partial(project_kernel, seqs, groups),
        out_shape=[
            jax.ShapeDtypeStruct((width, cols), jnp.bfloat16),
            jax.ShapeDtypeStruct((tok, cols), jnp.bfloat16),
            jax.ShapeDtypeStruct((groups, tok, kv_blocks.shape[0]), jnp.bfloat16),
        ],
        in_specs=[vmem] * 3,
        out_specs=[pl.BlockSpec(memory_space=pl.ANY), vmem, vmem],
        scratch_shapes=[
            pltpu.VMEM((width, cols), jnp.bfloat16),
            pltpu.VMEM((tok, cols), jnp.float32),
            pltpu.SemaphoreType.DMA((2, groups)),
            pltpu.SemaphoreType.DMA((groups,)),
            pltpu.SemaphoreType.DMA((groups - 1, 2, seqs - 1)),
            pltpu.SemaphoreType.DMA((groups - 1, 2, seqs - 1)),
            pltpu.SemaphoreType.DMA((groups - 1,)),
            pltpu.SemaphoreType.DMA((groups - 1,)),
            pltpu.SemaphoreType.DMA((groups,)),
        ],
        compiler_params=pltpu.CompilerParams(has_side_effects=True),
        name="project",
    )(hidden, kv_blocks, spread)


def finish_kernel(
    seqs, groups, reach, back_ref, own_ref, in_ref, col_ref, gh_ref, wg_ref,
    w_ref, wsem, ret, every, inside, acc, sends, recvs, hsend, hrecv, gsend, grecv, rsend, rrecv, asend, arecv,
):
    s = lax.axis_index("seq")
    z = lax.axis_index("fsdp")
    linear = s * groups + z
    devices = seqs * groups
    tok, cols = own_ref.shape
    rows = col_ref.shape[1]
    bits = seqs.bit_length() - 1
    mesh_id = pl.DeviceIdType.MESH
    load = pltpu.make_async_copy(in_ref, w_ref, wsem)
    load.start()

    def halo_copy(offset, incoming):
        other = linear + offset if incoming else linear - offset
        return pltpu.make_async_remote_copy(
            src_ref=back_ref.at[pl.ds((reach - offset) * tok, tok), :],
            dst_ref=ret.at[offset - 1],
            send_sem=hsend.at[offset - 1],
            recv_sem=hrecv.at[offset - 1],
            device_id=(other // groups, other % groups),
            device_id_type=mesh_id,
        )

    for offset in range(1, reach + 1):

        @pl.when(linear >= offset)
        def _():
            halo_copy(offset, False).start()

    for offset in range(1, reach + 1):

        @pl.when(linear + offset < devices)
        def _():
            halo_copy(offset, True).wait_recv()

        @pl.when(linear + offset >= devices)
        def _():
            ret[offset - 1] = jnp.zeros((tok, cols), jnp.bfloat16)

    total = own_ref[...]
    seg = total
    for offset in range(1, reach + 1):
        piece = ret[offset - 1].astype(jnp.float32)
        total = total + piece
        seg = seg + piece * jnp.where(z + offset < groups, 1.0, 0.0)
    every[z] = total.astype(jnp.bfloat16)
    inside[...] = seg.astype(jnp.bfloat16)

    def gather_copy(gap, incoming):
        other = (z - gap + groups) % groups if incoming else (z + gap) % groups
        block = every.at[other if incoming else z]
        return pltpu.make_async_remote_copy(
            src_ref=block,
            dst_ref=block,
            send_sem=gsend.at[gap - 1],
            recv_sem=grecv.at[gap - 1],
            device_id=(s, other),
            device_id_type=mesh_id,
        )

    for gap in range(1, groups):
        gather_copy(gap, False).start()

    load.wait()
    wide = 512

    def spread(i, carry):
        at = pl.multiple_of(i * wide, wide)
        gh_ref[:, pl.ds(at, wide)] = lax.dot_general(
            inside[...], w_ref[pl.ds(at, wide), :], (((1,), (1,)), ((), ())), preferred_element_type=jnp.float32
        ).astype(jnp.bfloat16)
        return carry

    lax.fori_loop(0, w_ref.shape[0] // wide, spread, 0)
    for gap in range(1, groups):
        gather_copy(gap, True).wait_recv()

    big = rows // 2
    tile = min(256, big)
    low = s % 2
    sibling = flipped(s, 1)
    grads = every[...].reshape(groups * tok, cols)

    def product(at):
        return lax.dot_general(
            col_ref[:, pl.ds(at, tile)], grads, (((0,), (0,)), ((), ())), preferred_element_type=jnp.float32
        )

    def theirs(i, carry):
        at = pl.multiple_of(i * tile, tile)
        sends[0][pl.ds(at, tile), :] = product(pl.multiple_of((1 - low) * big + at, tile)).astype(jnp.bfloat16)
        return carry

    lax.fori_loop(0, big // tile, theirs, 0)

    def reduce_copy(step, h, peer):
        cut = slice(None) if h is None else pl.ds(h * (cols // 2), cols // 2)
        return pltpu.make_async_remote_copy(
            src_ref=sends[step].at[:, cut] if h is not None else sends[step],
            dst_ref=recvs[step].at[:, cut] if h is not None else recvs[step],
            send_sem=rsend.at[step, h or 0],
            recv_sem=rrecv.at[step, h or 0],
            device_id=(peer, z),
            device_id_type=mesh_id,
        )

    reduce_copy(0, None, sibling).start()

    def mine(i, carry):
        at = pl.multiple_of(i * tile, tile)
        acc[pl.ds(at, tile), :] = product(pl.multiple_of(low * big + at, tile))
        return carry

    lax.fori_loop(0, big // tile, mine, 0)
    reduce_copy(0, None, sibling).wait_recv()

    def fold(i, carry):
        at = pl.multiple_of(i * tile, tile)
        acc[pl.ds(at, tile), :] += recvs[0][pl.ds(at, tile), :].astype(jnp.float32)
        return carry

    lax.fori_loop(0, big // tile, fold, 0)
    orders = (list(range(1, bits)), list(range(bits - 1, 0, -1)))
    offsets = [[0], [0]]
    side = cols // 2
    for step in range(1, bits):
        size = rows >> (step + 1)
        for h in range(2):
            place = orders[h][step - 1]
            bit = s // (1 << place) % 2
            start = offsets[h][-1]
            away = pl.multiple_of(start + (1 - bit) * size, 16)
            sends[step][:, h * side : (h + 1) * side] = acc[
                pl.ds(away, size), h * side : (h + 1) * side
            ].astype(jnp.bfloat16)
            reduce_copy(step, h, flipped(s, 1 << place)).start()
            offsets[h].append(start + bit * size)
        for h in range(2):
            place = orders[h][step - 1]
            reduce_copy(step, h, flipped(s, 1 << place)).wait_recv()
            keep = pl.ds(pl.multiple_of(offsets[h][-1], 16), size)
            cut = slice(h * side, (h + 1) * side)
            acc[keep, cut] += recvs[step][:, cut].astype(jnp.float32)
    size = rows >> bits
    for h in range(2):
        at = offsets[h][-1]
        cut = slice(h * side, (h + 1) * side)
        wg_ref[pl.ds(pl.multiple_of(low * big + at, 16), size), cut] = acc[
            pl.ds(pl.multiple_of(at, 16), size), cut
        ].astype(jnp.bfloat16)

    def spread_copy(step, h, incoming):
        place = orders[h][step - 1]
        bit = s // (1 << place) % 2
        size = rows >> (step + 1)
        at = low * big + offsets[h][step - 1] + ((1 - bit) if incoming else bit) * size
        block = wg_ref.at[pl.ds(pl.multiple_of(at, 16), size), pl.ds(h * side, side)]
        return pltpu.make_async_remote_copy(
            src_ref=block,
            dst_ref=block,
            send_sem=asend.at[step, h],
            recv_sem=arecv.at[step, h],
            device_id=(flipped(s, 1 << place), z),
            device_id_type=mesh_id,
        )

    for step in range(bits - 1, 0, -1):
        for h in range(2):
            spread_copy(step, h, False).start()
        for h in range(2):
            spread_copy(step, h, True).wait_recv()

    def last_copy(incoming):
        block = wg_ref.at[pl.ds(pl.multiple_of(((1 - low) if incoming else low) * big, 16), big), :]
        return pltpu.make_async_remote_copy(
            src_ref=block,
            dst_ref=block,
            send_sem=asend.at[0, 0],
            recv_sem=arecv.at[0, 0],
            device_id=(sibling, z),
            device_id_type=mesh_id,
        )

    last_copy(False).start()
    last_copy(True).wait_recv()
    for offset in range(1, reach + 1):

        @pl.when(linear >= offset)
        def _():
            halo_copy(offset, False).wait_send()

    for gap in range(1, groups):
        gather_copy(gap, False).wait_send()
    reduce_copy(0, None, sibling).wait_send()
    for step in range(1, bits):
        for h in range(2):
            reduce_copy(step, h, flipped(s, 1 << orders[h][step - 1])).wait_send()
            spread_copy(step, h, False).wait_send()
    last_copy(False).wait_send()


def finish(back, own, weights, columns, reach):
    seqs = lax.axis_size("seq")
    groups = lax.axis_size("fsdp")
    tok, cols = own.shape
    rows = columns.shape[1]
    bits = seqs.bit_length() - 1
    vmem = pl.BlockSpec(memory_space=pltpu.VMEM)
    steps = [pltpu.VMEM((rows >> (k + 1), cols), jnp.bfloat16) for k in range(bits)]
    dma = pltpu.SemaphoreType.DMA
    return pl.pallas_call(
        functools.partial(finish_kernel, seqs, groups, reach),
        out_shape=[
            jax.ShapeDtypeStruct((tok, weights.shape[0]), jnp.bfloat16),
            jax.ShapeDtypeStruct((rows, cols), jnp.bfloat16),
        ],
        in_specs=[vmem, vmem, pl.BlockSpec(memory_space=pl.ANY), vmem],
        out_specs=[vmem] * 2,
        scratch_shapes=[
            pltpu.VMEM(weights.shape, jnp.bfloat16),
            dma(()),
            pltpu.VMEM((reach, tok, cols), jnp.bfloat16),
            pltpu.VMEM((groups, tok, cols), jnp.bfloat16),
            pltpu.VMEM((tok, cols), jnp.bfloat16),
            pltpu.VMEM((rows // 2, cols), jnp.float32),
            steps,
            steps,
            dma((reach,)),
            dma((reach,)),
            dma((groups - 1,)),
            dma((groups - 1,)),
            dma((bits, 2)),
            dma((bits, 2)),
            dma((bits, 2)),
            dma((bits, 2)),
        ],
        compiler_params=pltpu.CompilerParams(has_side_effects=True),
        name="finish",
    )(back, own, weights, columns)


def fused_kernel(
    seqs, groups, reach,
    hid_in, blk_in, sc_ref, q_in, g_in, ao, dq, gh, wgb,
    hid, blk, q_ref, g_ref, w_ref, win, back, ret, own, every, inside, hb, ht, part,
    ups, upr, dns, dnr, bias, lead_ref,
    lsem, zsend, zrecv, qsend, qrecv, csend, crecv, hsend, hrecv, ksend, krecv, bsend, brecv,
    esend, erecv, fsend, frecv, usend, urecv, dsend, drecv, wsend, wrecv, xsend, xrecv,
):
    s = lax.axis_index("seq")
    z = lax.axis_index("fsdp")
    linear = s * groups + z
    devices = seqs * groups
    tok, width = hid.shape
    rows, cols = blk.shape
    unit = rows // seqs
    bits = seqs.bit_length() - 1
    heads = cols // (2 * HEAD)
    duo = 2 * HEAD
    group = q_ref.shape[1] // HEAD // heads
    span = reach * tok
    last = groups - 1
    sibling = flipped(s, 1)
    peers = [m << 1 for m in range(1, seqs // 2)]
    nt = (((1,), (1,)), ((), ()))
    tn = (((0,), (0,)), ((), ()))
    mesh_id = pl.DeviceIdType.MESH

    def chunk(g):
        return pl.ds(g * duo, duo)

    def remote(src, dst, send, recv, to_s, to_z):
        return pltpu.make_async_remote_copy(
            src_ref=src, dst_ref=dst, send_sem=send, recv_sem=recv, device_id=(to_s, to_z), device_id_type=mesh_id
        )

    barrier = pltpu.get_barrier_semaphore()
    partners = [(None, flipped(s, m), z) for m in range(1, seqs)]
    partners += [(z < last, s, z + 1), (z > 0, s, z - 1)]
    for offset in range(1, reach + 1):
        up, down = linear + offset, linear - offset
        partners.append((up < devices, up // groups, up % groups))
        partners.append((down >= 0, down // groups, down % groups))

    def greet(to_s, to_z):
        pl.semaphore_signal(barrier, inc=1, device_id=(to_s, to_z), device_id_type=mesh_id)

    for present, to_s, to_z in partners:
        if present is None:
            greet(to_s, to_z)
        else:
            pl.when(present)(functools.partial(greet, to_s, to_z))

    mine = pl.ds(pl.multiple_of(s * unit, 16), unit)
    first = pltpu.make_async_copy(blk_in.at[mine, :], lead_ref, lsem.at[0])
    first.start()
    loads = [
        pltpu.make_async_copy(blk_in, blk, lsem.at[1]),
        pltpu.make_async_copy(hid_in, hid, lsem.at[2]),
        pltpu.make_async_copy(q_in, q_ref, lsem.at[3]),
        pltpu.make_async_copy(g_in, g_ref, lsem.at[4]),
    ]
    loads[1].start()

    def scale_block(i, source, at):
        to = pl.ds(pl.multiple_of(z * rows + i * QB, QB), QB)
        for j in range(cols // QB):
            block = source[pl.ds(at, QB), j * QB : (j + 1) * QB].astype(jnp.float32) * sc_ref[j, i]
            side = j // heads * HEAD
            w_ref[j % heads, to, side : side + HEAD] = block.astype(jnp.bfloat16)

    near = jnp.minimum(z, last - z)

    def shard_at(turn):
        step = turn // 2 + 1
        paired = z - step if turn % 2 == 0 else z + step
        far = turn - near + 1
        single = jnp.where(z > last - z, z - far, z + far)
        return jnp.where(turn < 2 * near, paired, single)

    shards = [shard_at(turn) for turn in range(groups - 1)]
    orders = (list(range(1, bits)), list(range(bits - 1, 0, -1)))

    def span_of(g, shard, owner, h=None):
        at = shard * rows + owner * unit + (0 if h is None else h * (unit // 2))
        return w_ref.at[g, pl.ds(pl.multiple_of(at, 16), unit if h is None else unit // 2), :]

    def kinds(g):
        return range(3 if g in WIDE else 1)

    def line_copy(shard, up, g, kind):
        if kind == 0:
            piece = span_of(g, shard, s)
        else:
            piece = span_of(g, shard, flipped(s, 1 << orders[kind - 1][0]), kind - 1)
        return remote(piece, piece, zsend.at[up, shard], zrecv.at[shard, g], s, z + 1 if up else z - 1)

    def cube_copy(turn, g, h, step, which, incoming):
        order = orders[h]
        bit = order[step]
        mask = 0
        for k in range(step):
            if which >> k & 1:
                mask |= 1 << order[k]
        piece = span_of(g, shards[turn], flipped(s, mask | (1 << bit) if incoming else mask), h)
        return remote(piece, piece, qsend.at[0], qrecv.at[turn, g, step], flipped(s, 1 << bit), z)

    def pair_copy(turn, g, m, incoming):
        piece = span_of(g, shards[turn], flipped(s, (m << 1) | 1 if incoming else m << 1))
        return remote(piece, piece, csend.at[0], crecv.at[turn, g], sibling, z)

    def hidden_copy(d, m):
        peer = flipped(s, m)
        return remote(
            hid.at[:, pl.ds(pl.multiple_of(d * rows + peer * unit, 128), unit)], hb.at[s, d],
            hsend.at[0], hrecv.at[d], peer, z,
        )

    def hidden_send(d):
        for m in range(1, seqs):
            hidden_copy(d, m).start()

    def hidden_wait(d):
        whole = hb.at[pl.ds(0, seqs - 1), d]
        remote(whole, whole, hsend.at[0], hrecv.at[d], s, z).wait_recv()

    def own_send(g):
        for kind in kinds(g):

            @pl.when(z < last)
            def _():
                line_copy(z, 1, g, kind).start()

            @pl.when(z > 0)
            def _():
                line_copy(z, 0, g, kind).start()

    def forward(turn, g):
        shard = shards[turn]
        whole = w_ref.at[g, pl.ds(0, unit * (2 if g in WIDE else 1)), :]
        remote(whole, whole, zsend.at[0, shard], zrecv.at[shard, g], s, z).wait_recv()
        for kind in kinds(g):

            @pl.when((shard < z) & (z < last))
            def _():
                line_copy(shard, 1, g, kind).start()

            @pl.when((shard > z) & (z > 0))
            def _():
                line_copy(shard, 0, g, kind).start()

    def cube_wait(turn, g, step):
        whole = w_ref.at[g, pl.ds(0, unit << step), :]
        remote(whole, whole, qsend.at[0], qrecv.at[turn, g, step], s, z).wait_recv()

    def cube_send(turn, g, step):
        for which in range(1 << step):
            for h in range(2):
                cube_copy(turn, g, h, step, which, False).start()

    def pair_send(turn, g):
        for m in range(seqs // 2):
            pair_copy(turn, g, m, False).start()

    def pair_wait(turn, g):
        whole = w_ref.at[g, pl.ds(0, unit * (seqs // 2)), :]
        remote(whole, whole, csend.at[0], crecv.at[turn, g], s, z).wait_recv()

    def begin(turn, g):
        if g not in WIDE:
            cube_send(turn, g, 0)
        else:
            cube_send(turn, g, 1)

    def cube_next(turn, g):
        cube_wait(turn, g, 0)
        cube_send(turn, g, 1)

    def pair_send_after(turn, g):
        cube_wait(turn, g, bits - 2)
        pair_send(turn, g)

    first.wait()
    loads[0].start()
    lead = unit // QB
    for i in range(lead):
        scale_block(s * lead + i, lead_ref, i * QB)
    pl.semaphore_wait(barrier, sum(1 if present is None else jnp.where(present, 1, 0) for present, _, _ in partners))

    own_send(0)
    loads[1].wait()
    hidden_send(0)
    loads[0].wait()

    def scale_rest(i, carry):
        place = (s * lead + lead + i) % (rows // QB)
        scale_block(place, blk, pl.multiple_of(place * QB, QB))
        return carry

    lax.fori_loop(0, rows // QB - lead, scale_rest, 0)
    loads[2].start()
    loads[3].start()
    row = lax.broadcasted_iota(jnp.int32, (tok, tok), 0)
    col = lax.broadcasted_iota(jnp.int32, (tok, tok), 1)
    bias[...] = jnp.where((col > row) & (linear < reach), NEG, 0.0)
    for offset in range(1, reach + 1):

        @pl.when(linear < offset)
        def _():
            win[(reach - offset) * tok : (reach - offset + 1) * tok, :] = jnp.zeros((tok, cols), jnp.bfloat16)

        @pl.when(linear + offset >= devices)
        def _():
            ret[offset - 1] = jnp.zeros((tok, cols), jnp.bfloat16)

    @pl.when(z == 0)
    def _():
        for g in range(heads):
            upr[g, 0] = jnp.zeros((unit, duo), jnp.bfloat16)

    @pl.when(z == last)
    def _():
        for g in range(heads):
            dnr[g, last] = jnp.zeros((unit, duo), jnp.bfloat16)

    deep = min(1024, width)

    def project_chunk(g):
        def step(i, total):
            at = pl.multiple_of(i * deep, deep)
            return total + jnp.dot(hid[:, pl.ds(at, deep)], w_ref[g, pl.ds(at, deep), :], preferred_element_type=jnp.float32)

        total = lax.fori_loop(0, width // deep, step, jnp.zeros((tok, duo), jnp.float32))
        win[span:, g * duo : (g + 1) * duo] = total.astype(jnp.bfloat16)
        for offset in range(1, reach + 1):

            @pl.when(linear + offset < devices)
            def _():
                halo_copy(g, offset, False).start()

    def halo_copy(g, offset, incoming):
        other = linear - offset if incoming else linear + offset
        return remote(
            win.at[pl.ds(span, tok), chunk(g)], win.at[pl.ds((reach - offset) * tok, tok), chunk(g)],
            ksend.at[offset - 1], krecv.at[g, offset - 1], other // groups, other % groups,
        )

    def back_copy(g, offset, incoming):
        other = linear + offset if incoming else linear - offset
        return remote(
            back.at[offset - 1, :, chunk(g)], ret.at[offset - 1, :, chunk(g)],
            bsend.at[offset - 1], brecv.at[g, offset - 1], other // groups, other % groups,
        )

    factor = 1.0 / float(HEAD) ** 0.5
    cat = lambda parts: jnp.concatenate(parts, axis=0)

    def attend_chunk(g):
        for offset in range(1, reach + 1):

            @pl.when(linear >= offset)
            def _():
                halo_copy(g, offset, True).wait_recv()

        keys = win[:, g * duo : g * duo + HEAD]
        values = win[:, g * duo + HEAD : (g + 1) * duo]
        cuts = [slice(h * HEAD, (h + 1) * HEAD) for h in range(g * group, (g + 1) * group)]
        q = cat([q_ref[:, cut] for cut in cuts])
        go = cat([g_ref[:, cut] for cut in cuts])
        upper = cat([col > row] * group)
        scores = lax.dot_general(q, keys, nt, preferred_element_type=jnp.float32)
        dprobs = lax.dot_general(go, values, nt, preferred_element_type=jnp.float32)

        def folded(x):
            return [jnp.where(upper, x[:, :tok], x[:, span:])] + [x[:, j * tok : (j + 1) * tok] for j in range(1, reach)]

        def unfolded(x):
            zero = jnp.zeros_like(x[0])
            parts = [jnp.where(upper, x[0], zero)] + x[1:] + [jnp.where(upper, zero, x[0])]
            return jnp.concatenate([part.astype(jnp.bfloat16) for part in parts], axis=1)

        masks = [cat([bias[...]] * group)] + [jnp.where(linear < reach - j, NEG, 0.0) for j in range(1, reach)]
        scores = [x * factor + mask for x, mask in zip(folded(scores), masks)]
        dprobs = folded(dprobs)
        top = jnp.max(functools.reduce(jnp.maximum, scores), axis=-1, keepdims=True)
        expd = [jnp.exp(x - top) for x in scores]
        scale = 1.0 / jnp.sum(functools.reduce(jnp.add, expd), axis=-1, keepdims=True)
        probs = [x * scale for x in expd]
        delta = jnp.sum(functools.reduce(jnp.add, [p * d for p, d in zip(probs, dprobs)]), axis=-1, keepdims=True)
        probs_b = unfolded(probs)
        dscores = unfolded([p * (d - delta) * factor for p, d in zip(probs, dprobs)])
        out = jnp.dot(probs_b, values, preferred_element_type=jnp.float32).astype(jnp.bfloat16)
        gq = jnp.dot(dscores, keys, preferred_element_type=jnp.float32).astype(jnp.bfloat16)
        for i, cut in enumerate(cuts):
            ao[:, cut] = out[i * tok : (i + 1) * tok]
            dq[:, cut] = gq[i * tok : (i + 1) * tok]
        dk = lax.dot_general(dscores, q, tn, preferred_element_type=jnp.float32)
        dv = lax.dot_general(probs_b, go, tn, preferred_element_type=jnp.float32)
        for side, value in ((0, dk), (HEAD, dv)):
            cut = slice(g * duo + side, g * duo + side + HEAD)
            for offset in range(1, reach + 1):
                back[offset - 1, :, cut] = value[(reach - offset) * tok : (reach - offset + 1) * tok].astype(jnp.bfloat16)
            own[:, cut] = value[span:]
        for offset in range(1, reach + 1):

            @pl.when(linear >= offset)
            def _():
                back_copy(g, offset, False).start()

    def cube_mask(h, step, which):
        return sum(1 << orders[h][k] for k in range(step) if which >> k & 1)

    def every_copy(g, h, step, which):
        block = every.at[flipped(s, cube_mask(h, step, which)), pl.ds(h * (tok // 2), tok // 2), chunk(g)]
        return remote(block, block, esend.at[0], erecv.at[g, step], flipped(s, 1 << orders[h][step]), z)

    def every_send(g, step):
        for which in range(1 << step):
            for h in range(2):
                every_copy(g, h, step, which).start()

    def every_pair(g, m, incoming):
        block = every.at[flipped(s, m | 1 if incoming else m), :, chunk(g)]
        return remote(block, block, fsend.at[0], frecv.at[g], sibling, z)

    def settle(g):
        for offset in range(1, reach + 1):

            @pl.when(linear + offset < devices)
            def _():
                back_copy(g, offset, True).wait_recv()

        cut = slice(g * duo, (g + 1) * duo)
        total = own[:, cut]
        seg = total
        for offset in range(1, reach + 1):
            piece = ret[offset - 1, :, cut].astype(jnp.float32)
            total = total + piece
            seg = seg + piece * jnp.where(z + offset < groups, 1.0, 0.0)
        every[s, :, cut] = total.astype(jnp.bfloat16)
        inside[:, cut] = seg.astype(jnp.bfloat16)
        every_send(g, 0)
        every_pair(g, 0, False).start()

    def widen(g):
        whole = every.at[0, :, chunk(g)]
        remote(whole, whole, esend.at[0], erecv.at[g, 0], s, z).wait_recv()
        every_send(g, 1)

    def share(g):
        whole = every.at[pl.ds(0, 2), :, chunk(g)]
        remote(whole, whole, esend.at[0], erecv.at[g, 1], s, z).wait_recv()
        for m in peers:
            every_pair(g, m, False).start()

    def up_copy(g, d):
        return remote(ups.at[g, d], upr.at[g, d], usend.at[d], urecv.at[g, d], s, z + 1)

    def down_copy(g, d):
        return remote(dns.at[g, d], dnr.at[g, d], dsend.at[d], drecv.at[g, d], s, z - 1)

    def hop(g, k):
        @pl.when(z == k)
        def _():
            for d in range(last, k, -1):
                value = part[g, d]
                if k > 0:
                    up_copy(g, d).wait_recv()
                    value = value + upr[g, d].astype(jnp.float32)
                ups[g, d] = value.astype(jnp.bfloat16)
                up_copy(g, d).start()

        @pl.when(z == last - k)
        def _():
            for d in range(last - k):
                value = part[g, d]
                if k > 0:
                    down_copy(g, d).wait_recv()
                    value = value + dnr[g, d].astype(jnp.float32)
                dns[g, d] = value.astype(jnp.bfloat16)
                down_copy(g, d).start()

    def product(g):
        whole = every.at[pl.ds(0, seqs // 2), :, chunk(g)]
        remote(whole, whole, fsend.at[0], frecv.at[g], s, z).wait_recv()
        grads = every[:, :, g * duo : (g + 1) * duo].reshape(seqs * tok, duo)

        def step(d, carry):
            part[g, d] = jnp.dot(
                ht[pl.ds(pl.multiple_of(d * unit, 128), unit), :], grads, preferred_element_type=jnp.float32
            )
            return carry

        lax.fori_loop(0, groups, step, 0)
        hop(g, 0)

    def grad_copy(g, h, step, which):
        at = flipped(s, cube_mask(h, step, which)) * unit + h * (unit // 2)
        block = wgb.at[g, pl.ds(pl.multiple_of(at, 16), unit // 2), :]
        return remote(block, block, wsend.at[0], wrecv.at[g, step], flipped(s, 1 << orders[h][step]), z)

    def grad_send(g, step):
        for which in range(1 << step):
            for h in range(2):
                grad_copy(g, h, step, which).start()

    def grad_pair(g, m, incoming):
        owner = flipped(s, m | 1 if incoming else m)
        block = wgb.at[g, pl.ds(pl.multiple_of(owner * unit, 128), unit), :]
        return remote(block, block, xsend.at[0], xrecv.at[g], sibling, z)

    def reduce(g):
        @pl.when(z > 0)
        def _():
            up_copy(g, z).wait_recv()

        @pl.when(z < last)
        def _():
            down_copy(g, z).wait_recv()

        total = part[g, z] + upr[g, z].astype(jnp.float32) + dnr[g, z].astype(jnp.float32)
        wgb[g, pl.ds(pl.multiple_of(s * unit, 128), unit), :] = total.astype(jnp.bfloat16)
        grad_send(g, 0)
        grad_pair(g, 0, False).start()

    def expand(g):
        whole = wgb.at[g, pl.ds(0, unit), :]
        remote(whole, whole, wsend.at[0], wrecv.at[g, 0], s, z).wait_recv()
        grad_send(g, 1)

    def relay(g):
        whole = wgb.at[g, pl.ds(0, 2 * unit), :]
        remote(whole, whole, wsend.at[0], wrecv.at[g, 1], s, z).wait_recv()
        for m in peers:
            grad_pair(g, m, False).start()

    def finish_chunk(g):
        whole = wgb.at[g, pl.ds(0, seqs // 2 * unit), :]
        remote(whole, whole, xsend.at[0], xrecv.at[g], s, z).wait_recv()

    def turn_hidden(d):
        hidden_wait(d)
        hb[s, d] = hid[:, pl.ds(pl.multiple_of(d * rows + s * unit, 128), unit)]
        for i in range(seqs):
            ht[d * unit : (d + 1) * unit, i * tok : (i + 1) * tok] = hb[i, d].T

    slices = 4
    span_cols = gh.shape[1] // slices
    tall = min(512, span_cols)

    def spread(i):
        def step(j, carry):
            at = pl.multiple_of(i * span_cols + j * tall, tall)
            total = jnp.zeros((tok, tall), jnp.float32)
            for g in range(heads):
                grads = inside[:, g * duo : (g + 1) * duo]
                total = total + lax.dot_general(grads, w_ref[g, pl.ds(at, tall), :], nt, preferred_element_type=jnp.float32)
            gh[:, pl.ds(at, tall)] = total.astype(jnp.bfloat16)
            return carry

        lax.fori_loop(0, span_cols // tall, step, 0)

    def drain(ref, sem):
        remote(ref, ref, sem, wrecv.at[0, 0], s, z).wait_send()

    def drain_weights():
        wide = len([g for g in range(heads) if g in WIDE])
        for shard in range(groups):
            moved = w_ref.at[0, pl.ds(0, unit * (heads + wide)), :]

            @pl.when((shard <= z) & (z < last))
            def _():
                drain(moved, zsend.at[1, shard])

            @pl.when((shard >= z) & (z > 0))
            def _():
                drain(moved, zsend.at[0, shard])

        turns = groups - 1
        plane = heads * (seqs // 2 - 1) - wide
        drain(w_ref.at[pl.ds(0, turns), pl.ds(0, unit * plane), :], qsend.at[0])
        drain(w_ref.at[pl.ds(0, turns), pl.ds(0, unit * heads * (seqs // 2)), :], csend.at[0])

    def drain_tokens():
        drain(hb.at[pl.ds(0, seqs - 1)], hsend.at[0])
        for offset in range(1, reach + 1):

            @pl.when(linear + offset < devices)
            def _():
                drain(ret.at[offset - 1], ksend.at[offset - 1])

            @pl.when(linear >= offset)
            def _():
                drain(ret.at[offset - 1], bsend.at[offset - 1])

        drain(every.at[pl.ds(0, len(peers))], esend.at[0])
        drain(every.at[pl.ds(0, seqs // 2)], fsend.at[0])

    works = [own_send, forward, begin, cube_next, pair_send_after, pair_wait, project_chunk, attend_chunk, settle, widen, share]
    works += [product, hop, reduce, expand, relay, finish_chunk, spread, hidden_send, turn_hidden]
    fetched = False
    for place, *places in ORDER:
        if works[place] is attend_chunk and not fetched:
            loads[2].wait()
            loads[3].wait()
            fetched = True
        works[place](*places)
    drain_weights()
    drain_tokens()
    drain(wgb.at[:, pl.ds(0, len(peers) * unit), :], wsend.at[0])
    drain(wgb.at[:, pl.ds(0, seqs // 2 * unit), :], xsend.at[0])
    for d in range(groups):

        @pl.when(d > z)
        def _():
            drain(ups.at[:, d], usend.at[d])

        @pl.when(d < z)
        def _():
            drain(dns.at[:, d], dsend.at[d])


def fused(hidden, kv_blocks, kv_scale, queries, grad_out, reach):
    seqs = lax.axis_size("seq")
    groups = lax.axis_size("fsdp")
    tok, depth = hidden.shape
    rows, cols = kv_blocks.shape
    width = queries.shape[1]
    unit = rows // seqs
    heads = cols // (2 * HEAD)
    duo = 2 * HEAD
    count = (reach + 1) * tok
    bits = seqs.bit_length() - 1
    any_space = pl.BlockSpec(memory_space=pl.ANY)
    dma = pltpu.SemaphoreType.DMA
    b16 = lambda *shape: pltpu.VMEM(shape, jnp.bfloat16)
    f32 = lambda *shape: pltpu.VMEM(shape, jnp.float32)
    return pl.pallas_call(
        functools.partial(fused_kernel, seqs, groups, reach),
        out_shape=[b16(tok, width), b16(tok, width), b16(tok, depth), b16(heads, rows, duo)],
        in_specs=[any_space, any_space, pl.BlockSpec(memory_space=pltpu.SMEM), any_space, any_space],
        out_specs=[pl.BlockSpec(memory_space=pltpu.VMEM)] * 4,
        scratch_shapes=[
            b16(tok, depth), b16(rows, cols), b16(tok, width), b16(tok, width),
            b16(heads, depth, duo), b16(count, cols),
            b16(reach, tok, cols), b16(reach, tok, cols), f32(tok, cols), b16(seqs, tok, cols), b16(tok, cols),
            b16(seqs, groups, tok, unit), b16(groups * unit, seqs * tok), f32(heads, groups, unit, duo),
            b16(heads, groups, unit, duo), b16(heads, groups, unit, duo), b16(heads, groups, unit, duo), b16(heads, groups, unit, duo),
            f32(tok, tok), b16(unit, cols),
            dma((5,)), dma((2, groups)), dma((groups, heads)),
            dma((1,)), dma((groups - 1, heads, bits - 1)), dma((1,)), dma((groups - 1, heads)), dma((1,)), dma((groups,)),
            dma((reach,)), dma((heads, reach)), dma((reach,)), dma((heads, reach)),
            dma((1,)), dma((heads, 2)), dma((1,)), dma((heads,)),
            dma((groups,)), dma((heads, groups)), dma((groups,)), dma((heads, groups)),
            dma((1,)), dma((heads, 2)), dma((1,)), dma((heads,)),
        ],
        compiler_params=pltpu.CompilerParams(collective_id=0, has_side_effects=True, vmem_limit_bytes=VMEM_LIMIT),
        name="fused",
    )(hidden, kv_blocks, kv_scale.T, queries, grad_out)


def write_kernel(ao, dq, gh, wgb, ao_out, dq_out, gh_out, wg_out, wide, osem):
    parts, size, cols = wide.shape
    heads = wgb.shape[0]
    triples = ((ao, ao_out), (dq, dq_out), (gh, gh_out))
    stores = [pltpu.make_async_copy(src, dst, osem.at[parts + k]) for k, (src, dst) in enumerate(triples)]
    for copy in stores:
        copy.start()
    for p in range(parts):
        for g in range(heads):
            block = wgb[g, p * size : (p + 1) * size, :].astype(jnp.float32)
            wide[p, :, g * HEAD : (g + 1) * HEAD] = block[:, :HEAD]
            wide[p, :, (heads + g) * HEAD : (heads + g + 1) * HEAD] = block[:, HEAD:]
        store = pltpu.make_async_copy(wide.at[p], wg_out.at[pl.ds(p * size, size), :], osem.at[p])
        store.start()
        stores.append(store)
    for copy in stores:
        copy.wait()


def write(ao, dq, gh, wgb):
    parts = 8
    heads, rows, duo = wgb.shape
    any_space = pl.BlockSpec(memory_space=pl.ANY)
    return pl.pallas_call(
        write_kernel,
        out_shape=[jax.ShapeDtypeStruct(x.shape, x.dtype) for x in (ao, dq, gh)]
        + [jax.ShapeDtypeStruct((rows, heads * duo), jnp.float32)],
        in_specs=[pl.BlockSpec(memory_space=pltpu.VMEM)] * 4,
        out_specs=[any_space] * 4,
        scratch_shapes=[pltpu.VMEM((parts, rows // parts, heads * duo), jnp.float32), pltpu.SemaphoreType.DMA((parts + 3,))],
        compiler_params=pltpu.CompilerParams(vmem_limit_bytes=12 << 20),
        name="write",
    )(ao, dq, gh, wgb)


def body(hidden, kv_blocks, kv_scale, queries, grad_out):
    tok = hidden.shape[0]
    groups = lax.axis_size("fsdp")
    reach = groups // 2
    unit = kv_blocks.shape[0] // lax.axis_size("seq")
    heads = kv_blocks.shape[1] // (2 * HEAD)
    if unit % QB == 0 and (heads, groups, lax.axis_size("seq")) == PLANNED:
        outs = fused(hidden, kv_blocks, kv_scale, queries, grad_out, reach)
        return tuple(write(*outs))
    weights, kv, columns = project(hidden, kv_blocks, kv_scale)
    pieces = []
    for offset in range(reach, 0, -1):
        pieces.append(shifted(kv, ("seq", "fsdp"), offset))
    window = jnp.concatenate(pieces + [kv], axis=0)
    columns = columns.reshape(groups * tok, columns.shape[2])
    attn_out, grad_queries, dwin = attend(queries, window, grad_out, reach)
    back = dwin[: reach * tok].astype(jnp.bfloat16)
    own = dwin[reach * tok :]
    grad_hidden, weight_grad = finish(back, own, weights, columns, reach)
    return (attn_out, grad_queries, grad_hidden, weight_grad.astype(jnp.float32))


def solution(mesh):
    return jax.shard_map(
        body,
        mesh=mesh,
        in_specs=(
            P(("seq", "fsdp"), None),
            P("fsdp", None),
            P("fsdp", None),
            P(("seq", "fsdp"), None),
            P(("seq", "fsdp"), None),
        ),
        out_specs=(
            P(("seq", "fsdp"), None),
            P(("seq", "fsdp"), None),
            P(("seq", "fsdp"), None),
            P("fsdp", None),
        ),
        check_vma=False,
    )
```

```python
import functools

import jax
import jax.numpy as jnp
from jax import lax
from jax.experimental import pallas as pl
from jax.experimental.pallas import tpu as pltpu
from jax.sharding import PartitionSpec as P

HEADS = 32
KV_HEADS = 4
HEAD = 128
QB = 128


NEG = -1e30
PLANNED = (4, 4, 8)
(SEND, FORWARD, BEGIN, CUBE, PAIR, LAND, PROJECT, ATTEND, SETTLE, WIDEN, SHARE) = range(11)
(PRODUCT, HOP, REDUCE, EXPAND, RELAY, FINISH, SPREAD, HIDDEN, TURN) = range(11, 20)
VMEM_LIMIT = 50 << 20
SPLIT = 2
WIDE = (2,)
ORDER = (
    (SEND, 3), (SEND, 1), (FORWARD, 0, 0), (BEGIN, 0, 0), (HIDDEN, 1), (FORWARD, 0, 3), (FORWARD, 1, 0),
    (BEGIN, 0, 3), (BEGIN, 1, 0), (FORWARD, 1, 3), (CUBE, 0, 0), (FORWARD, 2, 0), (BEGIN, 2, 0), (FORWARD, 0, 1),
    (CUBE, 1, 0), (BEGIN, 0, 1), (FORWARD, 1, 1), (SEND, 2), (BEGIN, 1, 1), (CUBE, 2, 0), (PAIR, 0, 0), (CUBE, 0, 3),
    (BEGIN, 1, 3), (FORWARD, 2, 1), (PAIR, 1, 0), (BEGIN, 2, 1), (LAND, 1, 0), (LAND, 0, 0), (CUBE, 1, 1),
    (FORWARD, 2, 3), (FORWARD, 0, 2), (BEGIN, 0, 2), (CUBE, 0, 1), (TURN, 0), (PAIR, 2, 0), (FORWARD, 1, 2),
    (BEGIN, 2, 3), (LAND, 2, 0), (PROJECT, 0), (CUBE, 2, 1), (CUBE, 1, 3), (PAIR, 0, 3), (FORWARD, 2, 2), (ATTEND, 0),
    (CUBE, 2, 3), (PAIR, 0, 2), (PAIR, 0, 1), (BEGIN, 1, 2), (TURN, 1), (PAIR, 2, 1), (PAIR, 1, 1), (LAND, 0, 1),
    (LAND, 2, 1), (PAIR, 1, 3), (LAND, 1, 1), (LAND, 0, 3), (BEGIN, 2, 2), (PROJECT, 1), (SETTLE, 0), (LAND, 1, 3),
    (PAIR, 2, 3), (LAND, 2, 3), (PAIR, 1, 2), (PROJECT, 3), (LAND, 1, 2), (LAND, 0, 2), (HIDDEN, 2), (PAIR, 2, 2),
    (WIDEN, 0), (HIDDEN, 3), (LAND, 2, 2), (PROJECT, 2), (ATTEND, 1), (TURN, 2), (ATTEND, 3), (ATTEND, 2), (SHARE, 0),
    (TURN, 3), (SETTLE, 1), (PRODUCT, 0), (WIDEN, 1), (HOP, 0, 1), (SHARE, 1), (SETTLE, 3), (HOP, 0, 2), (PRODUCT, 1),
    (SETTLE, 2), (WIDEN, 3), (WIDEN, 2), (HOP, 1, 1), (SHARE, 3), (SPREAD, 0), (REDUCE, 0), (PRODUCT, 3), (SHARE, 2),
    (HOP, 1, 2), (HOP, 3, 1), (REDUCE, 1), (EXPAND, 0), (HOP, 3, 2), (PRODUCT, 2), (REDUCE, 3), (EXPAND, 1),
    (HOP, 2, 1), (HOP, 2, 2), (EXPAND, 3), (SPREAD, 3), (RELAY, 1), (REDUCE, 2), (SPREAD, 2), (RELAY, 3), (RELAY, 0),
    (FINISH, 1), (EXPAND, 2), (FINISH, 3), (SPREAD, 1), (RELAY, 2), (FINISH, 0), (FINISH, 2),
)


def shifted(block, axis, distance):
    devices = range(lax.axis_size(axis))
    route = [(i - distance, i) for i in devices if i - distance in devices]
    return lax.ppermute(block, axis, route)


def attend_kernel(reach, q_ref, g_ref, k_ref, v_ref, out_ref, dq_ref, dk_ref, dv_ref):
    tok = q_ref.shape[0]
    group = q_ref.shape[1] // HEAD
    count = k_ref.shape[0]
    span = reach * tok
    factor = 1.0 / float(HEAD) ** 0.5
    base = (lax.axis_index("seq") * lax.axis_size("fsdp") + lax.axis_index("fsdp")) * tok
    row = lax.broadcasted_iota(jnp.int32, (tok, count), 0)
    col = lax.broadcasted_iota(jnp.int32, (tok, count), 1)
    allowed = (col > row) & (col <= row + span) & (col >= span - base)
    keys = k_ref[...]
    values = v_ref[...]
    nt = (((1,), (1,)), ((), ()))
    tn = (((0,), (0,)), ((), ()))
    ps, ds, qs, gs = [], [], [], []
    for h in range(group):
        cut = slice(h * HEAD, (h + 1) * HEAD)
        q = q_ref[:, cut]
        g = g_ref[:, cut]
        scores = lax.dot_general(q, keys, nt, preferred_element_type=jnp.float32) * factor
        scores = jnp.where(allowed, scores, NEG)
        expd = jnp.exp(scores - jnp.max(scores, axis=-1, keepdims=True))
        probs = expd * (1.0 / jnp.sum(expd, axis=-1, keepdims=True))
        probs_b = probs.astype(jnp.bfloat16)
        out_ref[:, cut] = jnp.dot(probs_b, values, preferred_element_type=jnp.float32).astype(jnp.bfloat16)
        dprobs = lax.dot_general(g, values, nt, preferred_element_type=jnp.float32)
        delta = jnp.sum(probs * dprobs, axis=-1, keepdims=True)
        dscores = (probs * (dprobs - delta) * factor).astype(jnp.bfloat16)
        dq_ref[:, cut] = jnp.dot(dscores, keys, preferred_element_type=jnp.float32).astype(jnp.bfloat16)
        ps.append(probs_b)
        ds.append(dscores)
        qs.append(q)
        gs.append(g)
    cat = lambda parts: jnp.concatenate(parts, axis=0)
    dk_ref[...] = lax.dot_general(cat(ds), cat(qs), tn, preferred_element_type=jnp.float32)
    dv_ref[...] = lax.dot_general(cat(ps), cat(gs), tn, preferred_element_type=jnp.float32)


def attend(queries, window, grad_out, reach):
    tok, width = queries.shape
    count = window.shape[0]
    heads = window.shape[1] // (2 * HEAD)
    wide = pl.BlockSpec((tok, width // heads), lambda i: (0, i))
    key = pl.BlockSpec((count, HEAD), lambda i: (0, i))
    value = pl.BlockSpec((count, HEAD), lambda i: (0, i + heads))
    out, dq, dk, dv = pl.pallas_call(
        functools.partial(attend_kernel, reach),
        grid=(heads,),
        in_specs=[wide, wide, key, value],
        out_specs=[wide, wide, key, key],
        out_shape=[
            jax.ShapeDtypeStruct((tok, width), jnp.bfloat16),
            jax.ShapeDtypeStruct((tok, width), jnp.bfloat16),
            jax.ShapeDtypeStruct((count, heads * HEAD), jnp.float32),
            jax.ShapeDtypeStruct((count, heads * HEAD), jnp.float32),
        ],
        cost_estimate=pl.CostEstimate(flops=12 * tok * width * count, bytes_accessed=8 * tok * width, transcendentals=0),
        name="attend",
    )(queries, grad_out, window, window)
    return out, dq, jnp.concatenate([dk, dv], axis=1)


def flipped(index, mask):
    for place in range(mask.bit_length()):
        if mask >> place & 1:
            index = index + (1 << place) * (1 - 2 * (index // (1 << place) % 2))
    return index


def orders_of(bits):
    return (list(range(1, bits)) + [0], list(range(bits - 1, 0, -1)) + [0])


def project_kernel(seqs, groups, hid_ref, blk_ref, sc_ref, out_ref, kv_ref, col_ref, w_ref, acc, zsend, zrecv, qsend, qrecv, csend, crecv, wsem):
    s = lax.axis_index("seq")
    z = lax.axis_index("fsdp")
    rows = blk_ref.shape[0]
    unit = rows // seqs
    half = unit // 2
    bits = seqs.bit_length() - 1
    chunk = min(512, rows)

    def scale_block(i, carry):
        at = pl.multiple_of(i * QB, QB)
        block = blk_ref[pl.ds(at, QB), :].astype(jnp.float32) * sc_ref[pl.ds(i, 1), :]
        w_ref[pl.ds(pl.multiple_of(z * rows + at, QB), QB), :] = block.astype(jnp.bfloat16)
        return carry

    lax.fori_loop(0, rows // QB, scale_block, 0)

    def line_copy(shard, up):
        piece = w_ref.at[pl.ds(pl.multiple_of(shard * rows + s * unit, 16), unit), :]
        return pltpu.make_async_remote_copy(
            src_ref=piece,
            dst_ref=piece,
            send_sem=zsend.at[up, shard],
            recv_sem=zrecv.at[shard],
            device_id=(s, z + 1 if up else z - 1),
            device_id_type=pl.DeviceIdType.MESH,
        )

    def cube_copy(turn, shard, order, step, which, incoming):
        bit = order[step]
        mask = 0
        for k in range(step):
            if which >> k & 1:
                mask |= 1 << order[k]
        h = 0 if order is orders[0] else 1
        owner = flipped(s, mask | (1 << bit) if incoming else mask)
        piece = w_ref.at[pl.ds(pl.multiple_of(shard * rows + owner * unit + h * half, 16), half), :]
        slot = (1 << step) - 1 + which
        return pltpu.make_async_remote_copy(
            src_ref=piece,
            dst_ref=piece,
            send_sem=qsend.at[turn, h, slot],
            recv_sem=qrecv.at[turn, h, slot],
            device_id=(flipped(s, 1 << bit), z),
            device_id_type=pl.DeviceIdType.MESH,
        )

    orders = orders_of(bits)
    near = jnp.minimum(z, groups - 1 - z)

    def shard_at(turn):
        step = turn // 2 + 1
        paired = z - step if turn % 2 == 0 else z + step
        far = turn - near + 1
        single = jnp.where(z > groups - 1 - z, z - far, z + far)
        return jnp.where(turn < 2 * near, paired, single)

    shards = [shard_at(turn) for turn in range(groups - 1)]

    @pl.when(z < groups - 1)
    def _():
        line_copy(z, 1).start()

    @pl.when(z > 0)
    def _():
        line_copy(z, 0).start()

    def column_copy(gap, incoming):
        other = (z - gap + groups) % groups if incoming else (z + gap) % groups
        part = pl.multiple_of(other * rows, 128)
        return pltpu.make_async_remote_copy(
            src_ref=hid_ref.at[:, pl.ds(part, rows)],
            dst_ref=col_ref.at[other if incoming else z],
            send_sem=csend.at[gap - 1],
            recv_sem=crecv.at[gap - 1],
            device_id=(s, other),
            device_id_type=pl.DeviceIdType.MESH,
        )

    acc[...] = jnp.zeros_like(acc)

    def store_copy(turn, shard):
        part = pl.ds(pl.multiple_of(shard * rows, 16), rows)
        return pltpu.make_async_copy(w_ref.at[part, :], out_ref.at[part, :], wsem.at[turn])

    def multiply(shard):
        def part(i, carry):
            at = pl.multiple_of(shard * rows + i * chunk, 128)
            acc[...] += jnp.dot(
                hid_ref[:, pl.ds(at, chunk)], w_ref[pl.ds(at, chunk), :], preferred_element_type=jnp.float32
            )
            return carry

        lax.fori_loop(0, rows // chunk, part, 0)

    multiply(z)
    store_copy(groups - 1, z).start()
    col_ref[z] = hid_ref[:, pl.ds(pl.multiple_of(z * rows, 128), rows)]
    for tick in range(groups - 1 + bits):
        for stage in range(bits, -1, -1):
            turn = tick - stage
            if turn < 0 or turn >= groups - 1:
                continue
            shard = shards[turn]
            if stage == 0:
                line_copy(shard, 0).wait_recv()

                @pl.when((shard < z) & (z < groups - 1))
                def _():
                    line_copy(shard, 1).start()

                @pl.when((shard > z) & (z > 0))
                def _():
                    line_copy(shard, 0).start()
            else:
                for order in orders:
                    for which in range(1 << (stage - 1)):
                        cube_copy(turn, shard, order, stage - 1, which, True).wait_recv()
            if stage < bits:
                for order in orders:
                    for which in range(1 << stage):
                        cube_copy(turn, shard, order, stage, which, False).start()
            else:
                multiply(shard)
                store_copy(turn, shard).start()
        if tick == groups - 2:
            for gap in range(1, groups):
                column_copy(gap, False).start()
    kv_ref[...] = acc[...].astype(jnp.bfloat16)
    for turn in range(groups - 1):
        store_copy(turn, shards[turn]).wait()
    store_copy(groups - 1, z).wait()
    for gap in range(1, groups):
        column_copy(gap, True).wait_recv()
        column_copy(gap, False).wait_send()
    for shard in range(groups):

        @pl.when((shard <= z) & (z < groups - 1))
        def _():
            line_copy(shard, 1).wait_send()

        @pl.when((shard >= z) & (z > 0))
        def _():
            line_copy(shard, 0).wait_send()

    for turn in range(groups - 1):
        for order in orders:
            for stage in range(bits):
                for which in range(1 << stage):
                    cube_copy(turn, shards[turn], order, stage, which, False).wait_send()


def project(hidden, kv_blocks, kv_scale):
    seqs = lax.axis_size("seq")
    groups = lax.axis_size("fsdp")
    tok, width = hidden.shape
    cols = kv_blocks.shape[1]
    spread = jnp.repeat(kv_scale, QB, axis=1)
    vmem = pl.BlockSpec(memory_space=pltpu.VMEM)
    return pl.pallas_call(
        functools.partial(project_kernel, seqs, groups),
        out_shape=[
            jax.ShapeDtypeStruct((width, cols), jnp.bfloat16),
            jax.ShapeDtypeStruct((tok, cols), jnp.bfloat16),
            jax.ShapeDtypeStruct((groups, tok, kv_blocks.shape[0]), jnp.bfloat16),
        ],
        in_specs=[vmem] * 3,
        out_specs=[pl.BlockSpec(memory_space=pl.ANY), vmem, vmem],
        scratch_shapes=[
            pltpu.VMEM((width, cols), jnp.bfloat16),
            pltpu.VMEM((tok, cols), jnp.float32),
            pltpu.SemaphoreType.DMA((2, groups)),
            pltpu.SemaphoreType.DMA((groups,)),
            pltpu.SemaphoreType.DMA((groups - 1, 2, seqs - 1)),
            pltpu.SemaphoreType.DMA((groups - 1, 2, seqs - 1)),
            pltpu.SemaphoreType.DMA((groups - 1,)),
            pltpu.SemaphoreType.DMA((groups - 1,)),
            pltpu.SemaphoreType.DMA((groups,)),
        ],
        compiler_params=pltpu.CompilerParams(has_side_effects=True),
        name="project",
    )(hidden, kv_blocks, spread)


def finish_kernel(
    seqs, groups, reach, back_ref, own_ref, in_ref, col_ref, gh_ref, wg_ref,
    w_ref, wsem, ret, every, inside, acc, sends, recvs, hsend, hrecv, gsend, grecv, rsend, rrecv, asend, arecv,
):
    s = lax.axis_index("seq")
    z = lax.axis_index("fsdp")
    linear = s * groups + z
    devices = seqs * groups
    tok, cols = own_ref.shape
    rows = col_ref.shape[1]
    bits = seqs.bit_length() - 1
    mesh_id = pl.DeviceIdType.MESH
    load = pltpu.make_async_copy(in_ref, w_ref, wsem)
    load.start()

    def halo_copy(offset, incoming):
        other = linear + offset if incoming else linear - offset
        return pltpu.make_async_remote_copy(
            src_ref=back_ref.at[pl.ds((reach - offset) * tok, tok), :],
            dst_ref=ret.at[offset - 1],
            send_sem=hsend.at[offset - 1],
            recv_sem=hrecv.at[offset - 1],
            device_id=(other // groups, other % groups),
            device_id_type=mesh_id,
        )

    for offset in range(1, reach + 1):

        @pl.when(linear >= offset)
        def _():
            halo_copy(offset, False).start()

    for offset in range(1, reach + 1):

        @pl.when(linear + offset < devices)
        def _():
            halo_copy(offset, True).wait_recv()

        @pl.when(linear + offset >= devices)
        def _():
            ret[offset - 1] = jnp.zeros((tok, cols), jnp.bfloat16)

    total = own_ref[...]
    seg = total
    for offset in range(1, reach + 1):
        piece = ret[offset - 1].astype(jnp.float32)
        total = total + piece
        seg = seg + piece * jnp.where(z + offset < groups, 1.0, 0.0)
    every[z] = total.astype(jnp.bfloat16)
    inside[...] = seg.astype(jnp.bfloat16)

    def gather_copy(gap, incoming):
        other = (z - gap + groups) % groups if incoming else (z + gap) % groups
        block = every.at[other if incoming else z]
        return pltpu.make_async_remote_copy(
            src_ref=block,
            dst_ref=block,
            send_sem=gsend.at[gap - 1],
            recv_sem=grecv.at[gap - 1],
            device_id=(s, other),
            device_id_type=mesh_id,
        )

    for gap in range(1, groups):
        gather_copy(gap, False).start()

    load.wait()
    wide = 512

    def spread(i, carry):
        at = pl.multiple_of(i * wide, wide)
        gh_ref[:, pl.ds(at, wide)] = lax.dot_general(
            inside[...], w_ref[pl.ds(at, wide), :], (((1,), (1,)), ((), ())), preferred_element_type=jnp.float32
        ).astype(jnp.bfloat16)
        return carry

    lax.fori_loop(0, w_ref.shape[0] // wide, spread, 0)
    for gap in range(1, groups):
        gather_copy(gap, True).wait_recv()

    big = rows // 2
    tile = min(256, big)
    low = s % 2
    sibling = flipped(s, 1)
    grads = every[...].reshape(groups * tok, cols)

    def product(at):
        return lax.dot_general(
            col_ref[:, pl.ds(at, tile)], grads, (((0,), (0,)), ((), ())), preferred_element_type=jnp.float32
        )

    def theirs(i, carry):
        at = pl.multiple_of(i * tile, tile)
        sends[0][pl.ds(at, tile), :] = product(pl.multiple_of((1 - low) * big + at, tile)).astype(jnp.bfloat16)
        return carry

    lax.fori_loop(0, big // tile, theirs, 0)

    def reduce_copy(step, h, peer):
        cut = slice(None) if h is None else pl.ds(h * (cols // 2), cols // 2)
        return pltpu.make_async_remote_copy(
            src_ref=sends[step].at[:, cut] if h is not None else sends[step],
            dst_ref=recvs[step].at[:, cut] if h is not None else recvs[step],
            send_sem=rsend.at[step, h or 0],
            recv_sem=rrecv.at[step, h or 0],
            device_id=(peer, z),
            device_id_type=mesh_id,
        )

    reduce_copy(0, None, sibling).start()

    def mine(i, carry):
        at = pl.multiple_of(i * tile, tile)
        acc[pl.ds(at, tile), :] = product(pl.multiple_of(low * big + at, tile))
        return carry

    lax.fori_loop(0, big // tile, mine, 0)
    reduce_copy(0, None, sibling).wait_recv()

    def fold(i, carry):
        at = pl.multiple_of(i * tile, tile)
        acc[pl.ds(at, tile), :] += recvs[0][pl.ds(at, tile), :].astype(jnp.float32)
        return carry

    lax.fori_loop(0, big // tile, fold, 0)
    orders = (list(range(1, bits)), list(range(bits - 1, 0, -1)))
    offsets = [[0], [0]]
    side = cols // 2
    for step in range(1, bits):
        size = rows >> (step + 1)
        for h in range(2):
            place = orders[h][step - 1]
            bit = s // (1 << place) % 2
            start = offsets[h][-1]
            away = pl.multiple_of(start + (1 - bit) * size, 16)
            sends[step][:, h * side : (h + 1) * side] = acc[
                pl.ds(away, size), h * side : (h + 1) * side
            ].astype(jnp.bfloat16)
            reduce_copy(step, h, flipped(s, 1 << place)).start()
            offsets[h].append(start + bit * size)
        for h in range(2):
            place = orders[h][step - 1]
            reduce_copy(step, h, flipped(s, 1 << place)).wait_recv()
            keep = pl.ds(pl.multiple_of(offsets[h][-1], 16), size)
            cut = slice(h * side, (h + 1) * side)
            acc[keep, cut] += recvs[step][:, cut].astype(jnp.float32)
    size = rows >> bits
    for h in range(2):
        at = offsets[h][-1]
        cut = slice(h * side, (h + 1) * side)
        wg_ref[pl.ds(pl.multiple_of(low * big + at, 16), size), cut] = acc[
            pl.ds(pl.multiple_of(at, 16), size), cut
        ].astype(jnp.bfloat16)

    def spread_copy(step, h, incoming):
        place = orders[h][step - 1]
        bit = s // (1 << place) % 2
        size = rows >> (step + 1)
        at = low * big + offsets[h][step - 1] + ((1 - bit) if incoming else bit) * size
        block = wg_ref.at[pl.ds(pl.multiple_of(at, 16), size), pl.ds(h * side, side)]
        return pltpu.make_async_remote_copy(
            src_ref=block,
            dst_ref=block,
            send_sem=asend.at[step, h],
            recv_sem=arecv.at[step, h],
            device_id=(flipped(s, 1 << place), z),
            device_id_type=mesh_id,
        )

    for step in range(bits - 1, 0, -1):
        for h in range(2):
            spread_copy(step, h, False).start()
        for h in range(2):
            spread_copy(step, h, True).wait_recv()

    def last_copy(incoming):
        block = wg_ref.at[pl.ds(pl.multiple_of(((1 - low) if incoming else low) * big, 16), big), :]
        return pltpu.make_async_remote_copy(
            src_ref=block,
            dst_ref=block,
            send_sem=asend.at[0, 0],
            recv_sem=arecv.at[0, 0],
            device_id=(sibling, z),
            device_id_type=mesh_id,
        )

    last_copy(False).start()
    last_copy(True).wait_recv()
    for offset in range(1, reach + 1):

        @pl.when(linear >= offset)
        def _():
            halo_copy(offset, False).wait_send()

    for gap in range(1, groups):
        gather_copy(gap, False).wait_send()
    reduce_copy(0, None, sibling).wait_send()
    for step in range(1, bits):
        for h in range(2):
            reduce_copy(step, h, flipped(s, 1 << orders[h][step - 1])).wait_send()
            spread_copy(step, h, False).wait_send()
    last_copy(False).wait_send()


def finish(back, own, weights, columns, reach):
    seqs = lax.axis_size("seq")
    groups = lax.axis_size("fsdp")
    tok, cols = own.shape
    rows = columns.shape[1]
    bits = seqs.bit_length() - 1
    vmem = pl.BlockSpec(memory_space=pltpu.VMEM)
    steps = [pltpu.VMEM((rows >> (k + 1), cols), jnp.bfloat16) for k in range(bits)]
    dma = pltpu.SemaphoreType.DMA
    return pl.pallas_call(
        functools.partial(finish_kernel, seqs, groups, reach),
        out_shape=[
            jax.ShapeDtypeStruct((tok, weights.shape[0]), jnp.bfloat16),
            jax.ShapeDtypeStruct((rows, cols), jnp.bfloat16),
        ],
        in_specs=[vmem, vmem, pl.BlockSpec(memory_space=pl.ANY), vmem],
        out_specs=[vmem] * 2,
        scratch_shapes=[
            pltpu.VMEM(weights.shape, jnp.bfloat16),
            dma(()),
            pltpu.VMEM((reach, tok, cols), jnp.bfloat16),
            pltpu.VMEM((groups, tok, cols), jnp.bfloat16),
            pltpu.VMEM((tok, cols), jnp.bfloat16),
            pltpu.VMEM((rows // 2, cols), jnp.float32),
            steps,
            steps,
            dma((reach,)),
            dma((reach,)),
            dma((groups - 1,)),
            dma((groups - 1,)),
            dma((bits, 2)),
            dma((bits, 2)),
            dma((bits, 2)),
            dma((bits, 2)),
        ],
        compiler_params=pltpu.CompilerParams(has_side_effects=True),
        name="finish",
    )(back, own, weights, columns)


def fused_kernel(
    seqs, groups, reach,
    hid_in, blk_in, sc_ref, q_in, g_in, ao, dq, gh, wgb,
    hid, blk, q_ref, g_ref, w_ref, win, back, ret, own, every, inside, hb, ht, part,
    ups, upr, dns, dnr, bias, lead_ref,
    lsem, zsend, zrecv, qsend, qrecv, csend, crecv, hsend, hrecv, ksend, krecv, bsend, brecv,
    esend, erecv, fsend, frecv, usend, urecv, dsend, drecv, wsend, wrecv, xsend, xrecv,
):
    s = lax.axis_index("seq")
    z = lax.axis_index("fsdp")
    linear = s * groups + z
    devices = seqs * groups
    tok, width = hid.shape
    rows, cols = blk.shape
    unit = rows // seqs
    bits = seqs.bit_length() - 1
    heads = cols // (2 * HEAD)
    duo = 2 * HEAD
    group = q_ref.shape[1] // HEAD // heads
    span = reach * tok
    last = groups - 1
    sibling = flipped(s, 1)
    peers = [m << 1 for m in range(1, seqs // 2)]
    nt = (((1,), (1,)), ((), ()))
    tn = (((0,), (0,)), ((), ()))
    mesh_id = pl.DeviceIdType.MESH

    def chunk(g):
        return pl.ds(g * duo, duo)

    def remote(src, dst, send, recv, to_s, to_z):
        return pltpu.make_async_remote_copy(
            src_ref=src, dst_ref=dst, send_sem=send, recv_sem=recv, device_id=(to_s, to_z), device_id_type=mesh_id
        )

    barrier = pltpu.get_barrier_semaphore()
    partners = [(None, flipped(s, m), z) for m in range(1, seqs)]
    partners += [(z < last, s, z + 1), (z > 0, s, z - 1)]
    for offset in range(1, reach + 1):
        up, down = linear + offset, linear - offset
        partners.append((up < devices, up // groups, up % groups))
        partners.append((down >= 0, down // groups, down % groups))

    def greet(to_s, to_z):
        pl.semaphore_signal(barrier, inc=1, device_id=(to_s, to_z), device_id_type=mesh_id)

    for present, to_s, to_z in partners:
        if present is None:
            greet(to_s, to_z)
        else:
            pl.when(present)(functools.partial(greet, to_s, to_z))

    mine = pl.ds(pl.multiple_of(s * unit, 16), unit)
    first = pltpu.make_async_copy(blk_in.at[mine, :], lead_ref, lsem.at[0])
    first.start()
    loads = [
        pltpu.make_async_copy(blk_in, blk, lsem.at[1]),
        pltpu.make_async_copy(hid_in, hid, lsem.at[2]),
        pltpu.make_async_copy(q_in, q_ref, lsem.at[3]),
        pltpu.make_async_copy(g_in, g_ref, lsem.at[4]),
    ]
    loads[1].start()

    def scale_block(i, source, at):
        to = pl.ds(pl.multiple_of(z * rows + i * QB, QB), QB)
        for j in range(cols // QB):
            block = source[pl.ds(at, QB), j * QB : (j + 1) * QB].astype(jnp.float32) * sc_ref[j, i]
            side = j // heads * HEAD
            w_ref[j % heads, to, side : side + HEAD] = block.astype(jnp.bfloat16)

    near = jnp.minimum(z, last - z)

    def shard_at(turn):
        step = turn // 2 + 1
        paired = z - step if turn % 2 == 0 else z + step
        far = turn - near + 1
        single = jnp.where(z > last - z, z - far, z + far)
        return jnp.where(turn < 2 * near, paired, single)

    shards = [shard_at(turn) for turn in range(groups - 1)]
    orders = (list(range(1, bits)), list(range(bits - 1, 0, -1)))

    def span_of(g, shard, owner, h=None):
        at = shard * rows + owner * unit + (0 if h is None else h * (unit // 2))
        return w_ref.at[g, pl.ds(pl.multiple_of(at, 16), unit if h is None else unit // 2), :]

    def kinds(g):
        return range(3 if g in WIDE else 1)

    def line_copy(shard, up, g, kind):
        if kind == 0:
            piece = span_of(g, shard, s)
        else:
            piece = span_of(g, shard, flipped(s, 1 << orders[kind - 1][0]), kind - 1)
        return remote(piece, piece, zsend.at[up, shard], zrecv.at[shard, g], s, z + 1 if up else z - 1)

    def cube_copy(turn, g, h, step, which, incoming):
        order = orders[h]
        bit = order[step]
        mask = 0
        for k in range(step):
            if which >> k & 1:
                mask |= 1 << order[k]
        piece = span_of(g, shards[turn], flipped(s, mask | (1 << bit) if incoming else mask), h)
        return remote(piece, piece, qsend.at[0], qrecv.at[turn, g, step], flipped(s, 1 << bit), z)

    def pair_copy(turn, g, m, incoming):
        piece = span_of(g, shards[turn], flipped(s, (m << 1) | 1 if incoming else m << 1))
        return remote(piece, piece, csend.at[0], crecv.at[turn, g], sibling, z)

    def hidden_copy(d, m):
        peer = flipped(s, m)
        return remote(
            hid.at[:, pl.ds(pl.multiple_of(d * rows + peer * unit, 128), unit)], hb.at[s, d],
            hsend.at[0], hrecv.at[d], peer, z,
        )

    def hidden_send(d):
        for m in range(1, seqs):
            hidden_copy(d, m).start()

    def hidden_wait(d):
        whole = hb.at[pl.ds(0, seqs - 1), d]
        remote(whole, whole, hsend.at[0], hrecv.at[d], s, z).wait_recv()

    def own_send(g):
        for kind in kinds(g):

            @pl.when(z < last)
            def _():
                line_copy(z, 1, g, kind).start()

            @pl.when(z > 0)
            def _():
                line_copy(z, 0, g, kind).start()

    def forward(turn, g):
        shard = shards[turn]
        whole = w_ref.at[g, pl.ds(0, unit * (2 if g in WIDE else 1)), :]
        remote(whole, whole, zsend.at[0, shard], zrecv.at[shard, g], s, z).wait_recv()
        for kind in kinds(g):

            @pl.when((shard < z) & (z < last))
            def _():
                line_copy(shard, 1, g, kind).start()

            @pl.when((shard > z) & (z > 0))
            def _():
                line_copy(shard, 0, g, kind).start()

    def cube_wait(turn, g, step):
        whole = w_ref.at[g, pl.ds(0, unit << step), :]
        remote(whole, whole, qsend.at[0], qrecv.at[turn, g, step], s, z).wait_recv()

    def cube_send(turn, g, step):
        for which in range(1 << step):
            for h in range(2):
                cube_copy(turn, g, h, step, which, False).start()

    def pair_send(turn, g):
        for m in range(seqs // 2):
            pair_copy(turn, g, m, False).start()

    def pair_wait(turn, g):
        whole = w_ref.at[g, pl.ds(0, unit * (seqs // 2)), :]
        remote(whole, whole, csend.at[0], crecv.at[turn, g], s, z).wait_recv()

    def begin(turn, g):
        if g not in WIDE:
            cube_send(turn, g, 0)
        else:
            cube_send(turn, g, 1)

    def cube_next(turn, g):
        cube_wait(turn, g, 0)
        cube_send(turn, g, 1)

    def pair_send_after(turn, g):
        cube_wait(turn, g, bits - 2)
        pair_send(turn, g)

    first.wait()
    loads[0].start()
    lead = unit // QB
    for i in range(lead):
        scale_block(s * lead + i, lead_ref, i * QB)
    pl.semaphore_wait(barrier, sum(1 if present is None else jnp.where(present, 1, 0) for present, _, _ in partners))

    own_send(0)
    loads[1].wait()
    hidden_send(0)
    loads[0].wait()

    def scale_rest(i, carry):
        place = (s * lead + lead + i) % (rows // QB)
        scale_block(place, blk, pl.multiple_of(place * QB, QB))
        return carry

    lax.fori_loop(0, rows // QB - lead, scale_rest, 0)
    loads[2].start()
    loads[3].start()
    row = lax.broadcasted_iota(jnp.int32, (tok, tok), 0)
    col = lax.broadcasted_iota(jnp.int32, (tok, tok), 1)
    bias[...] = jnp.where((col > row) & (linear < reach), NEG, 0.0)
    for offset in range(1, reach + 1):

        @pl.when(linear < offset)
        def _():
            win[(reach - offset) * tok : (reach - offset + 1) * tok, :] = jnp.zeros((tok, cols), jnp.bfloat16)

        @pl.when(linear + offset >= devices)
        def _():
            ret[offset - 1] = jnp.zeros((tok, cols), jnp.bfloat16)

    @pl.when(z == 0)
    def _():
        for g in range(heads):
            upr[g, 0] = jnp.zeros((unit, duo), jnp.bfloat16)

    @pl.when(z == last)
    def _():
        for g in range(heads):
            dnr[g, last] = jnp.zeros((unit, duo), jnp.bfloat16)

    deep = min(1024, width)

    def project_chunk(g):
        def step(i, total):
            at = pl.multiple_of(i * deep, deep)
            return total + jnp.dot(hid[:, pl.ds(at, deep)], w_ref[g, pl.ds(at, deep), :], preferred_element_type=jnp.float32)

        total = lax.fori_loop(0, width // deep, step, jnp.zeros((tok, duo), jnp.float32))
        win[span:, g * duo : (g + 1) * duo] = total.astype(jnp.bfloat16)
        for offset in range(1, reach + 1):

            @pl.when(linear + offset < devices)
            def _():
                halo_copy(g, offset, False).start()

    def halo_copy(g, offset, incoming):
        other = linear - offset if incoming else linear + offset
        return remote(
            win.at[pl.ds(span, tok), chunk(g)], win.at[pl.ds((reach - offset) * tok, tok), chunk(g)],
            ksend.at[offset - 1], krecv.at[g, offset - 1], other // groups, other % groups,
        )

    def back_copy(g, offset, incoming):
        other = linear + offset if incoming else linear - offset
        return remote(
            back.at[offset - 1, :, chunk(g)], ret.at[offset - 1, :, chunk(g)],
            bsend.at[offset - 1], brecv.at[g, offset - 1], other // groups, other % groups,
        )

    factor = 1.0 / float(HEAD) ** 0.5
    cat = lambda parts: jnp.concatenate(parts, axis=0)

    def attend_chunk(g):
        for offset in range(1, reach + 1):

            @pl.when(linear >= offset)
            def _():
                halo_copy(g, offset, True).wait_recv()

        keys = win[:, g * duo : g * duo + HEAD]
        values = win[:, g * duo + HEAD : (g + 1) * duo]
        cuts = [slice(h * HEAD, (h + 1) * HEAD) for h in range(g * group, (g + 1) * group)]
        q = cat([q_ref[:, cut] for cut in cuts])
        go = cat([g_ref[:, cut] for cut in cuts])
        upper = cat([col > row] * group)
        scores = lax.dot_general(q, keys, nt, preferred_element_type=jnp.float32)
        dprobs = lax.dot_general(go, values, nt, preferred_element_type=jnp.float32)

        def folded(x):
            return [jnp.where(upper, x[:, :tok], x[:, span:])] + [x[:, j * tok : (j + 1) * tok] for j in range(1, reach)]

        def unfolded(x):
            zero = jnp.zeros_like(x[0])
            parts = [jnp.where(upper, x[0], zero)] + x[1:] + [jnp.where(upper, zero, x[0])]
            return jnp.concatenate([part.astype(jnp.bfloat16) for part in parts], axis=1)

        masks = [cat([bias[...]] * group)] + [jnp.where(linear < reach - j, NEG, 0.0) for j in range(1, reach)]
        scores = [x * factor + mask for x, mask in zip(folded(scores), masks)]
        dprobs = folded(dprobs)
        top = jnp.max(functools.reduce(jnp.maximum, scores), axis=-1, keepdims=True)
        expd = [jnp.exp(x - top) for x in scores]
        scale = 1.0 / jnp.sum(functools.reduce(jnp.add, expd), axis=-1, keepdims=True)
        probs = [x * scale for x in expd]
        delta = jnp.sum(functools.reduce(jnp.add, [p * d for p, d in zip(probs, dprobs)]), axis=-1, keepdims=True)
        probs_b = unfolded(probs)
        dscores = unfolded([p * (d - delta) * factor for p, d in zip(probs, dprobs)])
        out = jnp.dot(probs_b, values, preferred_element_type=jnp.float32).astype(jnp.bfloat16)
        gq = jnp.dot(dscores, keys, preferred_element_type=jnp.float32).astype(jnp.bfloat16)
        for i, cut in enumerate(cuts):
            ao[:, cut] = out[i * tok : (i + 1) * tok]
            dq[:, cut] = gq[i * tok : (i + 1) * tok]
        dk = lax.dot_general(dscores, q, tn, preferred_element_type=jnp.float32)
        dv = lax.dot_general(probs_b, go, tn, preferred_element_type=jnp.float32)
        for side, value in ((0, dk), (HEAD, dv)):
            cut = slice(g * duo + side, g * duo + side + HEAD)
            for offset in range(1, reach + 1):
                back[offset - 1, :, cut] = value[(reach - offset) * tok : (reach - offset + 1) * tok].astype(jnp.bfloat16)
            own[:, cut] = value[span:]
        for offset in range(1, reach + 1):

            @pl.when(linear >= offset)
            def _():
                back_copy(g, offset, False).start()

    def cube_mask(h, step, which):
        return sum(1 << orders[h][k] for k in range(step) if which >> k & 1)

    def every_copy(g, h, step, which):
        block = every.at[flipped(s, cube_mask(h, step, which)), pl.ds(h * (tok // 2), tok // 2), chunk(g)]
        return remote(block, block, esend.at[0], erecv.at[g, step], flipped(s, 1 << orders[h][step]), z)

    def every_send(g, step):
        for which in range(1 << step):
            for h in range(2):
                every_copy(g, h, step, which).start()

    def every_pair(g, m, incoming):
        block = every.at[flipped(s, m | 1 if incoming else m), :, chunk(g)]
        return remote(block, block, fsend.at[0], frecv.at[g], sibling, z)

    def settle(g):
        for offset in range(1, reach + 1):

            @pl.when(linear + offset < devices)
            def _():
                back_copy(g, offset, True).wait_recv()

        cut = slice(g * duo, (g + 1) * duo)
        total = own[:, cut]
        seg = total
        for offset in range(1, reach + 1):
            piece = ret[offset - 1, :, cut].astype(jnp.float32)
            total = total + piece
            seg = seg + piece * jnp.where(z + offset < groups, 1.0, 0.0)
        every[s, :, cut] = total.astype(jnp.bfloat16)
        inside[:, cut] = seg.astype(jnp.bfloat16)
        every_send(g, 0)
        every_pair(g, 0, False).start()

    def widen(g):
        whole = every.at[0, :, chunk(g)]
        remote(whole, whole, esend.at[0], erecv.at[g, 0], s, z).wait_recv()
        every_send(g, 1)

    def share(g):
        whole = every.at[pl.ds(0, 2), :, chunk(g)]
        remote(whole, whole, esend.at[0], erecv.at[g, 1], s, z).wait_recv()
        for m in peers:
            every_pair(g, m, False).start()

    part_rows = unit // SPLIT

    def half_of(ref, g, d, q):
        return ref.at[g, d, pl.ds(q * part_rows, part_rows), :]

    def up_copy(g, d, q):
        return remote(half_of(ups, g, d, q), half_of(upr, g, d, q), usend.at[d], urecv.at[g, d, q], s, z + 1)

    def down_copy(g, d, q):
        return remote(half_of(dns, g, d, q), half_of(dnr, g, d, q), dsend.at[d], drecv.at[g, d, q], s, z - 1)

    def pass_on(g, d, up, adds):
        source, here, copy = (ups, upr, up_copy) if up else (dns, dnr, down_copy)
        for q in range(SPLIT):
            cut = slice(q * part_rows, (q + 1) * part_rows)
            value = part[g, d, cut]
            if adds:
                copy(g, d, q).wait_recv()
                value = value + here[g, d, cut].astype(jnp.float32)
            source[g, d, cut] = value.astype(jnp.bfloat16)
            copy(g, d, q).start()

    def hop(g, k):
        @pl.when(z == k)
        def _():
            for d in range(last, k, -1):
                pass_on(g, d, True, True)

        @pl.when(z == last - k)
        def _():
            for d in range(last - k):
                pass_on(g, d, False, True)

    def product(g):
        whole = every.at[pl.ds(0, seqs // 2), :, chunk(g)]
        remote(whole, whole, fsend.at[0], frecv.at[g], s, z).wait_recv()
        grads = every[:, :, g * duo : (g + 1) * duo].reshape(seqs * tok, duo)
        for i in range(groups):
            d = jnp.where(z == 0, last - i, i)
            rows_of = pl.ds(pl.multiple_of(d * unit, 128), unit)
            part[g, d] = jnp.dot(ht[rows_of, :], grads, preferred_element_type=jnp.float32)
            if i < last:

                @pl.when(z == 0)
                def _():
                    pass_on(g, last - i, True, False)

                @pl.when(z == last)
                def _():
                    pass_on(g, i, False, False)

    def grad_copy(g, h, step, which):
        at = flipped(s, cube_mask(h, step, which)) * unit + h * (unit // 2)
        block = wgb.at[g, pl.ds(pl.multiple_of(at, 16), unit // 2), :]
        return remote(block, block, wsend.at[0], wrecv.at[g, step], flipped(s, 1 << orders[h][step]), z)

    def grad_send(g, step):
        for which in range(1 << step):
            for h in range(2):
                grad_copy(g, h, step, which).start()

    def grad_pair(g, m, incoming):
        owner = flipped(s, m | 1 if incoming else m)
        block = wgb.at[g, pl.ds(pl.multiple_of(owner * unit, 128), unit), :]
        return remote(block, block, xsend.at[0], xrecv.at[g], sibling, z)

    def reduce(g):
        @pl.when(z > 0)
        def _():
            for q in range(SPLIT):
                up_copy(g, z, q).wait_recv()

        @pl.when(z < last)
        def _():
            for q in range(SPLIT):
                down_copy(g, z, q).wait_recv()

        total = part[g, z] + upr[g, z].astype(jnp.float32) + dnr[g, z].astype(jnp.float32)
        wgb[g, pl.ds(pl.multiple_of(s * unit, 128), unit), :] = total.astype(jnp.bfloat16)
        grad_send(g, 0)
        grad_pair(g, 0, False).start()

    def expand(g):
        whole = wgb.at[g, pl.ds(0, unit), :]
        remote(whole, whole, wsend.at[0], wrecv.at[g, 0], s, z).wait_recv()
        grad_send(g, 1)

    def relay(g):
        whole = wgb.at[g, pl.ds(0, 2 * unit), :]
        remote(whole, whole, wsend.at[0], wrecv.at[g, 1], s, z).wait_recv()
        for m in peers:
            grad_pair(g, m, False).start()

    def finish_chunk(g):
        whole = wgb.at[g, pl.ds(0, seqs // 2 * unit), :]
        remote(whole, whole, xsend.at[0], xrecv.at[g], s, z).wait_recv()

    def turn_hidden(d):
        hidden_wait(d)
        hb[s, d] = hid[:, pl.ds(pl.multiple_of(d * rows + s * unit, 128), unit)]
        for i in range(seqs):
            ht[d * unit : (d + 1) * unit, i * tok : (i + 1) * tok] = hb[i, d].T

    slices = 4
    span_cols = gh.shape[1] // slices
    tall = min(512, span_cols)

    def spread(i):
        def step(j, carry):
            at = pl.multiple_of(i * span_cols + j * tall, tall)
            total = jnp.zeros((tok, tall), jnp.float32)
            for g in range(heads):
                grads = inside[:, g * duo : (g + 1) * duo]
                total = total + lax.dot_general(grads, w_ref[g, pl.ds(at, tall), :], nt, preferred_element_type=jnp.float32)
            gh[:, pl.ds(at, tall)] = total.astype(jnp.bfloat16)
            return carry

        lax.fori_loop(0, span_cols // tall, step, 0)

    def drain(ref, sem):
        remote(ref, ref, sem, wrecv.at[0, 0], s, z).wait_send()

    def drain_weights():
        wide = len([g for g in range(heads) if g in WIDE])
        for shard in range(groups):
            moved = w_ref.at[0, pl.ds(0, unit * (heads + wide)), :]

            @pl.when((shard <= z) & (z < last))
            def _():
                drain(moved, zsend.at[1, shard])

            @pl.when((shard >= z) & (z > 0))
            def _():
                drain(moved, zsend.at[0, shard])

        turns = groups - 1
        plane = heads * (seqs // 2 - 1) - wide
        drain(w_ref.at[pl.ds(0, turns), pl.ds(0, unit * plane), :], qsend.at[0])
        drain(w_ref.at[pl.ds(0, turns), pl.ds(0, unit * heads * (seqs // 2)), :], csend.at[0])

    def drain_tokens():
        drain(hb.at[pl.ds(0, seqs - 1)], hsend.at[0])
        for offset in range(1, reach + 1):

            @pl.when(linear + offset < devices)
            def _():
                drain(ret.at[offset - 1], ksend.at[offset - 1])

            @pl.when(linear >= offset)
            def _():
                drain(ret.at[offset - 1], bsend.at[offset - 1])

        drain(every.at[pl.ds(0, len(peers))], esend.at[0])
        drain(every.at[pl.ds(0, seqs // 2)], fsend.at[0])

    works = [own_send, forward, begin, cube_next, pair_send_after, pair_wait, project_chunk, attend_chunk, settle, widen, share]
    works += [product, hop, reduce, expand, relay, finish_chunk, spread, hidden_send, turn_hidden]
    fetched = False
    for place, *places in ORDER:
        if works[place] is attend_chunk and not fetched:
            loads[2].wait()
            loads[3].wait()
            fetched = True
        works[place](*places)
    drain_weights()
    drain_tokens()
    drain(wgb.at[:, pl.ds(0, len(peers) * unit), :], wsend.at[0])
    drain(wgb.at[:, pl.ds(0, seqs // 2 * unit), :], xsend.at[0])
    for d in range(groups):

        @pl.when(d > z)
        def _():
            drain(ups.at[:, d], usend.at[d])

        @pl.when(d < z)
        def _():
            drain(dns.at[:, d], dsend.at[d])


def fused(hidden, kv_blocks, kv_scale, queries, grad_out, reach):
    seqs = lax.axis_size("seq")
    groups = lax.axis_size("fsdp")
    tok, depth = hidden.shape
    rows, cols = kv_blocks.shape
    width = queries.shape[1]
    unit = rows // seqs
    heads = cols // (2 * HEAD)
    duo = 2 * HEAD
    count = (reach + 1) * tok
    bits = seqs.bit_length() - 1
    any_space = pl.BlockSpec(memory_space=pl.ANY)
    dma = pltpu.SemaphoreType.DMA
    b16 = lambda *shape: pltpu.VMEM(shape, jnp.bfloat16)
    f32 = lambda *shape: pltpu.VMEM(shape, jnp.float32)
    return pl.pallas_call(
        functools.partial(fused_kernel, seqs, groups, reach),
        out_shape=[b16(tok, width), b16(tok, width), b16(tok, depth), b16(heads, rows, duo)],
        in_specs=[any_space, any_space, pl.BlockSpec(memory_space=pltpu.SMEM), any_space, any_space],
        out_specs=[pl.BlockSpec(memory_space=pltpu.VMEM)] * 4,
        scratch_shapes=[
            b16(tok, depth), b16(rows, cols), b16(tok, width), b16(tok, width),
            b16(heads, depth, duo), b16(count, cols),
            b16(reach, tok, cols), b16(reach, tok, cols), f32(tok, cols), b16(seqs, tok, cols), b16(tok, cols),
            b16(seqs, groups, tok, unit), b16(groups * unit, seqs * tok), f32(heads, groups, unit, duo),
            b16(heads, groups, unit, duo), b16(heads, groups, unit, duo), b16(heads, groups, unit, duo), b16(heads, groups, unit, duo),
            f32(tok, tok), b16(unit, cols),
            dma((5,)), dma((2, groups)), dma((groups, heads)),
            dma((1,)), dma((groups - 1, heads, bits - 1)), dma((1,)), dma((groups - 1, heads)), dma((1,)), dma((groups,)),
            dma((reach,)), dma((heads, reach)), dma((reach,)), dma((heads, reach)),
            dma((1,)), dma((heads, 2)), dma((1,)), dma((heads,)),
            dma((groups,)), dma((heads, groups, SPLIT)), dma((groups,)), dma((heads, groups, SPLIT)),
            dma((1,)), dma((heads, 2)), dma((1,)), dma((heads,)),
        ],
        compiler_params=pltpu.CompilerParams(collective_id=0, has_side_effects=True, vmem_limit_bytes=VMEM_LIMIT),
        name="fused",
    )(hidden, kv_blocks, kv_scale.T, queries, grad_out)


def write_kernel(ao, dq, gh, wgb, ao_out, dq_out, gh_out, wg_out, wide, osem):
    parts, size, cols = wide.shape
    heads = wgb.shape[0]
    triples = ((ao, ao_out), (dq, dq_out), (gh, gh_out))
    stores = [pltpu.make_async_copy(src, dst, osem.at[parts + k]) for k, (src, dst) in enumerate(triples)]
    for copy in stores:
        copy.start()
    for p in range(parts):
        for g in range(heads):
            block = wgb[g, p * size : (p + 1) * size, :].astype(jnp.float32)
            wide[p, :, g * HEAD : (g + 1) * HEAD] = block[:, :HEAD]
            wide[p, :, (heads + g) * HEAD : (heads + g + 1) * HEAD] = block[:, HEAD:]
        store = pltpu.make_async_copy(wide.at[p], wg_out.at[pl.ds(p * size, size), :], osem.at[p])
        store.start()
        stores.append(store)
    for copy in stores:
        copy.wait()


def write(ao, dq, gh, wgb):
    parts = 8
    heads, rows, duo = wgb.shape
    any_space = pl.BlockSpec(memory_space=pl.ANY)
    return pl.pallas_call(
        write_kernel,
        out_shape=[jax.ShapeDtypeStruct(x.shape, x.dtype) for x in (ao, dq, gh)]
        + [jax.ShapeDtypeStruct((rows, heads * duo), jnp.float32)],
        in_specs=[pl.BlockSpec(memory_space=pltpu.VMEM)] * 4,
        out_specs=[any_space] * 4,
        scratch_shapes=[pltpu.VMEM((parts, rows // parts, heads * duo), jnp.float32), pltpu.SemaphoreType.DMA((parts + 3,))],
        compiler_params=pltpu.CompilerParams(vmem_limit_bytes=12 << 20),
        name="write",
    )(ao, dq, gh, wgb)


def body(hidden, kv_blocks, kv_scale, queries, grad_out):
    tok = hidden.shape[0]
    groups = lax.axis_size("fsdp")
    reach = groups // 2
    unit = kv_blocks.shape[0] // lax.axis_size("seq")
    heads = kv_blocks.shape[1] // (2 * HEAD)
    if unit % QB == 0 and (heads, groups, lax.axis_size("seq")) == PLANNED:
        outs = fused(hidden, kv_blocks, kv_scale, queries, grad_out, reach)
        return tuple(write(*outs))
    weights, kv, columns = project(hidden, kv_blocks, kv_scale)
    pieces = []
    for offset in range(reach, 0, -1):
        pieces.append(shifted(kv, ("seq", "fsdp"), offset))
    window = jnp.concatenate(pieces + [kv], axis=0)
    columns = columns.reshape(groups * tok, columns.shape[2])
    attn_out, grad_queries, dwin = attend(queries, window, grad_out, reach)
    back = dwin[: reach * tok].astype(jnp.bfloat16)
    own = dwin[reach * tok :]
    grad_hidden, weight_grad = finish(back, own, weights, columns, reach)
    return (attn_out, grad_queries, grad_hidden, weight_grad.astype(jnp.float32))


def solution(mesh):
    return jax.shard_map(
        body,
        mesh=mesh,
        in_specs=(
            P(("seq", "fsdp"), None),
            P("fsdp", None),
            P("fsdp", None),
            P(("seq", "fsdp"), None),
            P(("seq", "fsdp"), None),
        ),
        out_specs=(
            P(("seq", "fsdp"), None),
            P(("seq", "fsdp"), None),
            P(("seq", "fsdp"), None),
            P("fsdp", None),
        ),
        check_vma=False,
    )
```

```python
import functools

import jax
import jax.numpy as jnp
from jax import lax
from jax.experimental import pallas as pl
from jax.experimental.pallas import tpu as pltpu
from jax.sharding import PartitionSpec as P

HEADS = 32
KV_HEADS = 4
HEAD = 128
QB = 128


NEG = -1e30
PLANNED = (4, 4, 8)
(SEND, FORWARD, BEGIN, CUBE, PAIR, LAND, PROJECT, ATTEND, SETTLE, WIDEN, SHARE) = range(11)
(PRODUCT, HOP, REDUCE, EXPAND, RELAY, FINISH, SPREAD, HIDDEN, TURN) = range(11, 20)
VMEM_LIMIT = 50 << 20
SPLIT = 2
WIDE = (2,)
ORDER = (
    (SEND, 2), (FORWARD, 1, 0), (FORWARD, 0, 0), (BEGIN, 0, 0), (HIDDEN, 2), (FORWARD, 1, 2), (CUBE, 0, 0),
    (BEGIN, 1, 0), (FORWARD, 0, 2), (FORWARD, 2, 0), (BEGIN, 0, 2), (FORWARD, 2, 2), (SEND, 1), (BEGIN, 1, 2),
    (BEGIN, 2, 0), (SEND, 3), (CUBE, 1, 0), (FORWARD, 1, 3), (BEGIN, 2, 2), (FORWARD, 0, 3), (FORWARD, 0, 1),
    (PAIR, 1, 2), (FORWARD, 1, 1), (PAIR, 1, 0), (CUBE, 2, 0), (BEGIN, 0, 3), (FORWARD, 2, 3), (PAIR, 2, 2),
    (BEGIN, 0, 1), (PAIR, 0, 0), (TURN, 0), (LAND, 1, 0), (BEGIN, 1, 3), (PAIR, 0, 2), (LAND, 1, 2), (LAND, 0, 0),
    (PAIR, 2, 0), (CUBE, 0, 3), (LAND, 2, 2), (LAND, 2, 0), (TURN, 2), (LAND, 0, 2), (FORWARD, 2, 1), (CUBE, 0, 1),
    (PROJECT, 2), (PROJECT, 0), (BEGIN, 2, 3), (PAIR, 0, 3), (BEGIN, 2, 1), (CUBE, 1, 3), (BEGIN, 1, 1), (CUBE, 2, 3),
    (ATTEND, 2), (PAIR, 1, 3), (CUBE, 1, 1), (ATTEND, 0), (PAIR, 0, 1), (CUBE, 2, 1), (PAIR, 2, 3), (SETTLE, 2),
    (HIDDEN, 3), (LAND, 2, 3), (LAND, 1, 3), (LAND, 0, 3), (PROJECT, 3), (PAIR, 1, 1), (PAIR, 2, 1), (WIDEN, 2),
    (LAND, 0, 1), (LAND, 1, 1), (LAND, 2, 1), (PROJECT, 1), (HIDDEN, 1), (ATTEND, 3), (SHARE, 2), (ATTEND, 1),
    (TURN, 3), (SETTLE, 0), (TURN, 1), (PRODUCT, 2), (WIDEN, 0), (SETTLE, 3), (SETTLE, 1), (HOP, 2, 1), (WIDEN, 3),
    (HOP, 2, 2), (SHARE, 0), (SPREAD, 2), (PRODUCT, 0), (REDUCE, 2), (SHARE, 3), (WIDEN, 1), (HOP, 0, 1), (EXPAND, 2),
    (PRODUCT, 3), (SHARE, 1), (HOP, 0, 2), (REDUCE, 0), (HOP, 3, 1), (PRODUCT, 1), (HOP, 3, 2), (EXPAND, 0),
    (RELAY, 2), (REDUCE, 3), (HOP, 1, 1), (HOP, 1, 2), (EXPAND, 3), (SPREAD, 0), (FINISH, 2), (REDUCE, 1),
    (SPREAD, 3), (EXPAND, 1), (RELAY, 3), (RELAY, 0), (SPREAD, 1), (RELAY, 1), (FINISH, 3), (FINISH, 0), (FINISH, 1),
)


def shifted(block, axis, distance):
    devices = range(lax.axis_size(axis))
    route = [(i - distance, i) for i in devices if i - distance in devices]
    return lax.ppermute(block, axis, route)


def attend_kernel(reach, q_ref, g_ref, k_ref, v_ref, out_ref, dq_ref, dk_ref, dv_ref):
    tok = q_ref.shape[0]
    group = q_ref.shape[1] // HEAD
    count = k_ref.shape[0]
    span = reach * tok
    factor = 1.0 / float(HEAD) ** 0.5
    base = (lax.axis_index("seq") * lax.axis_size("fsdp") + lax.axis_index("fsdp")) * tok
    row = lax.broadcasted_iota(jnp.int32, (tok, count), 0)
    col = lax.broadcasted_iota(jnp.int32, (tok, count), 1)
    allowed = (col > row) & (col <= row + span) & (col >= span - base)
    keys = k_ref[...]
    values = v_ref[...]
    nt = (((1,), (1,)), ((), ()))
    tn = (((0,), (0,)), ((), ()))
    ps, ds, qs, gs = [], [], [], []
    for h in range(group):
        cut = slice(h * HEAD, (h + 1) * HEAD)
        q = q_ref[:, cut]
        g = g_ref[:, cut]
        scores = lax.dot_general(q, keys, nt, preferred_element_type=jnp.float32) * factor
        scores = jnp.where(allowed, scores, NEG)
        expd = jnp.exp(scores - jnp.max(scores, axis=-1, keepdims=True))
        probs = expd * (1.0 / jnp.sum(expd, axis=-1, keepdims=True))
        probs_b = probs.astype(jnp.bfloat16)
        out_ref[:, cut] = jnp.dot(probs_b, values, preferred_element_type=jnp.float32).astype(jnp.bfloat16)
        dprobs = lax.dot_general(g, values, nt, preferred_element_type=jnp.float32)
        delta = jnp.sum(probs * dprobs, axis=-1, keepdims=True)
        dscores = (probs * (dprobs - delta) * factor).astype(jnp.bfloat16)
        dq_ref[:, cut] = jnp.dot(dscores, keys, preferred_element_type=jnp.float32).astype(jnp.bfloat16)
        ps.append(probs_b)
        ds.append(dscores)
        qs.append(q)
        gs.append(g)
    cat = lambda parts: jnp.concatenate(parts, axis=0)
    dk_ref[...] = lax.dot_general(cat(ds), cat(qs), tn, preferred_element_type=jnp.float32)
    dv_ref[...] = lax.dot_general(cat(ps), cat(gs), tn, preferred_element_type=jnp.float32)


def attend(queries, window, grad_out, reach):
    tok, width = queries.shape
    count = window.shape[0]
    heads = window.shape[1] // (2 * HEAD)
    wide = pl.BlockSpec((tok, width // heads), lambda i: (0, i))
    key = pl.BlockSpec((count, HEAD), lambda i: (0, i))
    value = pl.BlockSpec((count, HEAD), lambda i: (0, i + heads))
    out, dq, dk, dv = pl.pallas_call(
        functools.partial(attend_kernel, reach),
        grid=(heads,),
        in_specs=[wide, wide, key, value],
        out_specs=[wide, wide, key, key],
        out_shape=[
            jax.ShapeDtypeStruct((tok, width), jnp.bfloat16),
            jax.ShapeDtypeStruct((tok, width), jnp.bfloat16),
            jax.ShapeDtypeStruct((count, heads * HEAD), jnp.float32),
            jax.ShapeDtypeStruct((count, heads * HEAD), jnp.float32),
        ],
        cost_estimate=pl.CostEstimate(flops=12 * tok * width * count, bytes_accessed=8 * tok * width, transcendentals=0),
        name="attend",
    )(queries, grad_out, window, window)
    return out, dq, jnp.concatenate([dk, dv], axis=1)


def flipped(index, mask):
    for place in range(mask.bit_length()):
        if mask >> place & 1:
            index = index + (1 << place) * (1 - 2 * (index // (1 << place) % 2))
    return index


def orders_of(bits):
    return (list(range(1, bits)) + [0], list(range(bits - 1, 0, -1)) + [0])


def project_kernel(seqs, groups, hid_ref, blk_ref, sc_ref, out_ref, kv_ref, col_ref, w_ref, acc, zsend, zrecv, qsend, qrecv, csend, crecv, wsem):
    s = lax.axis_index("seq")
    z = lax.axis_index("fsdp")
    rows = blk_ref.shape[0]
    unit = rows // seqs
    half = unit // 2
    bits = seqs.bit_length() - 1
    chunk = min(512, rows)

    def scale_block(i, carry):
        at = pl.multiple_of(i * QB, QB)
        block = blk_ref[pl.ds(at, QB), :].astype(jnp.float32) * sc_ref[pl.ds(i, 1), :]
        w_ref[pl.ds(pl.multiple_of(z * rows + at, QB), QB), :] = block.astype(jnp.bfloat16)
        return carry

    lax.fori_loop(0, rows // QB, scale_block, 0)

    def line_copy(shard, up):
        piece = w_ref.at[pl.ds(pl.multiple_of(shard * rows + s * unit, 16), unit), :]
        return pltpu.make_async_remote_copy(
            src_ref=piece,
            dst_ref=piece,
            send_sem=zsend.at[up, shard],
            recv_sem=zrecv.at[shard],
            device_id=(s, z + 1 if up else z - 1),
            device_id_type=pl.DeviceIdType.MESH,
        )

    def cube_copy(turn, shard, order, step, which, incoming):
        bit = order[step]
        mask = 0
        for k in range(step):
            if which >> k & 1:
                mask |= 1 << order[k]
        h = 0 if order is orders[0] else 1
        owner = flipped(s, mask | (1 << bit) if incoming else mask)
        piece = w_ref.at[pl.ds(pl.multiple_of(shard * rows + owner * unit + h * half, 16), half), :]
        slot = (1 << step) - 1 + which
        return pltpu.make_async_remote_copy(
            src_ref=piece,
            dst_ref=piece,
            send_sem=qsend.at[turn, h, slot],
            recv_sem=qrecv.at[turn, h, slot],
            device_id=(flipped(s, 1 << bit), z),
            device_id_type=pl.DeviceIdType.MESH,
        )

    orders = orders_of(bits)
    near = jnp.minimum(z, groups - 1 - z)

    def shard_at(turn):
        step = turn // 2 + 1
        paired = z - step if turn % 2 == 0 else z + step
        far = turn - near + 1
        single = jnp.where(z > groups - 1 - z, z - far, z + far)
        return jnp.where(turn < 2 * near, paired, single)

    shards = [shard_at(turn) for turn in range(groups - 1)]

    @pl.when(z < groups - 1)
    def _():
        line_copy(z, 1).start()

    @pl.when(z > 0)
    def _():
        line_copy(z, 0).start()

    def column_copy(gap, incoming):
        other = (z - gap + groups) % groups if incoming else (z + gap) % groups
        part = pl.multiple_of(other * rows, 128)
        return pltpu.make_async_remote_copy(
            src_ref=hid_ref.at[:, pl.ds(part, rows)],
            dst_ref=col_ref.at[other if incoming else z],
            send_sem=csend.at[gap - 1],
            recv_sem=crecv.at[gap - 1],
            device_id=(s, other),
            device_id_type=pl.DeviceIdType.MESH,
        )

    acc[...] = jnp.zeros_like(acc)

    def store_copy(turn, shard):
        part = pl.ds(pl.multiple_of(shard * rows, 16), rows)
        return pltpu.make_async_copy(w_ref.at[part, :], out_ref.at[part, :], wsem.at[turn])

    def multiply(shard):
        def part(i, carry):
            at = pl.multiple_of(shard * rows + i * chunk, 128)
            acc[...] += jnp.dot(
                hid_ref[:, pl.ds(at, chunk)], w_ref[pl.ds(at, chunk), :], preferred_element_type=jnp.float32
            )
            return carry

        lax.fori_loop(0, rows // chunk, part, 0)

    multiply(z)
    store_copy(groups - 1, z).start()
    col_ref[z] = hid_ref[:, pl.ds(pl.multiple_of(z * rows, 128), rows)]
    for tick in range(groups - 1 + bits):
        for stage in range(bits, -1, -1):
            turn = tick - stage
            if turn < 0 or turn >= groups - 1:
                continue
            shard = shards[turn]
            if stage == 0:
                line_copy(shard, 0).wait_recv()

                @pl.when((shard < z) & (z < groups - 1))
                def _():
                    line_copy(shard, 1).start()

                @pl.when((shard > z) & (z > 0))
                def _():
                    line_copy(shard, 0).start()
            else:
                for order in orders:
                    for which in range(1 << (stage - 1)):
                        cube_copy(turn, shard, order, stage - 1, which, True).wait_recv()
            if stage < bits:
                for order in orders:
                    for which in range(1 << stage):
                        cube_copy(turn, shard, order, stage, which, False).start()
            else:
                multiply(shard)
                store_copy(turn, shard).start()
        if tick == groups - 2:
            for gap in range(1, groups):
                column_copy(gap, False).start()
    kv_ref[...] = acc[...].astype(jnp.bfloat16)
    for turn in range(groups - 1):
        store_copy(turn, shards[turn]).wait()
    store_copy(groups - 1, z).wait()
    for gap in range(1, groups):
        column_copy(gap, True).wait_recv()
        column_copy(gap, False).wait_send()
    for shard in range(groups):

        @pl.when((shard <= z) & (z < groups - 1))
        def _():
            line_copy(shard, 1).wait_send()

        @pl.when((shard >= z) & (z > 0))
        def _():
            line_copy(shard, 0).wait_send()

    for turn in range(groups - 1):
        for order in orders:
            for stage in range(bits):
                for which in range(1 << stage):
                    cube_copy(turn, shards[turn], order, stage, which, False).wait_send()


def project(hidden, kv_blocks, kv_scale):
    seqs = lax.axis_size("seq")
    groups = lax.axis_size("fsdp")
    tok, width = hidden.shape
    cols = kv_blocks.shape[1]
    spread = jnp.repeat(kv_scale, QB, axis=1)
    vmem = pl.BlockSpec(memory_space=pltpu.VMEM)
    return pl.pallas_call(
        functools.partial(project_kernel, seqs, groups),
        out_shape=[
            jax.ShapeDtypeStruct((width, cols), jnp.bfloat16),
            jax.ShapeDtypeStruct((tok, cols), jnp.bfloat16),
            jax.ShapeDtypeStruct((groups, tok, kv_blocks.shape[0]), jnp.bfloat16),
        ],
        in_specs=[vmem] * 3,
        out_specs=[pl.BlockSpec(memory_space=pl.ANY), vmem, vmem],
        scratch_shapes=[
            pltpu.VMEM((width, cols), jnp.bfloat16),
            pltpu.VMEM((tok, cols), jnp.float32),
            pltpu.SemaphoreType.DMA((2, groups)),
            pltpu.SemaphoreType.DMA((groups,)),
            pltpu.SemaphoreType.DMA((groups - 1, 2, seqs - 1)),
            pltpu.SemaphoreType.DMA((groups - 1, 2, seqs - 1)),
            pltpu.SemaphoreType.DMA((groups - 1,)),
            pltpu.SemaphoreType.DMA((groups - 1,)),
            pltpu.SemaphoreType.DMA((groups,)),
        ],
        compiler_params=pltpu.CompilerParams(has_side_effects=True),
        name="project",
    )(hidden, kv_blocks, spread)


def finish_kernel(
    seqs, groups, reach, back_ref, own_ref, in_ref, col_ref, gh_ref, wg_ref,
    w_ref, wsem, ret, every, inside, acc, sends, recvs, hsend, hrecv, gsend, grecv, rsend, rrecv, asend, arecv,
):
    s = lax.axis_index("seq")
    z = lax.axis_index("fsdp")
    linear = s * groups + z
    devices = seqs * groups
    tok, cols = own_ref.shape
    rows = col_ref.shape[1]
    bits = seqs.bit_length() - 1
    mesh_id = pl.DeviceIdType.MESH
    load = pltpu.make_async_copy(in_ref, w_ref, wsem)
    load.start()

    def halo_copy(offset, incoming):
        other = linear + offset if incoming else linear - offset
        return pltpu.make_async_remote_copy(
            src_ref=back_ref.at[pl.ds((reach - offset) * tok, tok), :],
            dst_ref=ret.at[offset - 1],
            send_sem=hsend.at[offset - 1],
            recv_sem=hrecv.at[offset - 1],
            device_id=(other // groups, other % groups),
            device_id_type=mesh_id,
        )

    for offset in range(1, reach + 1):

        @pl.when(linear >= offset)
        def _():
            halo_copy(offset, False).start()

    for offset in range(1, reach + 1):

        @pl.when(linear + offset < devices)
        def _():
            halo_copy(offset, True).wait_recv()

        @pl.when(linear + offset >= devices)
        def _():
            ret[offset - 1] = jnp.zeros((tok, cols), jnp.bfloat16)

    total = own_ref[...]
    seg = total
    for offset in range(1, reach + 1):
        piece = ret[offset - 1].astype(jnp.float32)
        total = total + piece
        seg = seg + piece * jnp.where(z + offset < groups, 1.0, 0.0)
    every[z] = total.astype(jnp.bfloat16)
    inside[...] = seg.astype(jnp.bfloat16)

    def gather_copy(gap, incoming):
        other = (z - gap + groups) % groups if incoming else (z + gap) % groups
        block = every.at[other if incoming else z]
        return pltpu.make_async_remote_copy(
            src_ref=block,
            dst_ref=block,
            send_sem=gsend.at[gap - 1],
            recv_sem=grecv.at[gap - 1],
            device_id=(s, other),
            device_id_type=mesh_id,
        )

    for gap in range(1, groups):
        gather_copy(gap, False).start()

    load.wait()
    wide = 512

    def spread(i, carry):
        at = pl.multiple_of(i * wide, wide)
        gh_ref[:, pl.ds(at, wide)] = lax.dot_general(
            inside[...], w_ref[pl.ds(at, wide), :], (((1,), (1,)), ((), ())), preferred_element_type=jnp.float32
        ).astype(jnp.bfloat16)
        return carry

    lax.fori_loop(0, w_ref.shape[0] // wide, spread, 0)
    for gap in range(1, groups):
        gather_copy(gap, True).wait_recv()

    big = rows // 2
    tile = min(256, big)
    low = s % 2
    sibling = flipped(s, 1)
    grads = every[...].reshape(groups * tok, cols)

    def product(at):
        return lax.dot_general(
            col_ref[:, pl.ds(at, tile)], grads, (((0,), (0,)), ((), ())), preferred_element_type=jnp.float32
        )

    def theirs(i, carry):
        at = pl.multiple_of(i * tile, tile)
        sends[0][pl.ds(at, tile), :] = product(pl.multiple_of((1 - low) * big + at, tile)).astype(jnp.bfloat16)
        return carry

    lax.fori_loop(0, big // tile, theirs, 0)

    def reduce_copy(step, h, peer):
        cut = slice(None) if h is None else pl.ds(h * (cols // 2), cols // 2)
        return pltpu.make_async_remote_copy(
            src_ref=sends[step].at[:, cut] if h is not None else sends[step],
            dst_ref=recvs[step].at[:, cut] if h is not None else recvs[step],
            send_sem=rsend.at[step, h or 0],
            recv_sem=rrecv.at[step, h or 0],
            device_id=(peer, z),
            device_id_type=mesh_id,
        )

    reduce_copy(0, None, sibling).start()

    def mine(i, carry):
        at = pl.multiple_of(i * tile, tile)
        acc[pl.ds(at, tile), :] = product(pl.multiple_of(low * big + at, tile))
        return carry

    lax.fori_loop(0, big // tile, mine, 0)
    reduce_copy(0, None, sibling).wait_recv()

    def fold(i, carry):
        at = pl.multiple_of(i * tile, tile)
        acc[pl.ds(at, tile), :] += recvs[0][pl.ds(at, tile), :].astype(jnp.float32)
        return carry

    lax.fori_loop(0, big // tile, fold, 0)
    orders = (list(range(1, bits)), list(range(bits - 1, 0, -1)))
    offsets = [[0], [0]]
    side = cols // 2
    for step in range(1, bits):
        size = rows >> (step + 1)
        for h in range(2):
            place = orders[h][step - 1]
            bit = s // (1 << place) % 2
            start = offsets[h][-1]
            away = pl.multiple_of(start + (1 - bit) * size, 16)
            sends[step][:, h * side : (h + 1) * side] = acc[
                pl.ds(away, size), h * side : (h + 1) * side
            ].astype(jnp.bfloat16)
            reduce_copy(step, h, flipped(s, 1 << place)).start()
            offsets[h].append(start + bit * size)
        for h in range(2):
            place = orders[h][step - 1]
            reduce_copy(step, h, flipped(s, 1 << place)).wait_recv()
            keep = pl.ds(pl.multiple_of(offsets[h][-1], 16), size)
            cut = slice(h * side, (h + 1) * side)
            acc[keep, cut] += recvs[step][:, cut].astype(jnp.float32)
    size = rows >> bits
    for h in range(2):
        at = offsets[h][-1]
        cut = slice(h * side, (h + 1) * side)
        wg_ref[pl.ds(pl.multiple_of(low * big + at, 16), size), cut] = acc[
            pl.ds(pl.multiple_of(at, 16), size), cut
        ].astype(jnp.bfloat16)

    def spread_copy(step, h, incoming):
        place = orders[h][step - 1]
        bit = s // (1 << place) % 2
        size = rows >> (step + 1)
        at = low * big + offsets[h][step - 1] + ((1 - bit) if incoming else bit) * size
        block = wg_ref.at[pl.ds(pl.multiple_of(at, 16), size), pl.ds(h * side, side)]
        return pltpu.make_async_remote_copy(
            src_ref=block,
            dst_ref=block,
            send_sem=asend.at[step, h],
            recv_sem=arecv.at[step, h],
            device_id=(flipped(s, 1 << place), z),
            device_id_type=mesh_id,
        )

    for step in range(bits - 1, 0, -1):
        for h in range(2):
            spread_copy(step, h, False).start()
        for h in range(2):
            spread_copy(step, h, True).wait_recv()

    def last_copy(incoming):
        block = wg_ref.at[pl.ds(pl.multiple_of(((1 - low) if incoming else low) * big, 16), big), :]
        return pltpu.make_async_remote_copy(
            src_ref=block,
            dst_ref=block,
            send_sem=asend.at[0, 0],
            recv_sem=arecv.at[0, 0],
            device_id=(sibling, z),
            device_id_type=mesh_id,
        )

    last_copy(False).start()
    last_copy(True).wait_recv()
    for offset in range(1, reach + 1):

        @pl.when(linear >= offset)
        def _():
            halo_copy(offset, False).wait_send()

    for gap in range(1, groups):
        gather_copy(gap, False).wait_send()
    reduce_copy(0, None, sibling).wait_send()
    for step in range(1, bits):
        for h in range(2):
            reduce_copy(step, h, flipped(s, 1 << orders[h][step - 1])).wait_send()
            spread_copy(step, h, False).wait_send()
    last_copy(False).wait_send()


def finish(back, own, weights, columns, reach):
    seqs = lax.axis_size("seq")
    groups = lax.axis_size("fsdp")
    tok, cols = own.shape
    rows = columns.shape[1]
    bits = seqs.bit_length() - 1
    vmem = pl.BlockSpec(memory_space=pltpu.VMEM)
    steps = [pltpu.VMEM((rows >> (k + 1), cols), jnp.bfloat16) for k in range(bits)]
    dma = pltpu.SemaphoreType.DMA
    return pl.pallas_call(
        functools.partial(finish_kernel, seqs, groups, reach),
        out_shape=[
            jax.ShapeDtypeStruct((tok, weights.shape[0]), jnp.bfloat16),
            jax.ShapeDtypeStruct((rows, cols), jnp.bfloat16),
        ],
        in_specs=[vmem, vmem, pl.BlockSpec(memory_space=pl.ANY), vmem],
        out_specs=[vmem] * 2,
        scratch_shapes=[
            pltpu.VMEM(weights.shape, jnp.bfloat16),
            dma(()),
            pltpu.VMEM((reach, tok, cols), jnp.bfloat16),
            pltpu.VMEM((groups, tok, cols), jnp.bfloat16),
            pltpu.VMEM((tok, cols), jnp.bfloat16),
            pltpu.VMEM((rows // 2, cols), jnp.float32),
            steps,
            steps,
            dma((reach,)),
            dma((reach,)),
            dma((groups - 1,)),
            dma((groups - 1,)),
            dma((bits, 2)),
            dma((bits, 2)),
            dma((bits, 2)),
            dma((bits, 2)),
        ],
        compiler_params=pltpu.CompilerParams(has_side_effects=True),
        name="finish",
    )(back, own, weights, columns)


def fused_kernel(
    seqs, groups, reach,
    hid_in, blk_in, sc_ref, q_in, g_in, ao, dq, gh, wgb,
    hid, blk, q_ref, g_ref, w_ref, win, back, ret, own, every, inside, hb, ht, part,
    ups, upr, dns, dnr, bias, lead_ref,
    lsem, zsend, zrecv, qsend, qrecv, csend, crecv, hsend, hrecv, ksend, krecv, bsend, brecv,
    esend, erecv, fsend, frecv, usend, urecv, dsend, drecv, wsend, wrecv, xsend, xrecv,
):
    s = lax.axis_index("seq")
    z = lax.axis_index("fsdp")
    linear = s * groups + z
    devices = seqs * groups
    tok, width = hid.shape
    rows, cols = blk.shape
    unit = rows // seqs
    bits = seqs.bit_length() - 1
    heads = cols // (2 * HEAD)
    duo = 2 * HEAD
    group = q_ref.shape[1] // HEAD // heads
    span = reach * tok
    last = groups - 1
    sibling = flipped(s, 1)
    peers = [m << 1 for m in range(1, seqs // 2)]
    nt = (((1,), (1,)), ((), ()))
    tn = (((0,), (0,)), ((), ()))
    mesh_id = pl.DeviceIdType.MESH

    def chunk(g):
        return pl.ds(g * duo, duo)

    def remote(src, dst, send, recv, to_s, to_z):
        return pltpu.make_async_remote_copy(
            src_ref=src, dst_ref=dst, send_sem=send, recv_sem=recv, device_id=(to_s, to_z), device_id_type=mesh_id
        )

    barrier = pltpu.get_barrier_semaphore()
    partners = [(None, flipped(s, m), z) for m in range(1, seqs)]
    partners += [(z < last, s, z + 1), (z > 0, s, z - 1)]
    for offset in range(1, reach + 1):
        up, down = linear + offset, linear - offset
        partners.append((up < devices, up // groups, up % groups))
        partners.append((down >= 0, down // groups, down % groups))

    def greet(to_s, to_z):
        pl.semaphore_signal(barrier, inc=1, device_id=(to_s, to_z), device_id_type=mesh_id)

    for present, to_s, to_z in partners:
        if present is None:
            greet(to_s, to_z)
        else:
            pl.when(present)(functools.partial(greet, to_s, to_z))

    mine = pl.ds(pl.multiple_of(s * unit, 16), unit)
    first = pltpu.make_async_copy(blk_in.at[mine, :], lead_ref, lsem.at[0])
    first.start()
    loads = [
        pltpu.make_async_copy(blk_in, blk, lsem.at[1]),
        pltpu.make_async_copy(hid_in, hid, lsem.at[2]),
        pltpu.make_async_copy(q_in, q_ref, lsem.at[3]),
        pltpu.make_async_copy(g_in, g_ref, lsem.at[4]),
    ]
    loads[1].start()

    def scale_block(i, source, at):
        to = pl.ds(pl.multiple_of(z * rows + i * QB, QB), QB)
        for j in range(cols // QB):
            block = source[pl.ds(at, QB), j * QB : (j + 1) * QB].astype(jnp.float32) * sc_ref[j, i]
            side = j // heads * HEAD
            w_ref[j % heads, to, side : side + HEAD] = block.astype(jnp.bfloat16)

    near = jnp.minimum(z, last - z)

    def shard_at(turn):
        step = turn // 2 + 1
        paired = z - step if turn % 2 == 0 else z + step
        far = turn - near + 1
        single = jnp.where(z > last - z, z - far, z + far)
        return jnp.where(turn < 2 * near, paired, single)

    shards = [shard_at(turn) for turn in range(groups - 1)]
    orders = (list(range(1, bits)), list(range(bits - 1, 0, -1)))

    def span_of(g, shard, owner, h=None):
        at = shard * rows + owner * unit + (0 if h is None else h * (unit // 2))
        return w_ref.at[g, pl.ds(pl.multiple_of(at, 16), unit if h is None else unit // 2), :]

    def kinds(g):
        return range(3 if g in WIDE else 1)

    def line_copy(shard, up, g, kind):
        if kind == 0:
            piece = span_of(g, shard, s)
        else:
            piece = span_of(g, shard, flipped(s, 1 << orders[kind - 1][0]), kind - 1)
        return remote(piece, piece, zsend.at[up, shard], zrecv.at[shard, g], s, z + 1 if up else z - 1)

    def cube_copy(turn, g, h, step, which, incoming):
        order = orders[h]
        bit = order[step]
        mask = 0
        for k in range(step):
            if which >> k & 1:
                mask |= 1 << order[k]
        piece = span_of(g, shards[turn], flipped(s, mask | (1 << bit) if incoming else mask), h)
        return remote(piece, piece, qsend.at[0], qrecv.at[turn, g, step], flipped(s, 1 << bit), z)

    def pair_copy(turn, g, m, incoming):
        piece = span_of(g, shards[turn], flipped(s, (m << 1) | 1 if incoming else m << 1))
        return remote(piece, piece, csend.at[0], crecv.at[turn, g], sibling, z)

    def hidden_copy(d, m):
        peer = flipped(s, m)
        return remote(
            hid.at[:, pl.ds(pl.multiple_of(d * rows + peer * unit, 128), unit)], hb.at[s, d],
            hsend.at[0], hrecv.at[d], peer, z,
        )

    def hidden_send(d):
        for m in range(1, seqs):
            hidden_copy(d, m).start()

    def hidden_wait(d):
        whole = hb.at[pl.ds(0, seqs - 1), d]
        remote(whole, whole, hsend.at[0], hrecv.at[d], s, z).wait_recv()

    def own_send(g):
        for kind in kinds(g):

            @pl.when(z < last)
            def _():
                line_copy(z, 1, g, kind).start()

            @pl.when(z > 0)
            def _():
                line_copy(z, 0, g, kind).start()

    inner = (z > 0) & (z < last)

    def line_wait(turn, g):
        whole = w_ref.at[g, pl.ds(0, unit * (2 if g in WIDE else 1)), :]
        remote(whole, whole, zsend.at[0, shards[turn]], zrecv.at[shards[turn], g], s, z).wait_recv()

    def forward(turn, g):
        shard = shards[turn]

        @pl.when(inner)
        def _():
            line_wait(turn, g)
            for kind in kinds(g):

                @pl.when(shard < z)
                def _():
                    line_copy(shard, 1, g, kind).start()

                @pl.when(shard > z)
                def _():
                    line_copy(shard, 0, g, kind).start()

    def cube_wait(turn, g, step):
        whole = w_ref.at[g, pl.ds(0, unit << step), :]
        remote(whole, whole, qsend.at[0], qrecv.at[turn, g, step], s, z).wait_recv()

    def cube_send(turn, g, step):
        for which in range(1 << step):
            for h in range(2):
                cube_copy(turn, g, h, step, which, False).start()

    def pair_send(turn, g):
        for m in range(seqs // 2):
            pair_copy(turn, g, m, False).start()

    def pair_wait(turn, g):
        whole = w_ref.at[g, pl.ds(0, unit * (seqs // 2)), :]
        remote(whole, whole, csend.at[0], crecv.at[turn, g], s, z).wait_recv()

    def begin(turn, g):
        @pl.when(jnp.logical_not(inner))
        def _():
            line_wait(turn, g)

        if g not in WIDE:
            cube_send(turn, g, 0)
        else:
            cube_send(turn, g, 1)

    def cube_next(turn, g):
        cube_wait(turn, g, 0)
        cube_send(turn, g, 1)

    def pair_send_after(turn, g):
        cube_wait(turn, g, bits - 2)
        pair_send(turn, g)

    first.wait()
    loads[0].start()
    lead = unit // QB
    for i in range(lead):
        scale_block(s * lead + i, lead_ref, i * QB)
    pl.semaphore_wait(barrier, sum(1 if present is None else jnp.where(present, 1, 0) for present, _, _ in partners))

    own_send(0)
    loads[1].wait()
    hidden_send(0)
    loads[0].wait()

    def scale_rest(i, carry):
        place = (s * lead + lead + i) % (rows // QB)
        scale_block(place, blk, pl.multiple_of(place * QB, QB))
        return carry

    lax.fori_loop(0, rows // QB - lead, scale_rest, 0)
    loads[2].start()
    loads[3].start()
    row = lax.broadcasted_iota(jnp.int32, (tok, tok), 0)
    col = lax.broadcasted_iota(jnp.int32, (tok, tok), 1)
    bias[...] = jnp.where((col > row) & (linear < reach), NEG, 0.0)
    for offset in range(1, reach + 1):

        @pl.when(linear < offset)
        def _():
            win[(reach - offset) * tok : (reach - offset + 1) * tok, :] = jnp.zeros((tok, cols), jnp.bfloat16)

        @pl.when(linear + offset >= devices)
        def _():
            ret[offset - 1] = jnp.zeros((tok, cols), jnp.bfloat16)

    @pl.when(z == 0)
    def _():
        for g in range(heads):
            upr[g, 0] = jnp.zeros((unit, duo), jnp.bfloat16)

    @pl.when(z == last)
    def _():
        for g in range(heads):
            dnr[g, last] = jnp.zeros((unit, duo), jnp.bfloat16)

    deep = min(1024, width)

    def project_chunk(g):
        def step(i, total):
            at = pl.multiple_of(i * deep, deep)
            return total + jnp.dot(hid[:, pl.ds(at, deep)], w_ref[g, pl.ds(at, deep), :], preferred_element_type=jnp.float32)

        total = lax.fori_loop(0, width // deep, step, jnp.zeros((tok, duo), jnp.float32))
        win[span:, g * duo : (g + 1) * duo] = total.astype(jnp.bfloat16)
        for offset in range(1, reach + 1):

            @pl.when(linear + offset < devices)
            def _():
                halo_copy(g, offset, False).start()

    def halo_copy(g, offset, incoming):
        other = linear - offset if incoming else linear + offset
        return remote(
            win.at[pl.ds(span, tok), chunk(g)], win.at[pl.ds((reach - offset) * tok, tok), chunk(g)],
            ksend.at[offset - 1], krecv.at[g, offset - 1], other // groups, other % groups,
        )

    def back_copy(g, offset, incoming):
        other = linear + offset if incoming else linear - offset
        return remote(
            back.at[offset - 1, :, chunk(g)], ret.at[offset - 1, :, chunk(g)],
            bsend.at[offset - 1], brecv.at[g, offset - 1], other // groups, other % groups,
        )

    factor = 1.0 / float(HEAD) ** 0.5
    cat = lambda parts: jnp.concatenate(parts, axis=0)

    def attend_chunk(g):
        for offset in range(1, reach + 1):

            @pl.when(linear >= offset)
            def _():
                halo_copy(g, offset, True).wait_recv()

        keys = win[:, g * duo : g * duo + HEAD]
        values = win[:, g * duo + HEAD : (g + 1) * duo]
        cuts = [slice(h * HEAD, (h + 1) * HEAD) for h in range(g * group, (g + 1) * group)]
        q = cat([q_ref[:, cut] for cut in cuts])
        go = cat([g_ref[:, cut] for cut in cuts])
        upper = cat([col > row] * group)
        scores = lax.dot_general(q, keys, nt, preferred_element_type=jnp.float32)
        dprobs = lax.dot_general(go, values, nt, preferred_element_type=jnp.float32)

        def folded(x):
            return [jnp.where(upper, x[:, :tok], x[:, span:])] + [x[:, j * tok : (j + 1) * tok] for j in range(1, reach)]

        def unfolded(x):
            zero = jnp.zeros_like(x[0])
            parts = [jnp.where(upper, x[0], zero)] + x[1:] + [jnp.where(upper, zero, x[0])]
            return jnp.concatenate([part.astype(jnp.bfloat16) for part in parts], axis=1)

        masks = [cat([bias[...]] * group)] + [jnp.where(linear < reach - j, NEG, 0.0) for j in range(1, reach)]
        scores = [x * factor + mask for x, mask in zip(folded(scores), masks)]
        dprobs = folded(dprobs)
        top = jnp.max(functools.reduce(jnp.maximum, scores), axis=-1, keepdims=True)
        expd = [jnp.exp(x - top) for x in scores]
        scale = 1.0 / jnp.sum(functools.reduce(jnp.add, expd), axis=-1, keepdims=True)
        probs = [x * scale for x in expd]
        delta = jnp.sum(functools.reduce(jnp.add, [p * d for p, d in zip(probs, dprobs)]), axis=-1, keepdims=True)
        probs_b = unfolded(probs)
        dscores = unfolded([p * (d - delta) * factor for p, d in zip(probs, dprobs)])
        out = jnp.dot(probs_b, values, preferred_element_type=jnp.float32).astype(jnp.bfloat16)
        gq = jnp.dot(dscores, keys, preferred_element_type=jnp.float32).astype(jnp.bfloat16)
        for i, cut in enumerate(cuts):
            ao[:, cut] = out[i * tok : (i + 1) * tok]
            dq[:, cut] = gq[i * tok : (i + 1) * tok]
        dk = lax.dot_general(dscores, q, tn, preferred_element_type=jnp.float32)
        dv = lax.dot_general(probs_b, go, tn, preferred_element_type=jnp.float32)
        for side, value in ((0, dk), (HEAD, dv)):
            cut = slice(g * duo + side, g * duo + side + HEAD)
            for offset in range(1, reach + 1):
                back[offset - 1, :, cut] = value[(reach - offset) * tok : (reach - offset + 1) * tok].astype(jnp.bfloat16)
            own[:, cut] = value[span:]
        for offset in range(1, reach + 1):

            @pl.when(linear >= offset)
            def _():
                back_copy(g, offset, False).start()

    def cube_mask(h, step, which):
        return sum(1 << orders[h][k] for k in range(step) if which >> k & 1)

    def every_copy(g, h, step, which):
        block = every.at[flipped(s, cube_mask(h, step, which)), pl.ds(h * (tok // 2), tok // 2), chunk(g)]
        return remote(block, block, esend.at[0], erecv.at[g, step], flipped(s, 1 << orders[h][step]), z)

    def every_send(g, step):
        for which in range(1 << step):
            for h in range(2):
                every_copy(g, h, step, which).start()

    def every_pair(g, m, incoming):
        block = every.at[flipped(s, m | 1 if incoming else m), :, chunk(g)]
        return remote(block, block, fsend.at[0], frecv.at[g], sibling, z)

    def settle(g):
        for offset in range(1, reach + 1):

            @pl.when(linear + offset < devices)
            def _():
                back_copy(g, offset, True).wait_recv()

        cut = slice(g * duo, (g + 1) * duo)
        total = own[:, cut]
        seg = total
        for offset in range(1, reach + 1):
            piece = ret[offset - 1, :, cut].astype(jnp.float32)
            total = total + piece
            seg = seg + piece * jnp.where(z + offset < groups, 1.0, 0.0)
        every[s, :, cut] = total.astype(jnp.bfloat16)
        inside[:, cut] = seg.astype(jnp.bfloat16)
        every_send(g, 0)
        every_pair(g, 0, False).start()

    def widen(g):
        whole = every.at[0, :, chunk(g)]
        remote(whole, whole, esend.at[0], erecv.at[g, 0], s, z).wait_recv()
        every_send(g, 1)

    def share(g):
        whole = every.at[pl.ds(0, 2), :, chunk(g)]
        remote(whole, whole, esend.at[0], erecv.at[g, 1], s, z).wait_recv()
        for m in peers:
            every_pair(g, m, False).start()

    part_rows = unit // SPLIT

    def half_of(ref, g, d, q):
        return ref.at[g, d, pl.ds(q * part_rows, part_rows), :]

    def up_copy(g, d, q):
        return remote(half_of(ups, g, d, q), half_of(upr, g, d, q), usend.at[d], urecv.at[g, d, q], s, z + 1)

    def down_copy(g, d, q):
        return remote(half_of(dns, g, d, q), half_of(dnr, g, d, q), dsend.at[d], drecv.at[g, d, q], s, z - 1)

    def pass_on(g, d, up, adds):
        source, here, copy = (ups, upr, up_copy) if up else (dns, dnr, down_copy)
        for q in range(SPLIT):
            cut = slice(q * part_rows, (q + 1) * part_rows)
            value = part[g, d, cut]
            if adds:
                copy(g, d, q).wait_recv()
                value = value + here[g, d, cut].astype(jnp.float32)
            source[g, d, cut] = value.astype(jnp.bfloat16)
            copy(g, d, q).start()

    def hop(g, k):
        @pl.when(z == k)
        def _():
            for d in range(last, k, -1):
                pass_on(g, d, True, True)

        @pl.when(z == last - k)
        def _():
            for d in range(last - k):
                pass_on(g, d, False, True)

    def product(g):
        whole = every.at[pl.ds(0, seqs // 2), :, chunk(g)]
        remote(whole, whole, fsend.at[0], frecv.at[g], s, z).wait_recv()
        grads = every[:, :, g * duo : (g + 1) * duo].reshape(seqs * tok, duo)
        for i in range(groups):
            d = jnp.where(z == 0, last - i, i)
            rows_of = pl.ds(pl.multiple_of(d * unit, 128), unit)
            part[g, d] = jnp.dot(ht[rows_of, :], grads, preferred_element_type=jnp.float32)
            if i < last:

                @pl.when(z == 0)
                def _():
                    pass_on(g, last - i, True, False)

                @pl.when(z == last)
                def _():
                    pass_on(g, i, False, False)

    def grad_copy(g, h, step, which):
        at = flipped(s, cube_mask(h, step, which)) * unit + h * (unit // 2)
        block = wgb.at[g, pl.ds(pl.multiple_of(at, 16), unit // 2), :]
        return remote(block, block, wsend.at[0], wrecv.at[g, step], flipped(s, 1 << orders[h][step]), z)

    def grad_send(g, step):
        for which in range(1 << step):
            for h in range(2):
                grad_copy(g, h, step, which).start()

    def grad_pair(g, m, incoming):
        owner = flipped(s, m | 1 if incoming else m)
        block = wgb.at[g, pl.ds(pl.multiple_of(owner * unit, 128), unit), :]
        return remote(block, block, xsend.at[0], xrecv.at[g], sibling, z)

    def reduce(g):
        @pl.when(z > 0)
        def _():
            for q in range(SPLIT):
                up_copy(g, z, q).wait_recv()

        @pl.when(z < last)
        def _():
            for q in range(SPLIT):
                down_copy(g, z, q).wait_recv()

        total = part[g, z] + upr[g, z].astype(jnp.float32) + dnr[g, z].astype(jnp.float32)
        wgb[g, pl.ds(pl.multiple_of(s * unit, 128), unit), :] = total.astype(jnp.bfloat16)
        grad_send(g, 0)
        grad_pair(g, 0, False).start()

    def expand(g):
        whole = wgb.at[g, pl.ds(0, unit), :]
        remote(whole, whole, wsend.at[0], wrecv.at[g, 0], s, z).wait_recv()
        grad_send(g, 1)

    def relay(g):
        whole = wgb.at[g, pl.ds(0, 2 * unit), :]
        remote(whole, whole, wsend.at[0], wrecv.at[g, 1], s, z).wait_recv()
        for m in peers:
            grad_pair(g, m, False).start()

    def finish_chunk(g):
        whole = wgb.at[g, pl.ds(0, seqs // 2 * unit), :]
        remote(whole, whole, xsend.at[0], xrecv.at[g], s, z).wait_recv()

    def turn_hidden(d):
        hidden_wait(d)
        hb[s, d] = hid[:, pl.ds(pl.multiple_of(d * rows + s * unit, 128), unit)]
        for i in range(seqs):
            ht[d * unit : (d + 1) * unit, i * tok : (i + 1) * tok] = hb[i, d].T

    slices = 4
    span_cols = gh.shape[1] // slices
    tall = min(512, span_cols)

    def spread(i):
        def step(j, carry):
            at = pl.multiple_of(i * span_cols + j * tall, tall)
            total = jnp.zeros((tok, tall), jnp.float32)
            for g in range(heads):
                grads = inside[:, g * duo : (g + 1) * duo]
                total = total + lax.dot_general(grads, w_ref[g, pl.ds(at, tall), :], nt, preferred_element_type=jnp.float32)
            gh[:, pl.ds(at, tall)] = total.astype(jnp.bfloat16)
            return carry

        lax.fori_loop(0, span_cols // tall, step, 0)

    def drain(ref, sem):
        remote(ref, ref, sem, wrecv.at[0, 0], s, z).wait_send()

    def drain_weights():
        wide = len([g for g in range(heads) if g in WIDE])
        for shard in range(groups):
            moved = w_ref.at[0, pl.ds(0, unit * (heads + wide)), :]

            @pl.when((shard <= z) & (z < last))
            def _():
                drain(moved, zsend.at[1, shard])

            @pl.when((shard >= z) & (z > 0))
            def _():
                drain(moved, zsend.at[0, shard])

        turns = groups - 1
        plane = heads * (seqs // 2 - 1) - wide
        drain(w_ref.at[pl.ds(0, turns), pl.ds(0, unit * plane), :], qsend.at[0])
        drain(w_ref.at[pl.ds(0, turns), pl.ds(0, unit * heads * (seqs // 2)), :], csend.at[0])

    def drain_tokens():
        drain(hb.at[pl.ds(0, seqs - 1)], hsend.at[0])
        for offset in range(1, reach + 1):

            @pl.when(linear + offset < devices)
            def _():
                drain(ret.at[offset - 1], ksend.at[offset - 1])

            @pl.when(linear >= offset)
            def _():
                drain(ret.at[offset - 1], bsend.at[offset - 1])

        drain(every.at[pl.ds(0, len(peers))], esend.at[0])
        drain(every.at[pl.ds(0, seqs // 2)], fsend.at[0])

    works = [own_send, forward, begin, cube_next, pair_send_after, pair_wait, project_chunk, attend_chunk, settle, widen, share]
    works += [product, hop, reduce, expand, relay, finish_chunk, spread, hidden_send, turn_hidden]
    fetched = False
    for place, *places in ORDER:
        if works[place] is attend_chunk and not fetched:
            loads[2].wait()
            loads[3].wait()
            fetched = True
        works[place](*places)
    drain_weights()
    drain_tokens()
    drain(wgb.at[:, pl.ds(0, len(peers) * unit), :], wsend.at[0])
    drain(wgb.at[:, pl.ds(0, seqs // 2 * unit), :], xsend.at[0])
    for d in range(groups):

        @pl.when(d > z)
        def _():
            drain(ups.at[:, d], usend.at[d])

        @pl.when(d < z)
        def _():
            drain(dns.at[:, d], dsend.at[d])


def fused(hidden, kv_blocks, kv_scale, queries, grad_out, reach):
    seqs = lax.axis_size("seq")
    groups = lax.axis_size("fsdp")
    tok, depth = hidden.shape
    rows, cols = kv_blocks.shape
    width = queries.shape[1]
    unit = rows // seqs
    heads = cols // (2 * HEAD)
    duo = 2 * HEAD
    count = (reach + 1) * tok
    bits = seqs.bit_length() - 1
    any_space = pl.BlockSpec(memory_space=pl.ANY)
    dma = pltpu.SemaphoreType.DMA
    b16 = lambda *shape: pltpu.VMEM(shape, jnp.bfloat16)
    f32 = lambda *shape: pltpu.VMEM(shape, jnp.float32)
    return pl.pallas_call(
        functools.partial(fused_kernel, seqs, groups, reach),
        out_shape=[b16(tok, width), b16(tok, width), b16(tok, depth), b16(heads, rows, duo)],
        in_specs=[any_space, any_space, pl.BlockSpec(memory_space=pltpu.SMEM), any_space, any_space],
        out_specs=[pl.BlockSpec(memory_space=pltpu.VMEM)] * 4,
        scratch_shapes=[
            b16(tok, depth), b16(rows, cols), b16(tok, width), b16(tok, width),
            b16(heads, depth, duo), b16(count, cols),
            b16(reach, tok, cols), b16(reach, tok, cols), f32(tok, cols), b16(seqs, tok, cols), b16(tok, cols),
            b16(seqs, groups, tok, unit), b16(groups * unit, seqs * tok), f32(heads, groups, unit, duo),
            b16(heads, groups, unit, duo), b16(heads, groups, unit, duo), b16(heads, groups, unit, duo), b16(heads, groups, unit, duo),
            f32(tok, tok), b16(unit, cols),
            dma((5,)), dma((2, groups)), dma((groups, heads)),
            dma((1,)), dma((groups - 1, heads, bits - 1)), dma((1,)), dma((groups - 1, heads)), dma((1,)), dma((groups,)),
            dma((reach,)), dma((heads, reach)), dma((reach,)), dma((heads, reach)),
            dma((1,)), dma((heads, 2)), dma((1,)), dma((heads,)),
            dma((groups,)), dma((heads, groups, SPLIT)), dma((groups,)), dma((heads, groups, SPLIT)),
            dma((1,)), dma((heads, 2)), dma((1,)), dma((heads,)),
        ],
        compiler_params=pltpu.CompilerParams(collective_id=0, has_side_effects=True, vmem_limit_bytes=VMEM_LIMIT),
        name="fused",
    )(hidden, kv_blocks, kv_scale.T, queries, grad_out)


def write_kernel(ao, dq, gh, wgb, ao_out, dq_out, gh_out, wg_out, wide, osem):
    parts, size, cols = wide.shape
    heads = wgb.shape[0]
    triples = ((ao, ao_out), (dq, dq_out), (gh, gh_out))
    stores = [pltpu.make_async_copy(src, dst, osem.at[parts + k]) for k, (src, dst) in enumerate(triples)]
    for copy in stores:
        copy.start()
    for p in range(parts):
        for g in range(heads):
            block = wgb[g, p * size : (p + 1) * size, :].astype(jnp.float32)
            wide[p, :, g * HEAD : (g + 1) * HEAD] = block[:, :HEAD]
            wide[p, :, (heads + g) * HEAD : (heads + g + 1) * HEAD] = block[:, HEAD:]
        store = pltpu.make_async_copy(wide.at[p], wg_out.at[pl.ds(p * size, size), :], osem.at[p])
        store.start()
        stores.append(store)
    for copy in stores:
        copy.wait()


def write(ao, dq, gh, wgb):
    parts = 8
    heads, rows, duo = wgb.shape
    any_space = pl.BlockSpec(memory_space=pl.ANY)
    return pl.pallas_call(
        write_kernel,
        out_shape=[jax.ShapeDtypeStruct(x.shape, x.dtype) for x in (ao, dq, gh)]
        + [jax.ShapeDtypeStruct((rows, heads * duo), jnp.float32)],
        in_specs=[pl.BlockSpec(memory_space=pltpu.VMEM)] * 4,
        out_specs=[any_space] * 4,
        scratch_shapes=[pltpu.VMEM((parts, rows // parts, heads * duo), jnp.float32), pltpu.SemaphoreType.DMA((parts + 3,))],
        compiler_params=pltpu.CompilerParams(vmem_limit_bytes=12 << 20),
        name="write",
    )(ao, dq, gh, wgb)


def body(hidden, kv_blocks, kv_scale, queries, grad_out):
    tok = hidden.shape[0]
    groups = lax.axis_size("fsdp")
    reach = groups // 2
    unit = kv_blocks.shape[0] // lax.axis_size("seq")
    heads = kv_blocks.shape[1] // (2 * HEAD)
    if unit % QB == 0 and (heads, groups, lax.axis_size("seq")) == PLANNED:
        outs = fused(hidden, kv_blocks, kv_scale, queries, grad_out, reach)
        return tuple(write(*outs))
    weights, kv, columns = project(hidden, kv_blocks, kv_scale)
    pieces = []
    for offset in range(reach, 0, -1):
        pieces.append(shifted(kv, ("seq", "fsdp"), offset))
    window = jnp.concatenate(pieces + [kv], axis=0)
    columns = columns.reshape(groups * tok, columns.shape[2])
    attn_out, grad_queries, dwin = attend(queries, window, grad_out, reach)
    back = dwin[: reach * tok].astype(jnp.bfloat16)
    own = dwin[reach * tok :]
    grad_hidden, weight_grad = finish(back, own, weights, columns, reach)
    return (attn_out, grad_queries, grad_hidden, weight_grad.astype(jnp.float32))


def solution(mesh):
    return jax.shard_map(
        body,
        mesh=mesh,
        in_specs=(
            P(("seq", "fsdp"), None),
            P("fsdp", None),
            P("fsdp", None),
            P(("seq", "fsdp"), None),
            P(("seq", "fsdp"), None),
        ),
        out_specs=(
            P(("seq", "fsdp"), None),
            P(("seq", "fsdp"), None),
            P(("seq", "fsdp"), None),
            P("fsdp", None),
        ),
        check_vma=False,
    )
```

```python
import functools

import jax
import jax.numpy as jnp
from jax import lax
from jax.experimental import pallas as pl
from jax.experimental.pallas import tpu as pltpu
from jax.sharding import PartitionSpec as P

HEADS = 32
KV_HEADS = 4
HEAD = 128
QB = 128


NEG = -1e30
PLANNED = (4, 4, 8)
(SEND, FORWARD, BEGIN, CUBE, PAIR, LAND, PROJECT, ATTEND, SETTLE, WIDEN, SHARE) = range(11)
(PRODUCT, HOP, REDUCE, EXPAND, RELAY, FINISH, SPREAD, HIDDEN, TURN) = range(11, 20)
VMEM_LIMIT = 51 << 20
SPLIT = 2
WIDE = (2,)
ORDER = (
    (SEND, 2), (FORWARD, 1, 0), (FORWARD, 0, 0), (BEGIN, 0, 0), (HIDDEN, 2), (FORWARD, 1, 2), (CUBE, 0, 0),
    (BEGIN, 1, 0), (FORWARD, 0, 2), (FORWARD, 2, 0), (BEGIN, 0, 2), (FORWARD, 2, 2), (SEND, 1), (BEGIN, 1, 2),
    (BEGIN, 2, 0), (SEND, 3), (CUBE, 1, 0), (FORWARD, 1, 3), (BEGIN, 2, 2), (FORWARD, 0, 3), (FORWARD, 0, 1),
    (PAIR, 1, 2), (FORWARD, 1, 1), (PAIR, 1, 0), (CUBE, 2, 0), (BEGIN, 0, 3), (FORWARD, 2, 3), (PAIR, 2, 2),
    (BEGIN, 0, 1), (PAIR, 0, 0), (TURN, 0), (LAND, 1, 0), (BEGIN, 1, 3), (PAIR, 0, 2), (LAND, 1, 2), (LAND, 0, 0),
    (PAIR, 2, 0), (CUBE, 0, 3), (LAND, 2, 2), (LAND, 2, 0), (TURN, 2), (LAND, 0, 2), (FORWARD, 2, 1), (CUBE, 0, 1),
    (PROJECT, 2), (PROJECT, 0), (BEGIN, 2, 3), (PAIR, 0, 3), (BEGIN, 2, 1), (CUBE, 1, 3), (BEGIN, 1, 1), (CUBE, 2, 3),
    (ATTEND, 2), (PAIR, 1, 3), (CUBE, 1, 1), (ATTEND, 0), (PAIR, 0, 1), (CUBE, 2, 1), (PAIR, 2, 3), (SETTLE, 2),
    (HIDDEN, 3), (LAND, 2, 3), (LAND, 1, 3), (LAND, 0, 3), (PROJECT, 3), (PAIR, 1, 1), (PAIR, 2, 1), (WIDEN, 2),
    (LAND, 0, 1), (LAND, 1, 1), (LAND, 2, 1), (PROJECT, 1), (HIDDEN, 1), (ATTEND, 3), (SHARE, 2), (ATTEND, 1),
    (TURN, 3), (SETTLE, 0), (TURN, 1), (PRODUCT, 2), (WIDEN, 0), (SETTLE, 3), (SETTLE, 1), (HOP, 2, 1), (WIDEN, 3),
    (HOP, 2, 2), (SHARE, 0), (SPREAD, 2), (PRODUCT, 0), (REDUCE, 2), (SHARE, 3), (WIDEN, 1), (HOP, 0, 1), (EXPAND, 2),
    (PRODUCT, 3), (SHARE, 1), (HOP, 0, 2), (REDUCE, 0), (HOP, 3, 1), (PRODUCT, 1), (HOP, 3, 2), (EXPAND, 0),
    (RELAY, 2), (REDUCE, 3), (HOP, 1, 1), (HOP, 1, 2), (EXPAND, 3), (SPREAD, 0), (FINISH, 2), (REDUCE, 1),
    (SPREAD, 3), (EXPAND, 1), (RELAY, 3), (RELAY, 0), (SPREAD, 1), (RELAY, 1), (FINISH, 3), (FINISH, 0), (FINISH, 1),
)


def shifted(block, axis, distance):
    devices = range(lax.axis_size(axis))
    route = [(i - distance, i) for i in devices if i - distance in devices]
    return lax.ppermute(block, axis, route)


def attend_kernel(reach, q_ref, g_ref, k_ref, v_ref, out_ref, dq_ref, dk_ref, dv_ref):
    tok = q_ref.shape[0]
    group = q_ref.shape[1] // HEAD
    count = k_ref.shape[0]
    span = reach * tok
    factor = 1.0 / float(HEAD) ** 0.5
    base = (lax.axis_index("seq") * lax.axis_size("fsdp") + lax.axis_index("fsdp")) * tok
    row = lax.broadcasted_iota(jnp.int32, (tok, count), 0)
    col = lax.broadcasted_iota(jnp.int32, (tok, count), 1)
    allowed = (col > row) & (col <= row + span) & (col >= span - base)
    keys = k_ref[...]
    values = v_ref[...]
    nt = (((1,), (1,)), ((), ()))
    tn = (((0,), (0,)), ((), ()))
    ps, ds, qs, gs = [], [], [], []
    for h in range(group):
        cut = slice(h * HEAD, (h + 1) * HEAD)
        q = q_ref[:, cut]
        g = g_ref[:, cut]
        scores = lax.dot_general(q, keys, nt, preferred_element_type=jnp.float32) * factor
        scores = jnp.where(allowed, scores, NEG)
        expd = jnp.exp(scores - jnp.max(scores, axis=-1, keepdims=True))
        probs = expd * (1.0 / jnp.sum(expd, axis=-1, keepdims=True))
        probs_b = probs.astype(jnp.bfloat16)
        out_ref[:, cut] = jnp.dot(probs_b, values, preferred_element_type=jnp.float32).astype(jnp.bfloat16)
        dprobs = lax.dot_general(g, values, nt, preferred_element_type=jnp.float32)
        delta = jnp.sum(probs * dprobs, axis=-1, keepdims=True)
        dscores = (probs * (dprobs - delta) * factor).astype(jnp.bfloat16)
        dq_ref[:, cut] = jnp.dot(dscores, keys, preferred_element_type=jnp.float32).astype(jnp.bfloat16)
        ps.append(probs_b)
        ds.append(dscores)
        qs.append(q)
        gs.append(g)
    cat = lambda parts: jnp.concatenate(parts, axis=0)
    dk_ref[...] = lax.dot_general(cat(ds), cat(qs), tn, preferred_element_type=jnp.float32)
    dv_ref[...] = lax.dot_general(cat(ps), cat(gs), tn, preferred_element_type=jnp.float32)


def attend(queries, window, grad_out, reach):
    tok, width = queries.shape
    count = window.shape[0]
    heads = window.shape[1] // (2 * HEAD)
    wide = pl.BlockSpec((tok, width // heads), lambda i: (0, i))
    key = pl.BlockSpec((count, HEAD), lambda i: (0, i))
    value = pl.BlockSpec((count, HEAD), lambda i: (0, i + heads))
    out, dq, dk, dv = pl.pallas_call(
        functools.partial(attend_kernel, reach),
        grid=(heads,),
        in_specs=[wide, wide, key, value],
        out_specs=[wide, wide, key, key],
        out_shape=[
            jax.ShapeDtypeStruct((tok, width), jnp.bfloat16),
            jax.ShapeDtypeStruct((tok, width), jnp.bfloat16),
            jax.ShapeDtypeStruct((count, heads * HEAD), jnp.float32),
            jax.ShapeDtypeStruct((count, heads * HEAD), jnp.float32),
        ],
        cost_estimate=pl.CostEstimate(flops=12 * tok * width * count, bytes_accessed=8 * tok * width, transcendentals=0),
        name="attend",
    )(queries, grad_out, window, window)
    return out, dq, jnp.concatenate([dk, dv], axis=1)


def flipped(index, mask):
    for place in range(mask.bit_length()):
        if mask >> place & 1:
            index = index + (1 << place) * (1 - 2 * (index // (1 << place) % 2))
    return index


def orders_of(bits):
    return (list(range(1, bits)) + [0], list(range(bits - 1, 0, -1)) + [0])


def project_kernel(seqs, groups, hid_ref, blk_ref, sc_ref, out_ref, kv_ref, col_ref, w_ref, acc, zsend, zrecv, qsend, qrecv, csend, crecv, wsem):
    s = lax.axis_index("seq")
    z = lax.axis_index("fsdp")
    rows = blk_ref.shape[0]
    unit = rows // seqs
    half = unit // 2
    bits = seqs.bit_length() - 1
    chunk = min(512, rows)

    def scale_block(i, carry):
        at = pl.multiple_of(i * QB, QB)
        block = blk_ref[pl.ds(at, QB), :].astype(jnp.float32) * sc_ref[pl.ds(i, 1), :]
        w_ref[pl.ds(pl.multiple_of(z * rows + at, QB), QB), :] = block.astype(jnp.bfloat16)
        return carry

    lax.fori_loop(0, rows // QB, scale_block, 0)

    def line_copy(shard, up):
        piece = w_ref.at[pl.ds(pl.multiple_of(shard * rows + s * unit, 16), unit), :]
        return pltpu.make_async_remote_copy(
            src_ref=piece,
            dst_ref=piece,
            send_sem=zsend.at[up, shard],
            recv_sem=zrecv.at[shard],
            device_id=(s, z + 1 if up else z - 1),
            device_id_type=pl.DeviceIdType.MESH,
        )

    def cube_copy(turn, shard, order, step, which, incoming):
        bit = order[step]
        mask = 0
        for k in range(step):
            if which >> k & 1:
                mask |= 1 << order[k]
        h = 0 if order is orders[0] else 1
        owner = flipped(s, mask | (1 << bit) if incoming else mask)
        piece = w_ref.at[pl.ds(pl.multiple_of(shard * rows + owner * unit + h * half, 16), half), :]
        slot = (1 << step) - 1 + which
        return pltpu.make_async_remote_copy(
            src_ref=piece,
            dst_ref=piece,
            send_sem=qsend.at[turn, h, slot],
            recv_sem=qrecv.at[turn, h, slot],
            device_id=(flipped(s, 1 << bit), z),
            device_id_type=pl.DeviceIdType.MESH,
        )

    orders = orders_of(bits)
    near = jnp.minimum(z, groups - 1 - z)

    def shard_at(turn):
        step = turn // 2 + 1
        paired = z - step if turn % 2 == 0 else z + step
        far = turn - near + 1
        single = jnp.where(z > groups - 1 - z, z - far, z + far)
        return jnp.where(turn < 2 * near, paired, single)

    shards = [shard_at(turn) for turn in range(groups - 1)]

    @pl.when(z < groups - 1)
    def _():
        line_copy(z, 1).start()

    @pl.when(z > 0)
    def _():
        line_copy(z, 0).start()

    def column_copy(gap, incoming):
        other = (z - gap + groups) % groups if incoming else (z + gap) % groups
        part = pl.multiple_of(other * rows, 128)
        return pltpu.make_async_remote_copy(
            src_ref=hid_ref.at[:, pl.ds(part, rows)],
            dst_ref=col_ref.at[other if incoming else z],
            send_sem=csend.at[gap - 1],
            recv_sem=crecv.at[gap - 1],
            device_id=(s, other),
            device_id_type=pl.DeviceIdType.MESH,
        )

    acc[...] = jnp.zeros_like(acc)

    def store_copy(turn, shard):
        part = pl.ds(pl.multiple_of(shard * rows, 16), rows)
        return pltpu.make_async_copy(w_ref.at[part, :], out_ref.at[part, :], wsem.at[turn])

    def multiply(shard):
        def part(i, carry):
            at = pl.multiple_of(shard * rows + i * chunk, 128)
            acc[...] += jnp.dot(
                hid_ref[:, pl.ds(at, chunk)], w_ref[pl.ds(at, chunk), :], preferred_element_type=jnp.float32
            )
            return carry

        lax.fori_loop(0, rows // chunk, part, 0)

    multiply(z)
    store_copy(groups - 1, z).start()
    col_ref[z] = hid_ref[:, pl.ds(pl.multiple_of(z * rows, 128), rows)]
    for tick in range(groups - 1 + bits):
        for stage in range(bits, -1, -1):
            turn = tick - stage
            if turn < 0 or turn >= groups - 1:
                continue
            shard = shards[turn]
            if stage == 0:
                line_copy(shard, 0).wait_recv()

                @pl.when((shard < z) & (z < groups - 1))
                def _():
                    line_copy(shard, 1).start()

                @pl.when((shard > z) & (z > 0))
                def _():
                    line_copy(shard, 0).start()
            else:
                for order in orders:
                    for which in range(1 << (stage - 1)):
                        cube_copy(turn, shard, order, stage - 1, which, True).wait_recv()
            if stage < bits:
                for order in orders:
                    for which in range(1 << stage):
                        cube_copy(turn, shard, order, stage, which, False).start()
            else:
                multiply(shard)
                store_copy(turn, shard).start()
        if tick == groups - 2:
            for gap in range(1, groups):
                column_copy(gap, False).start()
    kv_ref[...] = acc[...].astype(jnp.bfloat16)
    for turn in range(groups - 1):
        store_copy(turn, shards[turn]).wait()
    store_copy(groups - 1, z).wait()
    for gap in range(1, groups):
        column_copy(gap, True).wait_recv()
        column_copy(gap, False).wait_send()
    for shard in range(groups):

        @pl.when((shard <= z) & (z < groups - 1))
        def _():
            line_copy(shard, 1).wait_send()

        @pl.when((shard >= z) & (z > 0))
        def _():
            line_copy(shard, 0).wait_send()

    for turn in range(groups - 1):
        for order in orders:
            for stage in range(bits):
                for which in range(1 << stage):
                    cube_copy(turn, shards[turn], order, stage, which, False).wait_send()


def project(hidden, kv_blocks, kv_scale):
    seqs = lax.axis_size("seq")
    groups = lax.axis_size("fsdp")
    tok, width = hidden.shape
    cols = kv_blocks.shape[1]
    spread = jnp.repeat(kv_scale, QB, axis=1)
    vmem = pl.BlockSpec(memory_space=pltpu.VMEM)
    return pl.pallas_call(
        functools.partial(project_kernel, seqs, groups),
        out_shape=[
            jax.ShapeDtypeStruct((width, cols), jnp.bfloat16),
            jax.ShapeDtypeStruct((tok, cols), jnp.bfloat16),
            jax.ShapeDtypeStruct((groups, tok, kv_blocks.shape[0]), jnp.bfloat16),
        ],
        in_specs=[vmem] * 3,
        out_specs=[pl.BlockSpec(memory_space=pl.ANY), vmem, vmem],
        scratch_shapes=[
            pltpu.VMEM((width, cols), jnp.bfloat16),
            pltpu.VMEM((tok, cols), jnp.float32),
            pltpu.SemaphoreType.DMA((2, groups)),
            pltpu.SemaphoreType.DMA((groups,)),
            pltpu.SemaphoreType.DMA((groups - 1, 2, seqs - 1)),
            pltpu.SemaphoreType.DMA((groups - 1, 2, seqs - 1)),
            pltpu.SemaphoreType.DMA((groups - 1,)),
            pltpu.SemaphoreType.DMA((groups - 1,)),
            pltpu.SemaphoreType.DMA((groups,)),
        ],
        compiler_params=pltpu.CompilerParams(has_side_effects=True),
        name="project",
    )(hidden, kv_blocks, spread)


def finish_kernel(
    seqs, groups, reach, back_ref, own_ref, in_ref, col_ref, gh_ref, wg_ref,
    w_ref, wsem, ret, every, inside, acc, sends, recvs, hsend, hrecv, gsend, grecv, rsend, rrecv, asend, arecv,
):
    s = lax.axis_index("seq")
    z = lax.axis_index("fsdp")
    linear = s * groups + z
    devices = seqs * groups
    tok, cols = own_ref.shape
    rows = col_ref.shape[1]
    bits = seqs.bit_length() - 1
    mesh_id = pl.DeviceIdType.MESH
    load = pltpu.make_async_copy(in_ref, w_ref, wsem)
    load.start()

    def halo_copy(offset, incoming):
        other = linear + offset if incoming else linear - offset
        return pltpu.make_async_remote_copy(
            src_ref=back_ref.at[pl.ds((reach - offset) * tok, tok), :],
            dst_ref=ret.at[offset - 1],
            send_sem=hsend.at[offset - 1],
            recv_sem=hrecv.at[offset - 1],
            device_id=(other // groups, other % groups),
            device_id_type=mesh_id,
        )

    for offset in range(1, reach + 1):

        @pl.when(linear >= offset)
        def _():
            halo_copy(offset, False).start()

    for offset in range(1, reach + 1):

        @pl.when(linear + offset < devices)
        def _():
            halo_copy(offset, True).wait_recv()

        @pl.when(linear + offset >= devices)
        def _():
            ret[offset - 1] = jnp.zeros((tok, cols), jnp.bfloat16)

    total = own_ref[...]
    seg = total
    for offset in range(1, reach + 1):
        piece = ret[offset - 1].astype(jnp.float32)
        total = total + piece
        seg = seg + piece * jnp.where(z + offset < groups, 1.0, 0.0)
    every[z] = total.astype(jnp.bfloat16)
    inside[...] = seg.astype(jnp.bfloat16)

    def gather_copy(gap, incoming):
        other = (z - gap + groups) % groups if incoming else (z + gap) % groups
        block = every.at[other if incoming else z]
        return pltpu.make_async_remote_copy(
            src_ref=block,
            dst_ref=block,
            send_sem=gsend.at[gap - 1],
            recv_sem=grecv.at[gap - 1],
            device_id=(s, other),
            device_id_type=mesh_id,
        )

    for gap in range(1, groups):
        gather_copy(gap, False).start()

    load.wait()
    wide = 512

    def spread(i, carry):
        at = pl.multiple_of(i * wide, wide)
        gh_ref[:, pl.ds(at, wide)] = lax.dot_general(
            inside[...], w_ref[pl.ds(at, wide), :], (((1,), (1,)), ((), ())), preferred_element_type=jnp.float32
        ).astype(jnp.bfloat16)
        return carry

    lax.fori_loop(0, w_ref.shape[0] // wide, spread, 0)
    for gap in range(1, groups):
        gather_copy(gap, True).wait_recv()

    big = rows // 2
    tile = min(256, big)
    low = s % 2
    sibling = flipped(s, 1)
    grads = every[...].reshape(groups * tok, cols)

    def product(at):
        return lax.dot_general(
            col_ref[:, pl.ds(at, tile)], grads, (((0,), (0,)), ((), ())), preferred_element_type=jnp.float32
        )

    def theirs(i, carry):
        at = pl.multiple_of(i * tile, tile)
        sends[0][pl.ds(at, tile), :] = product(pl.multiple_of((1 - low) * big + at, tile)).astype(jnp.bfloat16)
        return carry

    lax.fori_loop(0, big // tile, theirs, 0)

    def reduce_copy(step, h, peer):
        cut = slice(None) if h is None else pl.ds(h * (cols // 2), cols // 2)
        return pltpu.make_async_remote_copy(
            src_ref=sends[step].at[:, cut] if h is not None else sends[step],
            dst_ref=recvs[step].at[:, cut] if h is not None else recvs[step],
            send_sem=rsend.at[step, h or 0],
            recv_sem=rrecv.at[step, h or 0],
            device_id=(peer, z),
            device_id_type=mesh_id,
        )

    reduce_copy(0, None, sibling).start()

    def mine(i, carry):
        at = pl.multiple_of(i * tile, tile)
        acc[pl.ds(at, tile), :] = product(pl.multiple_of(low * big + at, tile))
        return carry

    lax.fori_loop(0, big // tile, mine, 0)
    reduce_copy(0, None, sibling).wait_recv()

    def fold(i, carry):
        at = pl.multiple_of(i * tile, tile)
        acc[pl.ds(at, tile), :] += recvs[0][pl.ds(at, tile), :].astype(jnp.float32)
        return carry

    lax.fori_loop(0, big // tile, fold, 0)
    orders = (list(range(1, bits)), list(range(bits - 1, 0, -1)))
    offsets = [[0], [0]]
    side = cols // 2
    for step in range(1, bits):
        size = rows >> (step + 1)
        for h in range(2):
            place = orders[h][step - 1]
            bit = s // (1 << place) % 2
            start = offsets[h][-1]
            away = pl.multiple_of(start + (1 - bit) * size, 16)
            sends[step][:, h * side : (h + 1) * side] = acc[
                pl.ds(away, size), h * side : (h + 1) * side
            ].astype(jnp.bfloat16)
            reduce_copy(step, h, flipped(s, 1 << place)).start()
            offsets[h].append(start + bit * size)
        for h in range(2):
            place = orders[h][step - 1]
            reduce_copy(step, h, flipped(s, 1 << place)).wait_recv()
            keep = pl.ds(pl.multiple_of(offsets[h][-1], 16), size)
            cut = slice(h * side, (h + 1) * side)
            acc[keep, cut] += recvs[step][:, cut].astype(jnp.float32)
    size = rows >> bits
    for h in range(2):
        at = offsets[h][-1]
        cut = slice(h * side, (h + 1) * side)
        wg_ref[pl.ds(pl.multiple_of(low * big + at, 16), size), cut] = acc[
            pl.ds(pl.multiple_of(at, 16), size), cut
        ].astype(jnp.bfloat16)

    def spread_copy(step, h, incoming):
        place = orders[h][step - 1]
        bit = s // (1 << place) % 2
        size = rows >> (step + 1)
        at = low * big + offsets[h][step - 1] + ((1 - bit) if incoming else bit) * size
        block = wg_ref.at[pl.ds(pl.multiple_of(at, 16), size), pl.ds(h * side, side)]
        return pltpu.make_async_remote_copy(
            src_ref=block,
            dst_ref=block,
            send_sem=asend.at[step, h],
            recv_sem=arecv.at[step, h],
            device_id=(flipped(s, 1 << place), z),
            device_id_type=mesh_id,
        )

    for step in range(bits - 1, 0, -1):
        for h in range(2):
            spread_copy(step, h, False).start()
        for h in range(2):
            spread_copy(step, h, True).wait_recv()

    def last_copy(incoming):
        block = wg_ref.at[pl.ds(pl.multiple_of(((1 - low) if incoming else low) * big, 16), big), :]
        return pltpu.make_async_remote_copy(
            src_ref=block,
            dst_ref=block,
            send_sem=asend.at[0, 0],
            recv_sem=arecv.at[0, 0],
            device_id=(sibling, z),
            device_id_type=mesh_id,
        )

    last_copy(False).start()
    last_copy(True).wait_recv()
    for offset in range(1, reach + 1):

        @pl.when(linear >= offset)
        def _():
            halo_copy(offset, False).wait_send()

    for gap in range(1, groups):
        gather_copy(gap, False).wait_send()
    reduce_copy(0, None, sibling).wait_send()
    for step in range(1, bits):
        for h in range(2):
            reduce_copy(step, h, flipped(s, 1 << orders[h][step - 1])).wait_send()
            spread_copy(step, h, False).wait_send()
    last_copy(False).wait_send()


def finish(back, own, weights, columns, reach):
    seqs = lax.axis_size("seq")
    groups = lax.axis_size("fsdp")
    tok, cols = own.shape
    rows = columns.shape[1]
    bits = seqs.bit_length() - 1
    vmem = pl.BlockSpec(memory_space=pltpu.VMEM)
    steps = [pltpu.VMEM((rows >> (k + 1), cols), jnp.bfloat16) for k in range(bits)]
    dma = pltpu.SemaphoreType.DMA
    return pl.pallas_call(
        functools.partial(finish_kernel, seqs, groups, reach),
        out_shape=[
            jax.ShapeDtypeStruct((tok, weights.shape[0]), jnp.bfloat16),
            jax.ShapeDtypeStruct((rows, cols), jnp.bfloat16),
        ],
        in_specs=[vmem, vmem, pl.BlockSpec(memory_space=pl.ANY), vmem],
        out_specs=[vmem] * 2,
        scratch_shapes=[
            pltpu.VMEM(weights.shape, jnp.bfloat16),
            dma(()),
            pltpu.VMEM((reach, tok, cols), jnp.bfloat16),
            pltpu.VMEM((groups, tok, cols), jnp.bfloat16),
            pltpu.VMEM((tok, cols), jnp.bfloat16),
            pltpu.VMEM((rows // 2, cols), jnp.float32),
            steps,
            steps,
            dma((reach,)),
            dma((reach,)),
            dma((groups - 1,)),
            dma((groups - 1,)),
            dma((bits, 2)),
            dma((bits, 2)),
            dma((bits, 2)),
            dma((bits, 2)),
        ],
        compiler_params=pltpu.CompilerParams(has_side_effects=True),
        name="finish",
    )(back, own, weights, columns)


def fused_kernel(
    seqs, groups, reach,
    hid_in, blk_in, sc_ref, q_in, g_in, ao, dq, gh, wgb,
    hid, blk, q_ref, g_ref, w_ref, win, back, ret, own, every, inside, hb, ht, part,
    ups, upr, dns, dnr, bias, lead_ref, sums,
    lsem, zsend, zrecv, qsend, qrecv, csend, crecv, hsend, hrecv, ksend, krecv, bsend, brecv,
    esend, erecv, fsend, frecv, usend, urecv, dsend, drecv, wsend, wrecv, xsend, xrecv,
):
    s = lax.axis_index("seq")
    z = lax.axis_index("fsdp")
    linear = s * groups + z
    devices = seqs * groups
    tok, width = hid.shape
    rows, cols = blk.shape
    unit = rows // seqs
    bits = seqs.bit_length() - 1
    heads = cols // (2 * HEAD)
    duo = 2 * HEAD
    group = q_ref.shape[1] // HEAD // heads
    span = reach * tok
    last = groups - 1
    sibling = flipped(s, 1)
    peers = [m << 1 for m in range(1, seqs // 2)]
    nt = (((1,), (1,)), ((), ()))
    tn = (((0,), (0,)), ((), ()))
    mesh_id = pl.DeviceIdType.MESH

    def chunk(g):
        return pl.ds(g * duo, duo)

    def remote(src, dst, send, recv, to_s, to_z):
        return pltpu.make_async_remote_copy(
            src_ref=src, dst_ref=dst, send_sem=send, recv_sem=recv, device_id=(to_s, to_z), device_id_type=mesh_id
        )

    barrier = pltpu.get_barrier_semaphore()
    partners = [(None, flipped(s, m), z) for m in range(1, seqs)]
    partners += [(z < last, s, z + 1), (z > 0, s, z - 1)]
    for offset in range(1, reach + 1):
        up, down = linear + offset, linear - offset
        partners.append((up < devices, up // groups, up % groups))
        partners.append((down >= 0, down // groups, down % groups))

    def greet(to_s, to_z):
        pl.semaphore_signal(barrier, inc=1, device_id=(to_s, to_z), device_id_type=mesh_id)

    for present, to_s, to_z in partners:
        if present is None:
            greet(to_s, to_z)
        else:
            pl.when(present)(functools.partial(greet, to_s, to_z))

    mine = pl.ds(pl.multiple_of(s * unit, 16), unit)
    first = pltpu.make_async_copy(blk_in.at[mine, :], lead_ref, lsem.at[0])
    first.start()
    loads = [
        pltpu.make_async_copy(blk_in, blk, lsem.at[1]),
        pltpu.make_async_copy(hid_in, hid, lsem.at[2]),
        pltpu.make_async_copy(q_in, q_ref, lsem.at[3]),
        pltpu.make_async_copy(g_in, g_ref, lsem.at[4]),
    ]
    loads[1].start()

    def scale_block(i, source, at):
        to = pl.ds(pl.multiple_of(z * rows + i * QB, QB), QB)
        for j in range(cols // QB):
            block = source[pl.ds(at, QB), j * QB : (j + 1) * QB].astype(jnp.float32) * sc_ref[j, i]
            side = j // heads * HEAD
            w_ref[j % heads, to, side : side + HEAD] = block.astype(jnp.bfloat16)

    near = jnp.minimum(z, last - z)

    def shard_at(turn):
        step = turn // 2 + 1
        paired = z - step if turn % 2 == 0 else z + step
        far = turn - near + 1
        single = jnp.where(z > last - z, z - far, z + far)
        return jnp.where(turn < 2 * near, paired, single)

    shards = [shard_at(turn) for turn in range(groups - 1)]
    orders = (list(range(1, bits)), list(range(bits - 1, 0, -1)))

    def span_of(g, shard, owner, h=None):
        at = shard * rows + owner * unit + (0 if h is None else h * (unit // 2))
        return w_ref.at[g, pl.ds(pl.multiple_of(at, 16), unit if h is None else unit // 2), :]

    def kinds(g):
        return range(3 if g in WIDE else 1)

    def line_copy(shard, up, g, kind):
        if kind == 0:
            piece = span_of(g, shard, s)
        else:
            piece = span_of(g, shard, flipped(s, 1 << orders[kind - 1][0]), kind - 1)
        return remote(piece, piece, zsend.at[up, shard], zrecv.at[shard, g], s, z + 1 if up else z - 1)

    def cube_copy(turn, g, h, step, which, incoming):
        order = orders[h]
        bit = order[step]
        mask = 0
        for k in range(step):
            if which >> k & 1:
                mask |= 1 << order[k]
        piece = span_of(g, shards[turn], flipped(s, mask | (1 << bit) if incoming else mask), h)
        return remote(piece, piece, qsend.at[0], qrecv.at[turn, g, step], flipped(s, 1 << bit), z)

    def pair_copy(turn, g, m, incoming):
        piece = span_of(g, shards[turn], flipped(s, (m << 1) | 1 if incoming else m << 1))
        return remote(piece, piece, csend.at[0], crecv.at[turn, g], sibling, z)

    def hidden_copy(d, m):
        peer = flipped(s, m)
        return remote(
            hid.at[:, pl.ds(pl.multiple_of(d * rows + peer * unit, 128), unit)], hb.at[s, d],
            hsend.at[0], hrecv.at[d], peer, z,
        )

    def hidden_send(d):
        for m in range(1, seqs):
            hidden_copy(d, m).start()

    def hidden_wait(d):
        whole = hb.at[pl.ds(0, seqs - 1), d]
        remote(whole, whole, hsend.at[0], hrecv.at[d], s, z).wait_recv()

    def own_send(g):
        for kind in kinds(g):

            @pl.when(z < last)
            def _():
                line_copy(z, 1, g, kind).start()

            @pl.when(z > 0)
            def _():
                line_copy(z, 0, g, kind).start()

    inner = (z > 0) & (z < last)

    def line_wait(turn, g):
        whole = w_ref.at[g, pl.ds(0, unit * (2 if g in WIDE else 1)), :]
        remote(whole, whole, zsend.at[0, shards[turn]], zrecv.at[shards[turn], g], s, z).wait_recv()

    def forward(turn, g):
        shard = shards[turn]

        @pl.when(inner)
        def _():
            line_wait(turn, g)
            for kind in kinds(g):

                @pl.when(shard < z)
                def _():
                    line_copy(shard, 1, g, kind).start()

                @pl.when(shard > z)
                def _():
                    line_copy(shard, 0, g, kind).start()

    def cube_wait(turn, g, step):
        whole = w_ref.at[g, pl.ds(0, unit << step), :]
        remote(whole, whole, qsend.at[0], qrecv.at[turn, g, step], s, z).wait_recv()

    def cube_send(turn, g, step):
        for which in range(1 << step):
            for h in range(2):
                cube_copy(turn, g, h, step, which, False).start()

    def pair_send(turn, g):
        for m in range(seqs // 2):
            pair_copy(turn, g, m, False).start()

    def pair_wait(turn, g):
        whole = w_ref.at[g, pl.ds(0, unit * (seqs // 2)), :]
        remote(whole, whole, csend.at[0], crecv.at[turn, g], s, z).wait_recv()
        if g not in landed:
            landed.add(g)
            sums[g] = shard_product(g, z)
        sums[g] += shard_product(g, shards[turn])

    def begin(turn, g):
        @pl.when(jnp.logical_not(inner))
        def _():
            line_wait(turn, g)

        if g not in WIDE:
            cube_send(turn, g, 0)
        else:
            cube_send(turn, g, 1)

    def cube_next(turn, g):
        cube_wait(turn, g, 0)
        cube_send(turn, g, 1)

    def pair_send_after(turn, g):
        cube_wait(turn, g, bits - 2)
        pair_send(turn, g)

    first.wait()
    loads[0].start()
    lead = unit // QB
    for i in range(lead):
        scale_block(s * lead + i, lead_ref, i * QB)
    pl.semaphore_wait(barrier, sum(1 if present is None else jnp.where(present, 1, 0) for present, _, _ in partners))

    own_send(0)
    loads[1].wait()
    hidden_send(0)
    loads[0].wait()

    def scale_rest(i, carry):
        place = (s * lead + lead + i) % (rows // QB)
        scale_block(place, blk, pl.multiple_of(place * QB, QB))
        return carry

    lax.fori_loop(0, rows // QB - lead, scale_rest, 0)
    loads[2].start()
    loads[3].start()
    row = lax.broadcasted_iota(jnp.int32, (tok, tok), 0)
    col = lax.broadcasted_iota(jnp.int32, (tok, tok), 1)
    bias[...] = jnp.where((col > row) & (linear < reach), NEG, 0.0)
    for offset in range(1, reach + 1):

        @pl.when(linear < offset)
        def _():
            win[(reach - offset) * tok : (reach - offset + 1) * tok, :] = jnp.zeros((tok, cols), jnp.bfloat16)

        @pl.when(linear + offset >= devices)
        def _():
            ret[offset - 1] = jnp.zeros((tok, cols), jnp.bfloat16)

    @pl.when(z == 0)
    def _():
        for g in range(heads):
            upr[g, 0] = jnp.zeros((unit, duo), jnp.bfloat16)

    @pl.when(z == last)
    def _():
        for g in range(heads):
            dnr[g, last] = jnp.zeros((unit, duo), jnp.bfloat16)

    landed = set()

    def shard_product(g, shard):
        at = pl.ds(pl.multiple_of(shard * rows, 128), rows)
        return jnp.dot(hid[:, at], w_ref[g, at, :], preferred_element_type=jnp.float32)

    def project_chunk(g):
        total = sums[g]
        win[span:, g * duo : (g + 1) * duo] = total.astype(jnp.bfloat16)
        for offset in range(1, reach + 1):

            @pl.when(linear + offset < devices)
            def _():
                halo_copy(g, offset, False).start()

    def halo_copy(g, offset, incoming):
        other = linear - offset if incoming else linear + offset
        return remote(
            win.at[pl.ds(span, tok), chunk(g)], win.at[pl.ds((reach - offset) * tok, tok), chunk(g)],
            ksend.at[offset - 1], krecv.at[g, offset - 1], other // groups, other % groups,
        )

    def back_copy(g, offset, incoming):
        other = linear + offset if incoming else linear - offset
        return remote(
            back.at[offset - 1, :, chunk(g)], ret.at[offset - 1, :, chunk(g)],
            bsend.at[offset - 1], brecv.at[g, offset - 1], other // groups, other % groups,
        )

    factor = 1.0 / float(HEAD) ** 0.5
    cat = lambda parts: jnp.concatenate(parts, axis=0)

    def attend_chunk(g):
        for offset in range(1, reach + 1):

            @pl.when(linear >= offset)
            def _():
                halo_copy(g, offset, True).wait_recv()

        keys = win[:, g * duo : g * duo + HEAD]
        values = win[:, g * duo + HEAD : (g + 1) * duo]
        cuts = [slice(h * HEAD, (h + 1) * HEAD) for h in range(g * group, (g + 1) * group)]
        q = cat([q_ref[:, cut] for cut in cuts])
        go = cat([g_ref[:, cut] for cut in cuts])
        upper = cat([col > row] * group)
        scores = lax.dot_general(q, keys, nt, preferred_element_type=jnp.float32)
        dprobs = lax.dot_general(go, values, nt, preferred_element_type=jnp.float32)

        def folded(x):
            return [jnp.where(upper, x[:, :tok], x[:, span:])] + [x[:, j * tok : (j + 1) * tok] for j in range(1, reach)]

        def unfolded(x):
            zero = jnp.zeros_like(x[0])
            parts = [jnp.where(upper, x[0], zero)] + x[1:] + [jnp.where(upper, zero, x[0])]
            return jnp.concatenate([part.astype(jnp.bfloat16) for part in parts], axis=1)

        masks = [cat([bias[...]] * group)] + [jnp.where(linear < reach - j, NEG, 0.0) for j in range(1, reach)]
        scores = [x * factor + mask for x, mask in zip(folded(scores), masks)]
        dprobs = folded(dprobs)
        top = jnp.max(functools.reduce(jnp.maximum, scores), axis=-1, keepdims=True)
        expd = [jnp.exp(x - top) for x in scores]
        scale = 1.0 / jnp.sum(functools.reduce(jnp.add, expd), axis=-1, keepdims=True)
        probs = [x * scale for x in expd]
        delta = jnp.sum(functools.reduce(jnp.add, [p * d for p, d in zip(probs, dprobs)]), axis=-1, keepdims=True)
        probs_b = unfolded(probs)
        dscores = unfolded([p * (d - delta) * factor for p, d in zip(probs, dprobs)])
        out = jnp.dot(probs_b, values, preferred_element_type=jnp.float32).astype(jnp.bfloat16)
        gq = jnp.dot(dscores, keys, preferred_element_type=jnp.float32).astype(jnp.bfloat16)
        for i, cut in enumerate(cuts):
            ao[:, cut] = out[i * tok : (i + 1) * tok]
            dq[:, cut] = gq[i * tok : (i + 1) * tok]
        dk = lax.dot_general(dscores, q, tn, preferred_element_type=jnp.float32)
        dv = lax.dot_general(probs_b, go, tn, preferred_element_type=jnp.float32)
        for side, value in ((0, dk), (HEAD, dv)):
            cut = slice(g * duo + side, g * duo + side + HEAD)
            for offset in range(1, reach + 1):
                back[offset - 1, :, cut] = value[(reach - offset) * tok : (reach - offset + 1) * tok].astype(jnp.bfloat16)
            own[:, cut] = value[span:]
        for offset in range(1, reach + 1):

            @pl.when(linear >= offset)
            def _():
                back_copy(g, offset, False).start()

    def cube_mask(h, step, which):
        return sum(1 << orders[h][k] for k in range(step) if which >> k & 1)

    def every_copy(g, h, step, which):
        block = every.at[flipped(s, cube_mask(h, step, which)), pl.ds(h * (tok // 2), tok // 2), chunk(g)]
        return remote(block, block, esend.at[0], erecv.at[g, step], flipped(s, 1 << orders[h][step]), z)

    def every_send(g, step):
        for which in range(1 << step):
            for h in range(2):
                every_copy(g, h, step, which).start()

    def every_pair(g, m, incoming):
        block = every.at[flipped(s, m | 1 if incoming else m), :, chunk(g)]
        return remote(block, block, fsend.at[0], frecv.at[g], sibling, z)

    def settle(g):
        for offset in range(1, reach + 1):

            @pl.when(linear + offset < devices)
            def _():
                back_copy(g, offset, True).wait_recv()

        cut = slice(g * duo, (g + 1) * duo)
        total = own[:, cut]
        seg = total
        for offset in range(1, reach + 1):
            piece = ret[offset - 1, :, cut].astype(jnp.float32)
            total = total + piece
            seg = seg + piece * jnp.where(z + offset < groups, 1.0, 0.0)
        every[s, :, cut] = total.astype(jnp.bfloat16)
        inside[:, cut] = seg.astype(jnp.bfloat16)
        every_send(g, 0)
        every_pair(g, 0, False).start()

    def widen(g):
        whole = every.at[0, :, chunk(g)]
        remote(whole, whole, esend.at[0], erecv.at[g, 0], s, z).wait_recv()
        every_send(g, 1)

    def share(g):
        whole = every.at[pl.ds(0, 2), :, chunk(g)]
        remote(whole, whole, esend.at[0], erecv.at[g, 1], s, z).wait_recv()
        for m in peers:
            every_pair(g, m, False).start()

    part_rows = unit // SPLIT

    def half_of(ref, g, d, q):
        return ref.at[g, d, pl.ds(q * part_rows, part_rows), :]

    def up_copy(g, d, q):
        return remote(half_of(ups, g, d, q), half_of(upr, g, d, q), usend.at[d], urecv.at[g, d, q], s, z + 1)

    def down_copy(g, d, q):
        return remote(half_of(dns, g, d, q), half_of(dnr, g, d, q), dsend.at[d], drecv.at[g, d, q], s, z - 1)

    def pass_on(g, d, up, adds):
        source, here, copy = (ups, upr, up_copy) if up else (dns, dnr, down_copy)
        for q in range(SPLIT):
            cut = slice(q * part_rows, (q + 1) * part_rows)
            value = part[g, d, cut]
            if adds:
                copy(g, d, q).wait_recv()
                value = value + here[g, d, cut].astype(jnp.float32)
            source[g, d, cut] = value.astype(jnp.bfloat16)
            copy(g, d, q).start()

    def hop(g, k):
        @pl.when(z == k)
        def _():
            for d in range(last, k, -1):
                pass_on(g, d, True, True)

        @pl.when(z == last - k)
        def _():
            for d in range(last - k):
                pass_on(g, d, False, True)

    def product(g):
        whole = every.at[pl.ds(0, seqs // 2), :, chunk(g)]
        remote(whole, whole, fsend.at[0], frecv.at[g], s, z).wait_recv()
        grads = every[:, :, g * duo : (g + 1) * duo].reshape(seqs * tok, duo)
        for i in range(groups):
            d = jnp.where(z == 0, last - i, i)
            rows_of = pl.ds(pl.multiple_of(d * unit, 128), unit)
            part[g, d] = jnp.dot(ht[rows_of, :], grads, preferred_element_type=jnp.float32)
            if i < last:

                @pl.when(z == 0)
                def _():
                    pass_on(g, last - i, True, False)

                @pl.when(z == last)
                def _():
                    pass_on(g, i, False, False)

    def grad_copy(g, h, step, which):
        at = flipped(s, cube_mask(h, step, which)) * unit + h * (unit // 2)
        block = wgb.at[g, pl.ds(pl.multiple_of(at, 16), unit // 2), :]
        return remote(block, block, wsend.at[0], wrecv.at[g, step], flipped(s, 1 << orders[h][step]), z)

    def grad_send(g, step):
        for which in range(1 << step):
            for h in range(2):
                grad_copy(g, h, step, which).start()

    def grad_pair(g, m, incoming):
        owner = flipped(s, m | 1 if incoming else m)
        block = wgb.at[g, pl.ds(pl.multiple_of(owner * unit, 128), unit), :]
        return remote(block, block, xsend.at[0], xrecv.at[g], sibling, z)

    def reduce(g):
        @pl.when(z > 0)
        def _():
            for q in range(SPLIT):
                up_copy(g, z, q).wait_recv()

        @pl.when(z < last)
        def _():
            for q in range(SPLIT):
                down_copy(g, z, q).wait_recv()

        total = part[g, z] + upr[g, z].astype(jnp.float32) + dnr[g, z].astype(jnp.float32)
        wgb[g, pl.ds(pl.multiple_of(s * unit, 128), unit), :] = total.astype(jnp.bfloat16)
        grad_send(g, 0)
        grad_pair(g, 0, False).start()

    def expand(g):
        whole = wgb.at[g, pl.ds(0, unit), :]
        remote(whole, whole, wsend.at[0], wrecv.at[g, 0], s, z).wait_recv()
        grad_send(g, 1)

    def relay(g):
        whole = wgb.at[g, pl.ds(0, 2 * unit), :]
        remote(whole, whole, wsend.at[0], wrecv.at[g, 1], s, z).wait_recv()
        for m in peers:
            grad_pair(g, m, False).start()

    def finish_chunk(g):
        whole = wgb.at[g, pl.ds(0, seqs // 2 * unit), :]
        remote(whole, whole, xsend.at[0], xrecv.at[g], s, z).wait_recv()

    def turn_hidden(d):
        hidden_wait(d)
        hb[s, d] = hid[:, pl.ds(pl.multiple_of(d * rows + s * unit, 128), unit)]
        for i in range(seqs):
            ht[d * unit : (d + 1) * unit, i * tok : (i + 1) * tok] = hb[i, d].T

    slices = 4
    span_cols = gh.shape[1] // slices
    tall = min(512, span_cols)

    def spread(i):
        def step(j, carry):
            at = pl.multiple_of(i * span_cols + j * tall, tall)
            total = jnp.zeros((tok, tall), jnp.float32)
            for g in range(heads):
                grads = inside[:, g * duo : (g + 1) * duo]
                total = total + lax.dot_general(grads, w_ref[g, pl.ds(at, tall), :], nt, preferred_element_type=jnp.float32)
            gh[:, pl.ds(at, tall)] = total.astype(jnp.bfloat16)
            return carry

        lax.fori_loop(0, span_cols // tall, step, 0)

    def drain(ref, sem):
        remote(ref, ref, sem, wrecv.at[0, 0], s, z).wait_send()

    def drain_weights():
        wide = len([g for g in range(heads) if g in WIDE])
        for shard in range(groups):
            moved = w_ref.at[0, pl.ds(0, unit * (heads + wide)), :]

            @pl.when((shard <= z) & (z < last))
            def _():
                drain(moved, zsend.at[1, shard])

            @pl.when((shard >= z) & (z > 0))
            def _():
                drain(moved, zsend.at[0, shard])

        turns = groups - 1
        plane = heads * (seqs // 2 - 1) - wide
        drain(w_ref.at[pl.ds(0, turns), pl.ds(0, unit * plane), :], qsend.at[0])
        drain(w_ref.at[pl.ds(0, turns), pl.ds(0, unit * heads * (seqs // 2)), :], csend.at[0])

    def drain_tokens():
        drain(hb.at[pl.ds(0, seqs - 1)], hsend.at[0])
        for offset in range(1, reach + 1):

            @pl.when(linear + offset < devices)
            def _():
                drain(ret.at[offset - 1], ksend.at[offset - 1])

            @pl.when(linear >= offset)
            def _():
                drain(ret.at[offset - 1], bsend.at[offset - 1])

        drain(every.at[pl.ds(0, len(peers))], esend.at[0])
        drain(every.at[pl.ds(0, seqs // 2)], fsend.at[0])

    works = [own_send, forward, begin, cube_next, pair_send_after, pair_wait, project_chunk, attend_chunk, settle, widen, share]
    works += [product, hop, reduce, expand, relay, finish_chunk, spread, hidden_send, turn_hidden]
    fetched = False
    for place, *places in ORDER:
        if works[place] is attend_chunk and not fetched:
            loads[2].wait()
            loads[3].wait()
            fetched = True
        works[place](*places)
    drain_weights()
    drain_tokens()
    drain(wgb.at[:, pl.ds(0, len(peers) * unit), :], wsend.at[0])
    drain(wgb.at[:, pl.ds(0, seqs // 2 * unit), :], xsend.at[0])
    for d in range(groups):

        @pl.when(d > z)
        def _():
            drain(ups.at[:, d], usend.at[d])

        @pl.when(d < z)
        def _():
            drain(dns.at[:, d], dsend.at[d])


def fused(hidden, kv_blocks, kv_scale, queries, grad_out, reach):
    seqs = lax.axis_size("seq")
    groups = lax.axis_size("fsdp")
    tok, depth = hidden.shape
    rows, cols = kv_blocks.shape
    width = queries.shape[1]
    unit = rows // seqs
    heads = cols // (2 * HEAD)
    duo = 2 * HEAD
    count = (reach + 1) * tok
    bits = seqs.bit_length() - 1
    any_space = pl.BlockSpec(memory_space=pl.ANY)
    dma = pltpu.SemaphoreType.DMA
    b16 = lambda *shape: pltpu.VMEM(shape, jnp.bfloat16)
    f32 = lambda *shape: pltpu.VMEM(shape, jnp.float32)
    return pl.pallas_call(
        functools.partial(fused_kernel, seqs, groups, reach),
        out_shape=[b16(tok, width), b16(tok, width), b16(tok, depth), b16(heads, rows, duo)],
        in_specs=[any_space, any_space, pl.BlockSpec(memory_space=pltpu.SMEM), any_space, any_space],
        out_specs=[pl.BlockSpec(memory_space=pltpu.VMEM)] * 4,
        scratch_shapes=[
            b16(tok, depth), b16(rows, cols), b16(tok, width), b16(tok, width),
            b16(heads, depth, duo), b16(count, cols),
            b16(reach, tok, cols), b16(reach, tok, cols), f32(tok, cols), b16(seqs, tok, cols), b16(tok, cols),
            b16(seqs, groups, tok, unit), b16(groups * unit, seqs * tok), f32(heads, groups, unit, duo),
            b16(heads, groups, unit, duo), b16(heads, groups, unit, duo), b16(heads, groups, unit, duo), b16(heads, groups, unit, duo),
            f32(tok, tok), b16(unit, cols), f32(heads, tok, duo),
            dma((5,)), dma((2, groups)), dma((groups, heads)),
            dma((1,)), dma((groups - 1, heads, bits - 1)), dma((1,)), dma((groups - 1, heads)), dma((1,)), dma((groups,)),
            dma((reach,)), dma((heads, reach)), dma((reach,)), dma((heads, reach)),
            dma((1,)), dma((heads, 2)), dma((1,)), dma((heads,)),
            dma((groups,)), dma((heads, groups, SPLIT)), dma((groups,)), dma((heads, groups, SPLIT)),
            dma((1,)), dma((heads, 2)), dma((1,)), dma((heads,)),
        ],
        compiler_params=pltpu.CompilerParams(collective_id=0, has_side_effects=True, vmem_limit_bytes=VMEM_LIMIT),
        name="fused",
    )(hidden, kv_blocks, kv_scale.T, queries, grad_out)


def write_kernel(ao, dq, gh, wgb, ao_out, dq_out, gh_out, wg_out, wide, osem):
    parts, size, cols = wide.shape
    heads = wgb.shape[0]
    triples = ((ao, ao_out), (dq, dq_out), (gh, gh_out))
    stores = [pltpu.make_async_copy(src, dst, osem.at[parts + k]) for k, (src, dst) in enumerate(triples)]
    for copy in stores:
        copy.start()
    for p in range(parts):
        for g in range(heads):
            block = wgb[g, p * size : (p + 1) * size, :].astype(jnp.float32)
            wide[p, :, g * HEAD : (g + 1) * HEAD] = block[:, :HEAD]
            wide[p, :, (heads + g) * HEAD : (heads + g + 1) * HEAD] = block[:, HEAD:]
        store = pltpu.make_async_copy(wide.at[p], wg_out.at[pl.ds(p * size, size), :], osem.at[p])
        store.start()
        stores.append(store)
    for copy in stores:
        copy.wait()


def write(ao, dq, gh, wgb):
    parts = 8
    heads, rows, duo = wgb.shape
    any_space = pl.BlockSpec(memory_space=pl.ANY)
    return pl.pallas_call(
        write_kernel,
        out_shape=[jax.ShapeDtypeStruct(x.shape, x.dtype) for x in (ao, dq, gh)]
        + [jax.ShapeDtypeStruct((rows, heads * duo), jnp.float32)],
        in_specs=[pl.BlockSpec(memory_space=pltpu.VMEM)] * 4,
        out_specs=[any_space] * 4,
        scratch_shapes=[pltpu.VMEM((parts, rows // parts, heads * duo), jnp.float32), pltpu.SemaphoreType.DMA((parts + 3,))],
        compiler_params=pltpu.CompilerParams(vmem_limit_bytes=12 << 20),
        name="write",
    )(ao, dq, gh, wgb)


def body(hidden, kv_blocks, kv_scale, queries, grad_out):
    tok = hidden.shape[0]
    groups = lax.axis_size("fsdp")
    reach = groups // 2
    unit = kv_blocks.shape[0] // lax.axis_size("seq")
    heads = kv_blocks.shape[1] // (2 * HEAD)
    if unit % QB == 0 and (heads, groups, lax.axis_size("seq")) == PLANNED:
        outs = fused(hidden, kv_blocks, kv_scale, queries, grad_out, reach)
        return tuple(write(*outs))
    weights, kv, columns = project(hidden, kv_blocks, kv_scale)
    pieces = []
    for offset in range(reach, 0, -1):
        pieces.append(shifted(kv, ("seq", "fsdp"), offset))
    window = jnp.concatenate(pieces + [kv], axis=0)
    columns = columns.reshape(groups * tok, columns.shape[2])
    attn_out, grad_queries, dwin = attend(queries, window, grad_out, reach)
    back = dwin[: reach * tok].astype(jnp.bfloat16)
    own = dwin[reach * tok :]
    grad_hidden, weight_grad = finish(back, own, weights, columns, reach)
    return (attn_out, grad_queries, grad_hidden, weight_grad.astype(jnp.float32))


def solution(mesh):
    return jax.shard_map(
        body,
        mesh=mesh,
        in_specs=(
            P(("seq", "fsdp"), None),
            P("fsdp", None),
            P("fsdp", None),
            P(("seq", "fsdp"), None),
            P(("seq", "fsdp"), None),
        ),
        out_specs=(
            P(("seq", "fsdp"), None),
            P(("seq", "fsdp"), None),
            P(("seq", "fsdp"), None),
            P("fsdp", None),
        ),
        check_vma=False,
    )
```
